64 devices in a mesh: data: 4 (over x, y), dap: 16 (over z, core).
Axes of the slice: x: 2, y: 2, z: 8, core: 2. Of those that a mesh axis runs over, the one named last changes fastest.
The devices are a block of a 4x4x8 slice.
Arguments:
- msa_act: bfloat16 [8, 64, 192, 256], P('data', 'dap'), parts along dimension 0
- pair_act: bfloat16 [8, 192, 192, 128], P('data', 'dap'), parts along dimension 0
- msa_mask: int32 [8, 64, 192], P('data'), parts along dimension 0
- res_mask: int32 [8, 192], P('data'), parts along dimension 0
- w_row_bias: bfloat16 [128, 8], replicated
- w_row_qkvg: bfloat16 [256, 4, 8, 32], replicated
- w_row_out: bfloat16 [8, 32, 256], replicated
- w_col_qkvg: bfloat16 [256, 4, 8, 32], replicated
- w_col_out: bfloat16 [8, 32, 256], replicated
- w_opm_ac: bfloat16 [256, 2, 32], replicated
- w_opm_out: bfloat16 [32, 32, 128], replicated
- w_ts_bias: bfloat16 [128, 4], replicated
- w_ts_qkvg: bfloat16 [128, 4, 4, 32], replicated
- w_ts_out: bfloat16 [4, 32, 128], replicated
- w_te_bias: bfloat16 [128, 4], replicated
- w_te_qkvg: bfloat16 [128, 4, 4, 32], replicated
- w_te_out: bfloat16 [4, 32, 128], replicated
Outputs:
- output 1: bfloat16 [8, 64, 192, 256], P('data', 'dap'), parts along dimension 0
- output 2: bfloat16 [8, 192, 192, 128], P('data', 'dap'), parts along dimension 0
There are 4 independent parts. The reference program is written for one: setup_inputs(seed, part) draws one part's arguments, and reference() takes and returns one part's arrays. A program takes and returns all parts, laid end to end along the dimension named above; an argument that names none is the same for every part.
All inputs are finite; a program needn't handle non-finite values.
Results may differ from the reference program's by a relative error of at most 0.0158742.
Values are sent between devices in bfloat16 or wider.
A program may use at most 768 MiB of HBM per device.

```python
import jax
import jax.numpy as jnp
from jax import lax

CROPS = 2
NS = 64
NR = 192
C_M = 256
C_Z = 128
MSA_HEADS = 8
MSA_HEAD = 32
TRI_HEADS = 4
TRI_HEAD = 32
OPM_DIM = 32
SCORE_ELEMS = 8388608
MASK_SCALE = 10000.0
LN_EPS = 1e-5
OPM_EPS = 1e-3


def as_float(tensor):
    return tensor.astype(jnp.float32)


def layer_norm(tensor):
    x_float = tensor.astype(jnp.float32)
    mean_val = jnp.mean(x_float, axis=-1, keepdims=True)
    centred = x_float - mean_val
    var_val = jnp.mean(centred * centred, axis=-1, keepdims=True)
    return (centred * lax.rsqrt(var_val + LN_EPS)).astype(jnp.bfloat16)


def mask_to_bias(mask):
    return (mask.astype(jnp.float32) - 1.0) * MASK_SCALE


def rows_per_map(n_rows, per_row):
    return max(1, min(n_rows, SCORE_ELEMS // per_row))


def gated_attention(x_row, key_bias, pair_bias, w_qkvg, w_out):
    normed = layer_norm(x_row)
    proj_all = jnp.einsum('lc,cghd->glhd', as_float(normed), as_float(w_qkvg))
    queries = proj_all[0].astype(jnp.bfloat16)
    keys_bf = proj_all[1].astype(jnp.bfloat16)
    values_bf = proj_all[2].astype(jnp.bfloat16)
    gate_sig = jax.nn.sigmoid(proj_all[3])
    inv_sqrt = queries.shape[-1] ** -0.5
    logits = jnp.einsum('qhd,khd->hqk', as_float(queries), as_float(keys_bf)) * inv_sqrt + key_bias
    if pair_bias is not None:
        logits = logits + as_float(pair_bias)
    attn_prob = jax.nn.softmax(logits, axis=-1).astype(jnp.bfloat16)
    mixed = jnp.einsum('hqk,khd->qhd', as_float(attn_prob), as_float(values_bf)) * gate_sig
    update = jnp.einsum('qhd,hdc->qc', as_float(mixed.astype(jnp.bfloat16)), as_float(w_out))
    return (x_row.astype(jnp.float32) + update).astype(jnp.bfloat16)


def attend_rows(row_stack, key_rows, pair_bias, w_qkvg, w_out):
    n_rows = row_stack.shape[0]
    length = row_stack.shape[1]
    n_heads = w_qkvg.shape[2]
    return lax.map(lambda row_in: gated_attention(row_in[0], row_in[1], pair_bias, w_qkvg, w_out),
                   (row_stack, key_rows), batch_size=rows_per_map(n_rows, n_heads * length * length))


def pair_bias_of(pair_act, w_bias):
    return jnp.einsum('ijc,ch->hij', as_float(layer_norm(pair_act)), as_float(w_bias)).astype(jnp.bfloat16)


def triangle_start(pair_act, res_mask, w_bias, w_qkvg, w_out):
    n_res = pair_act.shape[0]
    key_rows = jnp.broadcast_to(mask_to_bias(res_mask)[None, :], (n_res, n_res))
    return attend_rows(pair_act, key_rows, pair_bias_of(pair_act, w_bias), w_qkvg, w_out)


def outer_product_mean(msa_act, pair_act, msa_mask, w_opm_ac, w_opm_out):
    mask_t = msa_mask.astype(jnp.float32).T
    proj_ac = jnp.einsum('sic,cpe->pise', as_float(layer_norm(msa_act)), as_float(w_opm_ac)).astype(jnp.bfloat16)
    left_proj = as_float(proj_ac[0]) * mask_t[:, :, None]
    right_proj = as_float(proj_ac[1]) * mask_t[:, :, None]
    norm_pairs = jnp.dot(mask_t, mask_t.T)
    n_res = right_proj.shape[0]
    width = right_proj.shape[2]

    def one_row(row_in):
        left_row, norm_row, pair_row = row_in
        outer = jnp.einsum('se,jsf->jef', left_row, right_proj) / (norm_row[:, None, None] + OPM_EPS)
        update = jnp.einsum('jef,efc->jc', as_float(outer.astype(jnp.bfloat16)), as_float(w_opm_out))
        return (pair_row.astype(jnp.float32) + update).astype(jnp.bfloat16)

    return lax.map(one_row, (left_proj, norm_pairs, pair_act), batch_size=rows_per_map(n_res, n_res * width * width))


def evoformer_crop(msa_act, pair_act, msa_mask, res_mask, weights):
    (w_row_bias, w_row_qkvg, w_row_out, w_col_qkvg, w_col_out, w_opm_ac, w_opm_out,
     w_ts_bias, w_ts_qkvg, w_ts_out, w_te_bias, w_te_qkvg, w_te_out) = weights
    msa_act = attend_rows(msa_act, mask_to_bias(msa_mask), pair_bias_of(pair_act, w_row_bias), w_row_qkvg, w_row_out)
    msa_cols = attend_rows(jnp.swapaxes(msa_act, 0, 1), mask_to_bias(msa_mask.T), None, w_col_qkvg, w_col_out)
    msa_act = jnp.swapaxes(msa_cols, 0, 1)
    pair_act = outer_product_mean(msa_act, pair_act, msa_mask, w_opm_ac, w_opm_out)
    pair_act = triangle_start(pair_act, res_mask, w_ts_bias, w_ts_qkvg, w_ts_out)
    pair_cols = triangle_start(jnp.swapaxes(pair_act, 0, 1), res_mask, w_te_bias, w_te_qkvg, w_te_out)
    return msa_act, jnp.swapaxes(pair_cols, 0, 1)


def normal_weight(key, shape, fan_in, gain):
    return (jax.random.normal(key, shape, jnp.float32) * (gain * fan_in ** -0.5)).astype(jnp.bfloat16)


def qkvg_weight(key, width, n_heads, head_dim):
    gains = jnp.array([1.5, 1.5, 1.0, 1.0], jnp.float32)[None, :, None, None]
    draw = jax.random.normal(key, (width, 4, n_heads, head_dim), jnp.float32)
    return (draw * gains * width ** -0.5).astype(jnp.bfloat16)


def setup_inputs(seed: int = 0, part: int = 0) -> dict:
    part_keys = jax.random.split(jax.random.fold_in(jax.random.key(seed), part), 5)
    w_keys = jax.random.split(jax.random.key(seed + 1), 13)
    base = jax.random.normal(part_keys[0], (CROPS, 1, NR, C_M), jnp.float32)
    noise = jax.random.normal(part_keys[1], (CROPS, NS, NR, C_M), jnp.float32)
    msa_act = (0.6 * base + 0.8 * noise).astype(jnp.bfloat16)
    pair_act = jax.random.normal(part_keys[2], (CROPS, NR, NR, C_Z), jnp.float32).astype(jnp.bfloat16)
    msa_mask = (jax.random.randint(part_keys[3], (CROPS, NS, NR), 0, 5) > 0).astype(jnp.int32)
    res_mask = (jax.random.randint(part_keys[4], (CROPS, NR), 0, 4) > 0).astype(jnp.int32)
    msa_width = MSA_HEADS * MSA_HEAD
    tri_width = TRI_HEADS * TRI_HEAD
    return {
        'msa_act': msa_act,
        'pair_act': pair_act,
        'msa_mask': msa_mask,
        'res_mask': res_mask,
        'w_row_bias': normal_weight(w_keys[0], (C_Z, MSA_HEADS), C_Z, 2.0),
        'w_row_qkvg': qkvg_weight(w_keys[1], C_M, MSA_HEADS, MSA_HEAD),
        'w_row_out': normal_weight(w_keys[2], (MSA_HEADS, MSA_HEAD, C_M), msa_width, 1.0),
        'w_col_qkvg': qkvg_weight(w_keys[3], C_M, MSA_HEADS, MSA_HEAD),
        'w_col_out': normal_weight(w_keys[4], (MSA_HEADS, MSA_HEAD, C_M), msa_width, 1.0),
        'w_opm_ac': normal_weight(w_keys[5], (C_M, 2, OPM_DIM), C_M, 1.0),
        'w_opm_out': normal_weight(w_keys[6], (OPM_DIM, OPM_DIM, C_Z), OPM_DIM * OPM_DIM, 1.0),
        'w_ts_bias': normal_weight(w_keys[7], (C_Z, TRI_HEADS), C_Z, 2.0),
        'w_ts_qkvg': qkvg_weight(w_keys[8], C_Z, TRI_HEADS, TRI_HEAD),
        'w_ts_out': normal_weight(w_keys[9], (TRI_HEADS, TRI_HEAD, C_Z), tri_width, 1.0),
        'w_te_bias': normal_weight(w_keys[10], (C_Z, TRI_HEADS), C_Z, 2.0),
        'w_te_qkvg': qkvg_weight(w_keys[11], C_Z, TRI_HEADS, TRI_HEAD),
        'w_te_out': normal_weight(w_keys[12], (TRI_HEADS, TRI_HEAD, C_Z), tri_width, 1.0),
    }


def reference(msa_act, pair_act, msa_mask, res_mask, w_row_bias, w_row_qkvg, w_row_out, w_col_qkvg, w_col_out,
              w_opm_ac, w_opm_out, w_ts_bias, w_ts_qkvg, w_ts_out, w_te_bias, w_te_qkvg, w_te_out):
    weights = (w_row_bias, w_row_qkvg, w_row_out, w_col_qkvg, w_col_out, w_opm_ac, w_opm_out,
               w_ts_bias, w_ts_qkvg, w_ts_out, w_te_bias, w_te_qkvg, w_te_out)
    msa_out, pair_out = lax.map(lambda crop_in: evoformer_crop(crop_in[0], crop_in[1], crop_in[2], crop_in[3], weights),
                                (msa_act, pair_act, msa_mask, res_mask))
    return msa_out, pair_out
```

```python
import functools
import math

import jax
import jax.numpy as jnp
import numpy as np
from jax import lax
from jax.experimental import pallas as pl
from jax.experimental.pallas import tpu as pltpu
from jax.sharding import PartitionSpec as P

MASK_SCALE = 10000.0
LN_EPS = 1e-5
OPM_EPS = 1e-3
LOG2E = math.log2(math.e)
N_WEIGHTS = 13
PART_AXIS = 'data'
GROUP_AXIS = 'dap'
MESH = pl.DeviceIdType.MESH
F32 = jnp.float32
BF16 = jnp.bfloat16
HD = 32
VMEM_BYTES = 60 * 1024 * 1024


def dot(a, b):
    return lax.dot_general(a, b, (((1,), (0,)), ((), ())), preferred_element_type=F32)


def dot_nt(a, b):
    return lax.dot_general(a, b, (((1,), (1,)), ((), ())), preferred_element_type=F32)


def dot_tn(a, b):
    return lax.dot_general(a, b, (((0,), (0,)), ((), ())), preferred_element_type=F32)


def layer_norm(x):
    x_float = x.astype(F32)
    centred = x_float - jnp.mean(x_float, axis=-1, keepdims=True)
    var = jnp.mean(centred * centred, axis=-1, keepdims=True)
    return (centred * lax.rsqrt(var + LN_EPS)).astype(BF16)


def sigmoid(x):
    return 1.0 / (1.0 + jnp.exp2(x * (-LOG2E)))


def iota(shape, dim):
    return lax.broadcasted_iota(jnp.int32, shape, dim)


def permutation(sizes, order, keep=None):
    total = int(np.prod(sizes))
    source = np.arange(total).reshape(sizes).transpose(order).reshape(-1)
    out = np.zeros((total, total), np.float32)
    out[np.arange(total), source] = 1.0
    return out


def softmax_cols(t):
    e = jnp.exp2(t - jnp.max(t, axis=0, keepdims=True))
    return (e * (1.0 / jnp.sum(e, axis=0, keepdims=True))).astype(BF16)


def pair_attention(y, w_t, w_out, bias_of):
    length, width = y.shape
    two = 2 * length
    scale = HD ** -0.5 * LOG2E
    y2 = jnp.concatenate([y, y], axis=0)
    q2 = dot_nt(w_t[0:width, :], y2)
    odd_head = (iota((width, two), 0) // HD) % 2
    right = (iota((width, two), 1) >= length).astype(jnp.int32)
    q2 = jnp.where(odd_head == right, q2, 0.0).astype(BF16)
    keys = dot_nt(y, w_t[width:2 * width, :]).astype(BF16)
    values = dot_nt(w_t[2 * width:3 * width, :], y).astype(BF16)
    gate = sigmoid(dot_nt(w_t[3 * width:4 * width, :], y))
    zeros = jnp.zeros((2 * HD, two), BF16)
    pieces = []
    for pair in range(width // (2 * HD)):
        rows = q2[2 * HD * pair:2 * HD * (pair + 1), :]
        lanes = 128 * (pair // 2)
        stacked = jnp.concatenate([rows, zeros] if pair % 2 == 0 else [zeros, rows], axis=0)
        logits = dot(keys[:, lanes:lanes + 128], stacked)
        probs = softmax_cols(logits * scale + bias_of(pair))
        mixed = dot(values[2 * HD * pair:2 * HD * (pair + 1), :], probs)
        pieces.append(mixed[0:HD, 0:length])
        pieces.append(mixed[HD:2 * HD, length:two])
    gated = (gate * jnp.concatenate(pieces, axis=0)).astype(BF16)
    return dot_tn(gated, w_out[...])


def column_attention(y, w_t, w_out, mask_bias):
    length, width = y.shape
    heads = width // HD
    scale = HD ** -0.5 * LOG2E
    wide = heads * length
    q_all = dot_nt(w_t[0:width, :], jnp.concatenate([y] * heads, axis=0))
    q_all = jnp.where(iota((width, wide), 0) // HD == iota((width, wide), 1) // length, q_all, 0.0).astype(BF16)
    keys = dot_nt(y, w_t[width:2 * width, :]).astype(BF16)
    values = dot_nt(w_t[2 * width:3 * width, :], y).astype(BF16)
    gate = sigmoid(dot_nt(w_t[3 * width:4 * width, :], y))
    probs = softmax_cols(dot(keys, q_all) * scale + mask_bias)
    mixed = dot(values, probs)
    pieces = [mixed[HD * h:HD * (h + 1), length * h:length * (h + 1)] for h in range(heads)]
    gated = (gate * jnp.concatenate(pieces, axis=0)).astype(BF16)
    return dot_tn(gated, w_out[...])


def block_kernel(n, x_ref, z_ref, mm_ref, rm_ref,
                 w_rb, w_r, w_ro, w_c, w_co, w_ac, w_oo, w_tsb, w_ts, w_tso, w_teb, w_te, w_teo,
                 p2, p2t, p3, p3t, p4, p4e, p5, p6, eye, tok,
                 out_m, out_z,
                 g_row, g_c, g_t1, g_t2, s1, r1, s2, r2, s3, r3, s4, r4,
                 tmp_b, b_q, bm_row, bm_tri, x1, y1, m_t, rn, a_t, c_t, c_f, u_s, w_f32, w_fe, z1, yn, x3,
                 gs_a, gr_a, gs_b, gr_b, as_sem, ar_sem):
    me = lax.axis_index(GROUP_AXIS)
    chips = n // 2
    chip = me // 2
    core = me % 2
    partner = me + 1 - 2 * core
    crops, seqs, length, width = x_ref.shape
    rows = z_ref.shape[1]
    quads = rows // 4
    blocks = length // 64
    blk = 4 * rows
    sup = 4 * blk
    steps = []
    for k in range(1, chips // 2 + 1):
        steps.append(k)
        if chips - k != k:
            steps.append(chips - k)

    barrier = pltpu.get_barrier_semaphore()
    for k in range(1, n):
        pl.semaphore_signal(barrier, inc=1, device_id={GROUP_AXIS: lax.rem(me + k, n)}, device_id_type=MESH)
    pl.semaphore_wait(barrier, n - 1)

    def remote(src, dst, send, recv, device):
        return pltpu.make_async_remote_copy(src_ref=src, dst_ref=dst, send_sem=send, recv_sem=recv,
                                            device_id={GROUP_AXIS: device}, device_id_type=MESH)

    def same_core(k):
        return 2 * lax.rem(chip + k, chips) + core

    def gather_start(buf, e, c):
        mine = buf.at[c, me]
        for k in steps:
            remote(mine, mine, gs_a.at[e, c], gr_a.at[e, c], same_core(k)).start()
        remote(mine, mine, gs_b.at[e, c], gr_b.at[e, c], partner).start()

    def wait_bytes(ref, sem):
        pltpu.make_async_copy(ref, ref, sem).wait()

    def gather_forward(buf, e, c):
        wait_bytes(buf.at[c, pl.ds(0, chips - 1)], gr_a.at[e, c])
        for k in steps:
            block = buf.at[c, same_core(k)]
            remote(block, block, gs_b.at[e, c], gr_b.at[e, c], partner).start()

    def gather_wait(buf, e, c):
        wait_bytes(buf.at[c, pl.ds(0, chips)], gr_b.at[e, c])

    def gather_end(buf, e, c):
        wait_bytes(buf.at[c, pl.ds(0, chips - 1)], gs_a.at[e, c])
        wait_bytes(buf.at[c, pl.ds(0, chips)], gs_b.at[e, c])

    def block_of(ref, c, d, planes):
        where = pl.ds(pl.multiple_of(d * blk, 16), blk)
        return ref.at[c, :, where, :] if planes else ref.at[c, where, :]

    def exchange_start(src, dst, e, c, planes):
        here = pl.ds(pl.multiple_of(me * blk, 16), blk)
        if planes:
            dst[c, :, here, :] = src[c, :, here, :]
        else:
            dst[c, here, :] = src[c, here, :]
        landing = block_of(dst, c, me, planes)
        for k in steps:
            for other in range(2):
                d = 2 * lax.rem(chip + k, chips) + (core + other) % 2
                remote(block_of(src, c, d, planes), landing, as_sem.at[e, c], ar_sem.at[e, c], d).start()
        remote(block_of(src, c, partner, planes), landing, as_sem.at[e, c], ar_sem.at[e, c], partner).start()

    def others(ref, c, planes):
        where = pl.ds(0, (n - 1) * blk)
        return ref.at[c, :, where, :] if planes else ref.at[c, where, :]

    def exchange_wait(dst, e, c, planes):
        wait_bytes(others(dst, c, planes), ar_sem.at[e, c])

    def exchange_end(src, e, c, planes):
        wait_bytes(others(src, c, planes), as_sem.at[e, c])

    def loop(count, body):
        lax.fori_loop(0, count, lambda i, carry: (body(i), carry)[1], 0)

    tmp_b[...] = jnp.zeros_like(tmp_b)

    def row_bias(c):
        def one(i):
            tmp_b[pl.ds(pl.multiple_of(i * 8, 8), 8), :] = dot_nt(w_rb[...], layer_norm(z_ref[c, i]))
        loop(rows, one)
        g_row[c, me] = dot(p6[...], tmp_b[...].astype(BF16)).astype(BF16)
        gather_start(g_row, 0, c)
    loop(crops, row_bias)

    w_f32[...] = w_oo[...].astype(F32)
    for fp in range(HD // 2):
        for half in range(2):
            at = fp * 2 * HD + half * HD
            w_fe[at:at + HD, :] = w_f32[pl.ds(half * (HD // 2) + fp, HD, stride=HD), :].astype(BF16)

    def unpack_bias(buf, c, group, perm, first, pieces, piece):
        for sb in range(n // 4):
            part = buf[c, 4 * sb:4 * sb + 4, blk * group:blk * (group + 1), :]
            moved = dot(perm[...], part.reshape(sup, length)).astype(BF16)
            for i in range(pieces):
                at = first + i * (length * 4 // pieces) + sb * piece
                b_q[at:at + piece, :] = moved[i * piece:(i + 1) * piece, :]

    def mask_columns(row, select):
        wide = jnp.broadcast_to(row.astype(F32), (128, length)).astype(BF16)
        return (dot_nt(select[...], wide) - 1.0) * (MASK_SCALE * LOG2E)

    def row_attention(c):
        gather_forward(g_row, 0, c)
        gather_wait(g_row, 0, c)
        for group in range(width // HD // 4):
            unpack_bias(g_row, c, group, p4, group * 4 * length, 4, blk)
        for pair in range(width // HD // 2):
            at = 2 * length * pair
            bm_row[:, at:at + 2 * length] = dot_nt(eye[...], b_q[at:at + 2 * length, :]) * LOG2E

        def one(s):
            x = x_ref[c, s]
            col = mask_columns(mm_ref[c, pl.ds(me * seqs + s, 1), :], eye)
            col3 = jnp.concatenate([col] * (2 * length // 128), axis=1)
            update = pair_attention(layer_norm(x), w_r, w_ro,
                                    lambda pair: bm_row[:, 2 * length * pair:2 * length * (pair + 1)] + col3)
            x1[s] = (x.astype(F32) + update).astype(BF16)
        loop(seqs, one)
        for b in range(blocks):
            part = x1[:, 64 * b:64 * (b + 1), :].reshape(256, width)
            s1[c, 256 * b:256 * (b + 1), :] = dot(p2[...], part).astype(BF16)
        exchange_start(s1, r1, 0, c, False)
    loop(crops, row_attention)

    def columns(c):
        exchange_wait(r1, 0, c, False)
        for sb in range(n // 4):
            moved = dot(p3[...], r1[c, sup * sb:sup * (sb + 1), :]).astype(BF16)
            for i in range(rows):
                y1[i, 16 * sb:16 * (sb + 1), :] = moved[16 * i:16 * (i + 1), :]
        n_seq = y1.shape[1]
        mk = mm_ref[c].astype(F32).astype(BF16)
        mine = (iota((16, length), 1) == me * rows + iota((16, length), 0)).astype(F32).astype(BF16)
        m_t[...] = dot_nt(mine, jnp.concatenate([mk, mk], axis=0))
        rn[c] = 1.0 / (dot(m_t[:, 0:n_seq].astype(BF16), mk) + OPM_EPS)
        low = iota((HD, 2 * n_seq), 1) < n_seq

        def one(i):
            x = y1[i]
            pick = (iota((128, length), 1) == me * rows + i).astype(F32).astype(BF16)
            col = (dot_nt(mk, pick) - 1.0) * (MASK_SCALE * LOG2E)
            heads = width // HD
            update = column_attention(layer_norm(x), w_c, w_co, jnp.concatenate([col] * (heads * n_seq // 128), axis=1))
            x = (x.astype(F32) + update).astype(BF16)
            y1[i] = x
            y = layer_norm(x)
            both = dot_nt(w_ac[...], jnp.concatenate([y, y], axis=0)).astype(BF16).astype(F32)
            both = both * m_t[pl.ds(i, 1), :]
            a = both[0:HD, :]
            at = pl.ds(pl.multiple_of(i * HD, HD), HD)
            a_t[c, 0, at, :] = jnp.where(low, a, 0.0).astype(BF16)
            a_t[c, 1, at, :] = jnp.where(low, 0.0, a).astype(BF16)
            half = HD // 2
            packed = jnp.where(low[0:half], both[HD:HD + half, :], both[HD + half:2 * HD, :])
            c_t[pl.ds(pl.multiple_of(i * half, half), half), :] = packed.astype(BF16)
        loop(rows, one)
        g_c[c, me] = dot(p5[...], c_t[...]).astype(BF16)
        gather_start(g_c, 1, c)
        for db in range(n // 4):
            part = y1[:, 16 * db:16 * (db + 1), :].reshape(16 * rows, width)
            s2[c, sup * db:sup * (db + 1), :] = dot(p3t[...], part).astype(BF16)
        exchange_start(s2, r2, 1, c, False)
    loop(crops, columns)

    def bias_send(buf, e, c):
        buf[c, me] = dot(p6[0:blk, :], tmp_b[...].astype(BF16)).astype(BF16)
        gather_start(buf, e, c)

    def outer(c):
        gather_forward(g_c, 1, c)
        gather_wait(g_c, 1, c)

        def unpack(q):
            for sb in range(n // 4):
                part = g_c[c, 4 * sb:4 * sb + 4, pl.ds(pl.multiple_of(blk * q, 16), blk), :].reshape(sup, 128)
                moved = dot(p4[...], part).astype(BF16)
                for i in range(4):
                    c_f[4 * q + i, blk * sb:blk * (sb + 1), :] = moved[blk * i:blk * (i + 1), :]
        loop(HD // 2 // 4, unpack)

        def products(fp):
            for half in range(2):
                u = dot_nt(a_t[c, half], c_f[fp])
                for i in range(rows):
                    at = pl.ds(pl.multiple_of(fp * 2 * HD + half * HD, HD), HD)
                    u_s[i, at, :] = (u[HD * i:HD * (i + 1), :] * rn[c, i:i + 1, :]).astype(BF16)
        loop(HD // 2, products)

        def one(i):
            update = dot_tn(u_s[i], w_fe[...])
            z = (z_ref[c, i].astype(F32) + update).astype(BF16)
            z1[c, i] = z
            y = layer_norm(z)
            yn[c, i] = y
            tmp_b[pl.ds(pl.multiple_of(i * 8, 8), 4), :] = dot_nt(w_tsb[...], y)
        loop(rows, one)
        bias_send(g_t1, 2, c)
    loop(crops, outer)

    def triangle(buf, e, c, perm, pieces, piece, select, w_t, w_out):
        gather_forward(buf, e, c)
        gather_wait(buf, e, c)
        unpack_bias(buf, c, 0, perm, 0, pieces, piece)
        col = mask_columns(rm_ref[c], select)
        col3 = jnp.concatenate([col] * (2 * length // 128), axis=1)
        for pair in range(2):
            at = 2 * length * pair
            bm_tri[:, at:at + 2 * length] = dot_nt(eye[...], b_q[at:at + 2 * length, :]) * LOG2E + col3

        def one(i):
            update = pair_attention(yn[c, i], w_t, w_out,
                                    lambda pair: bm_tri[:, 2 * length * pair:2 * length * (pair + 1)])
            x3[i] = (z1[c, i].astype(F32) + update).astype(BF16)
        loop(rows, one)

    def start_node(c):
        triangle(g_t1, 2, c, p4, 4, blk, eye, w_ts, w_tso)
        for q in range(quads):
            for b in range(blocks):
                part = x3[4 * q:4 * q + 4, 64 * b:64 * (b + 1), :].reshape(256, 128)
                s3[c, q, 256 * b:256 * (b + 1), :] = dot(p2[...], part).astype(BF16)
        exchange_start(s3, r3, 2, c, True)
    loop(crops, start_node)

    def transposed(c):
        exchange_wait(r3, 2, c, True)
        for q in range(quads):
            for sb in range(n // 4):
                moved = dot(p3[...], r3[c, q, sup * sb:sup * (sb + 1), :]).astype(BF16)
                for i in range(rows):
                    at = 64 * q + 16 * sb
                    z1[c, i, at:at + 16, :] = moved[16 * i:16 * (i + 1), :]

        def one(i):
            y = layer_norm(z1[c, i])
            yn[c, i] = y
            tmp_b[pl.ds(pl.multiple_of(i * 8, 8), 4), :] = dot_nt(w_teb[...], y)
        loop(rows, one)
        bias_send(g_t2, 3, c)
    loop(crops, transposed)

    def end_node(c):
        triangle(g_t2, 3, c, p4e, 4 * quads, 16, tok, w_te, w_teo)
        for q in range(quads):
            for db in range(n // 4):
                part = x3[:, 64 * q + 16 * db:64 * q + 16 * (db + 1), :].reshape(16 * rows, 128)
                s4[c, q, sup * db:sup * (db + 1), :] = dot(p3t[...], part).astype(BF16)
        exchange_start(s4, r4, 3, c, True)
    loop(crops, end_node)

    def finish(c):
        exchange_wait(r2, 1, c, False)
        for b in range(blocks):
            moved = dot(p2t[...], r2[c, 256 * b:256 * (b + 1), :]).astype(BF16)
            for i in range(seqs):
                out_m[c, i, 64 * b:64 * (b + 1), :] = moved[64 * i:64 * (i + 1), :]
        exchange_wait(r4, 3, c, True)
        for q in range(quads):
            for b in range(blocks):
                moved = dot(p2t[...], r4[c, q, 256 * b:256 * (b + 1), :]).astype(BF16)
                for i in range(4):
                    out_z[c, 4 * q + i, 64 * b:64 * (b + 1), :] = moved[64 * i:64 * (i + 1), :]
    loop(crops, finish)

    def drain(c):
        for e, buf in enumerate((g_row, g_c, g_t1, g_t2)):
            gather_end(buf, e, c)
        for e, (buf, planes) in enumerate(((s1, False), (s2, False), (s3, True), (s4, True))):
            exchange_end(buf, e, c, planes)
    loop(crops, drain)


def solution(mesh):
    n = mesh.shape[GROUP_AXIS]
    rows_spec = P(PART_AXIS, GROUP_AXIS, None, None)
    in_specs = (rows_spec, rows_spec, P(PART_AXIS, None, None), P(PART_AXIS, None)) + (P(),) * N_WEIGHTS

    def local_block(msa, pair, msa_mask, res_mask, *weights):
        (w_rb, w_r, w_ro, w_c, w_co, w_ac, w_oo, w_tsb, w_ts, w_tso, w_teb, w_te, w_teo) = weights
        crops, seqs, length, width = msa.shape
        rows, pair_width = pair.shape[1], pair.shape[3]
        n_seq = msa_mask.shape[1]
        heads, tri_heads = w_r.shape[2], w_ts.shape[2]
        quads = rows // 4

        def flat_t(w):
            return jnp.transpose(w, (1, 2, 3, 0)).reshape(-1, w.shape[0])

        operands = [
            msa, pair, msa_mask, res_mask.reshape(crops, 1, length),
            w_rb.T, flat_t(w_r), w_ro.reshape(width, width), flat_t(w_c), w_co.reshape(width, width),
            jnp.transpose(w_ac, (1, 2, 0)).reshape(-1, width), w_oo.reshape(-1, pair_width),
            w_tsb.T, flat_t(w_ts), w_tso.reshape(pair_width, pair_width),
            w_teb.T, flat_t(w_te), w_teo.reshape(pair_width, pair_width),
        ]
        p2 = permutation((4, 64), (1, 0))
        p3 = permutation((4, rows, 4), (1, 0, 2))
        p4 = permutation((4, 4, rows), (1, 0, 2))
        p4e = permutation((4, 4, quads, 4), (1, 2, 0, 3))
        p5 = permutation((rows, HD // 2), (1, 0))
        p6 = permutation((rows, heads), (1, 0))
        tok = permutation((n, quads, 4), (1, 0, 2))
        consts = [p2, p2.T, p3, p3.T, p4, p4e, p5, p6, np.eye(length), tok]
        operands += [jnp.asarray(a, BF16) for a in consts]

        vmem = pl.BlockSpec(memory_space=pltpu.VMEM)
        total = n * 4 * rows
        scratch = [
            pltpu.VMEM((crops, n, heads * rows, length), BF16),
            pltpu.VMEM((crops, n, HD // 2 * rows, 128), BF16),
            pltpu.VMEM((crops, n, tri_heads * rows, length), BF16),
            pltpu.VMEM((crops, n, tri_heads * rows, length), BF16),
        ]
        scratch += [pltpu.VMEM((crops, total, width), BF16)] * 4
        scratch += [pltpu.VMEM((crops, quads, total, pair_width), BF16)] * 4
        scratch += [
            pltpu.VMEM((8 * rows, length), F32),
            pltpu.VMEM((heads * length, length), BF16),
            pltpu.VMEM((length, heads * length), F32),
            pltpu.VMEM((length, tri_heads * length), F32),
            pltpu.VMEM((seqs, length, width), BF16),
            pltpu.VMEM((rows, n_seq, width), BF16),
            pltpu.VMEM((16, 2 * n_seq), F32),
            pltpu.VMEM((crops, 16, length), F32),
            pltpu.VMEM((crops, 2, rows * HD, 128), BF16),
            pltpu.VMEM((rows * HD // 2, 128), BF16),
            pltpu.VMEM((HD // 2, length, 128), BF16),
            pltpu.VMEM((rows, HD * HD, length), BF16),
            pltpu.VMEM((HD * HD, pair_width), F32),
            pltpu.VMEM((HD * HD, pair_width), BF16),
            pltpu.VMEM((crops, rows, length, pair_width), BF16),
            pltpu.VMEM((crops, rows, length, pair_width), BF16),
            pltpu.VMEM((rows, length, pair_width), BF16),
        ]
        scratch += [pltpu.SemaphoreType.DMA((4, crops))] * 6
        return pl.pallas_call(
            functools.partial(block_kernel, n),
            out_shape=(jax.ShapeDtypeStruct(msa.shape, BF16), jax.ShapeDtypeStruct(pair.shape, BF16)),
            in_specs=[vmem] * len(operands),
            out_specs=(vmem, vmem),
            scratch_shapes=scratch,
            compiler_params=pltpu.CompilerParams(collective_id=0, has_side_effects=True, vmem_limit_bytes=VMEM_BYTES),
            name='evoformer_block',
        )(*operands)

    return jax.shard_map(local_block, mesh=mesh, in_specs=in_specs, out_specs=(rows_spec, rows_spec),
                         check_vma=False)
```

```python
import functools
import math

import jax
import jax.numpy as jnp
import numpy as np
from jax import lax
from jax.experimental import pallas as pl
from jax.experimental.pallas import tpu as pltpu
from jax.sharding import PartitionSpec as P

MASK_SCALE = 10000.0
LN_EPS = 1e-5
OPM_EPS = 1e-3
LOG2E = math.log2(math.e)
N_WEIGHTS = 13
PART_AXIS = 'data'
GROUP_AXIS = 'dap'
MESH = pl.DeviceIdType.MESH
F32 = jnp.float32
BF16 = jnp.bfloat16
HD = 32
U_LN, U_UNP, U_PROD, U_OUT = 12, 2, 4, 3
U_PR, U_PO, U_TP, U_TA, U_CP, U_CM, U_CA, U_CF = 2, 4, 3, 4, 1, 1, 3, 3
VMEM_BYTES = 60 * 1024 * 1024


def dot(a, b):
    return lax.dot_general(a, b, (((1,), (0,)), ((), ())), preferred_element_type=F32)


def dot_nt(a, b):
    return lax.dot_general(a, b, (((1,), (1,)), ((), ())), preferred_element_type=F32)


def dot_tn(a, b):
    return lax.dot_general(a, b, (((0,), (0,)), ((), ())), preferred_element_type=F32)


def layer_norm(x):
    x_float = x.astype(F32)
    centred = x_float - jnp.mean(x_float, axis=-1, keepdims=True)
    var = jnp.mean(centred * centred, axis=-1, keepdims=True)
    return (centred * lax.rsqrt(var + LN_EPS)).astype(BF16)


def seg(i, size):
    return slice(i * size, (i + 1) * size)


def sigmoid(x):
    return 1.0 / (1.0 + jnp.exp2(x * (-LOG2E)))


def iota(shape, dim):
    return lax.broadcasted_iota(jnp.int32, shape, dim)


def permutation(sizes, order, keep=None):
    total = int(np.prod(sizes))
    source = np.arange(total).reshape(sizes).transpose(order).reshape(-1)
    out = np.zeros((total, total), np.float32)
    out[np.arange(total), source] = 1.0
    return out


def softmax_cols(t):
    e = jnp.exp2(t - jnp.max(t, axis=0, keepdims=True))
    return (e * (1.0 / jnp.sum(e, axis=0, keepdims=True))).astype(BF16)


def same_half(width, lanes, half):
    return (iota((width, lanes), 0) // HD) % 2 == (iota((width, lanes), 1) // half) % 2


def block_kernel(n, x_ref, z_ref, mm_ref, rm_ref,
                 w_rb, w_r, w_ro, w_c, w_co, w_ac, w_oo, w_tsb, w_ts, w_tso, w_teb, w_te, w_teo,
                 p2, p2t, p3, p3t, p4, p4e, p5, p6, eye, tok,
                 out_m, out_z,
                 g_row, g_c, g_t1, g_t2, s1, r1, s2, r2, s3, r3, s4, r4,
                 tmp_b, b_q, bm_row, bm_tri, x1, y1, m_t, rn, a_t, c_t, c_f, u_s, w_f32, w_fe, w_fet, z1, yn, x3,
                 q_s, k_s, v_s, g_s, o_s, s_buf, m_s, qc_s, kc_s, vc_s, gc_s, oc_s, mc_s,
                 gs_a, gr_a, gs_b, gr_b, as_sem, ar_sem):
    me = lax.axis_index(GROUP_AXIS)
    chips = n // 2
    chip = me // 2
    core = me % 2
    partner = me + 1 - 2 * core
    crops, seqs, length, width = x_ref.shape
    rows = z_ref.shape[1]
    quads = rows // 4
    blocks = length // 64
    blk = 4 * rows
    sup = 4 * blk
    steps = []
    for k in range(1, chips // 2 + 1):
        steps.append(k)
        if chips - k != k:
            steps.append(chips - k)

    barrier = pltpu.get_barrier_semaphore()
    for k in range(1, n):
        pl.semaphore_signal(barrier, inc=1, device_id={GROUP_AXIS: lax.rem(me + k, n)}, device_id_type=MESH)
    pl.semaphore_wait(barrier, n - 1)

    def remote(src, dst, send, recv, device):
        return pltpu.make_async_remote_copy(src_ref=src, dst_ref=dst, send_sem=send, recv_sem=recv,
                                            device_id={GROUP_AXIS: device}, device_id_type=MESH)

    def same_core(k):
        return 2 * lax.rem(chip + k, chips) + core

    def gather_start(buf, e, c):
        mine = buf.at[c, me]
        for k in steps:
            remote(mine, mine, gs_a.at[e, c], gr_a.at[e, c], same_core(k)).start()
        remote(mine, mine, gs_b.at[e, c], gr_b.at[e, c], partner).start()

    def wait_bytes(ref, sem):
        pltpu.make_async_copy(ref, ref, sem).wait()

    def gather_forward(buf, e, c):
        wait_bytes(buf.at[c, pl.ds(0, chips - 1)], gr_a.at[e, c])
        for k in steps:
            block = buf.at[c, same_core(k)]
            remote(block, block, gs_b.at[e, c], gr_b.at[e, c], partner).start()

    def gather_wait(buf, e, c):
        wait_bytes(buf.at[c, pl.ds(0, chips)], gr_b.at[e, c])

    def gather_end(buf, e, c):
        wait_bytes(buf.at[c, pl.ds(0, chips - 1)], gs_a.at[e, c])
        wait_bytes(buf.at[c, pl.ds(0, chips)], gs_b.at[e, c])

    def block_of(ref, c, d, planes):
        where = pl.ds(pl.multiple_of(d * blk, 16), blk)
        return ref.at[c, :, where, :] if planes else ref.at[c, where, :]

    def exchange_start(src, dst, e, c, planes):
        here = pl.ds(pl.multiple_of(me * blk, 16), blk)
        if planes:
            dst[c, :, here, :] = src[c, :, here, :]
        else:
            dst[c, here, :] = src[c, here, :]
        landing = block_of(dst, c, me, planes)
        for k in steps:
            for other in range(2):
                d = 2 * lax.rem(chip + k, chips) + (core + other) % 2
                remote(block_of(src, c, d, planes), landing, as_sem.at[e, c], ar_sem.at[e, c], d).start()
        remote(block_of(src, c, partner, planes), landing, as_sem.at[e, c], ar_sem.at[e, c], partner).start()

    def others(ref, c, planes):
        where = pl.ds(0, (n - 1) * blk)
        return ref.at[c, :, where, :] if planes else ref.at[c, where, :]

    def exchange_wait(dst, e, c, planes):
        wait_bytes(others(dst, c, planes), ar_sem.at[e, c])

    def exchange_end(src, e, c, planes):
        wait_bytes(others(src, c, planes), as_sem.at[e, c])

    def loop(count, body, unroll=1):
        def several(i, carry):
            for k in range(unroll):
                body(i * unroll + k)
            return carry
        lax.fori_loop(0, count // unroll, several, 0)

    tmp_b[:] = jnp.zeros_like(tmp_b)

    def row_bias(c):
        def one(i):
            tmp_b[pl.ds(pl.multiple_of(i * 8, 8), 8), :] = dot_nt(w_rb[:], layer_norm(z_ref[c, i]))
        loop(rows, one, U_LN)
        g_row[c, me] = dot(p6[:], tmp_b[:].astype(BF16)).astype(BF16)
        gather_start(g_row, 0, c)
    loop(crops, row_bias)

    w_f32[:] = w_oo[:].astype(F32)
    for fp in range(HD // 2):
        for half in range(2):
            at = fp * 2 * HD + half * HD
            w_fe[at:at + HD, :] = w_f32[pl.ds(half * (HD // 2) + fp, HD, stride=HD), :]
    for b in range(HD * HD // 128):
        w_fet[:, seg(b, 128)] = w_fe[seg(b, 128), :].T.astype(BF16)
    q_s[:] = jnp.zeros_like(q_s)

    def unpack_bias(buf, c, group, perm, first, pieces, piece):
        for sb in range(n // 4):
            part = buf[c, 4 * sb:4 * sb + 4, seg(group, blk), :]
            moved = dot(perm[:], part.reshape(sup, length)).astype(BF16)
            for i in range(pieces):
                at = first + i * (length * 4 // pieces) + sb * piece
                b_q[at:at + piece, :] = moved[i * piece:(i + 1) * piece, :]

    def mask_columns(row, select):
        wide = jnp.broadcast_to(row.astype(F32), (128, length)).astype(BF16)
        return (dot_nt(select[:], wide) - 1.0) * (MASK_SCALE * LOG2E)

    scale = HD ** -0.5 * LOG2E
    two, four = 2 * length, 4 * length

    def project(y, w_t, first):
        wide = y.shape[1]
        q = dot_nt(w_t[0:wide, :], jnp.concatenate([y, y], axis=0))
        q = jnp.where(same_half(wide, two, length), q, 0.0).astype(BF16)
        keys = dot_nt(y, w_t[wide:2 * wide, :]).astype(BF16)
        values = dot_nt(w_t[2 * wide:3 * wide, :], y).astype(BF16)
        gate = sigmoid(dot_nt(w_t[3 * wide:4 * wide, :], y))
        for g in range(wide // 128):
            u = first + g
            q_s[u, 0:64, 0:two] = q[128 * g:128 * g + 64, :]
            q_s[u, 64:128, two:four] = q[128 * g + 64:128 * g + 128, :]
            k_s[u] = keys[:, seg(g, 128)]
            v_s[u] = values[seg(g, 128), :]
            g_s[u] = gate[seg(g, 128), :]

    def attend(count, bias_of):
        def mix(u, probs):
            pieces = []
            for p in range(2):
                mixed = dot(v_s[u, seg(p, 64), :], probs[:, seg(p, two)])
                pieces += [mixed[0:HD, 0:length], mixed[HD:2 * HD, length:two]]
            return jnp.concatenate(pieces, axis=0)

        def finish(u, mixed):
            o_s[u] = (g_s[u] * mixed).astype(BF16)

        s_buf[0] = dot(k_s[0], q_s[0])

        def pair(i):
            u = 2 * i
            s_buf[1] = dot(k_s[u + 1], q_s[u + 1])
            mixed = mix(u, softmax_cols(s_buf[0] * scale + bias_of(u)))
            after = jnp.minimum(u + 2, count - 1)
            s_buf[0] = dot(k_s[after], q_s[after])
            probs = softmax_cols(s_buf[1] * scale + bias_of(u + 1))
            finish(u, mixed)
            finish(u + 1, mix(u + 1, probs))
        loop(count // 2, pair)

    groups = width // 128

    def row_attention(c):
        gather_forward(g_row, 0, c)
        gather_wait(g_row, 0, c)
        for group in range(groups):
            unpack_bias(g_row, c, group, p4, group * four, 4, blk)
        for pair in range(2 * groups):
            bm_row[pair // 2, :, two * (pair % 2):two * (pair % 2 + 1)] = \
                dot_nt(eye[:], b_q[seg(pair, two), :]) * LOG2E

        def before(s):
            m_s[s] = mask_columns(mm_ref[c, pl.ds(me * seqs + s, 1), :], eye)
            project(layer_norm(x_ref[c, s]), w_r, s * groups)
        loop(seqs, before, U_PR)

        def bias_of(u):
            return bm_row[u % groups] + jnp.concatenate([m_s[u // groups]] * (four // 128), axis=1)
        attend(seqs * groups, bias_of)

        def after(s):
            gated = jnp.concatenate([o_s[s * groups + g] for g in range(groups)], axis=0)
            x1[s] = (x_ref[c, s].astype(F32) + dot_tn(gated, w_ro[:])).astype(BF16)
        loop(seqs, after, U_PO)
        for b in range(blocks):
            part = x1[:, seg(b, 64), :].reshape(256, width)
            s1[c, seg(b, 256), :] = dot(p2[:], part).astype(BF16)
        exchange_start(s1, r1, 0, c, False)
    loop(crops, row_attention)

    def columns(c):
        exchange_wait(r1, 0, c, False)
        for sb in range(n // 4):
            moved = dot(p3[:], r1[c, seg(sb, sup), :]).astype(BF16)
            for i in range(rows):
                y1[i, seg(sb, 16), :] = moved[seg(i, 16), :]
        n_seq = y1.shape[1]
        mk = mm_ref[c].astype(F32).astype(BF16)
        mine = (iota((16, length), 1) == me * rows + iota((16, length), 0)).astype(F32).astype(BF16)
        m_t[:] = dot_nt(mine, jnp.concatenate([mk, mk], axis=0))
        rn[c] = 1.0 / (dot(m_t[:, 0:n_seq].astype(BF16), mk) + OPM_EPS)
        low = iota((HD, 2 * n_seq), 1) < n_seq
        picks = (iota((128 * rows, length), 1) == me * rows + iota((128 * rows, length), 0) // 128)
        mask_all = (dot_nt(mk, picks.astype(F32).astype(BF16)) - 1.0) * (MASK_SCALE * LOG2E)
        for i in range(rows):
            mc_s[i] = mask_all[:, seg(i, 128)]
        tokens = 4 * n_seq

        def doubled(y):
            return jnp.concatenate([y[n_seq * (r // 2):n_seq * (r // 2 + 1), :] for r in range(8)], axis=0)

        def before(q):
            y = layer_norm(y1[pl.ds(4 * q, 4)].reshape(tokens, width))
            qq = dot_nt(w_c[0:width, :], doubled(y))
            qc_s[q] = jnp.where(same_half(width, 2 * tokens, n_seq), qq, 0.0).astype(BF16)
            kc_s[q] = dot_nt(y, w_c[width:2 * width, :]).astype(BF16)
            vc_s[q] = dot_nt(y, w_c[2 * width:3 * width, :]).astype(BF16)
            gc_s[q] = sigmoid(dot_nt(w_c[3 * width:4 * width, :], y))
        loop(quads, before, U_CP)

        def middle(q):
            zeros = jnp.zeros((64, 128), BF16)
            for g in range(groups):
                heads = [[] for _ in range(4)]
                for r in range(4):
                    at = n_seq * r
                    wide = qc_s[q, seg(g, 128), seg(r, 128)]
                    stacked = jnp.concatenate([jnp.concatenate([wide[0:64], zeros], axis=0),
                                               jnp.concatenate([zeros, wide[64:128]], axis=0)], axis=1)
                    logits = dot(kc_s[q, at:at + n_seq, seg(g, 128)], stacked)
                    col = mc_s[4 * q + r]
                    probs = softmax_cols(logits * scale + jnp.concatenate([col, col], axis=1))
                    mixed = dot_tn(vc_s[q, at:at + n_seq, seg(g, 128)], probs)
                    for h in range(4):
                        heads[h].append(mixed[seg(h, HD), seg(h, n_seq)])
                mixed = jnp.concatenate([jnp.concatenate(h, axis=1) for h in heads], axis=0)
                oc_s[q, seg(g, 128), :] = (gc_s[q, seg(g, 128), :] * mixed).astype(BF16)
        loop(quads, middle, U_CM)

        def after(q):
            update = dot_tn(oc_s[q], w_co[:])
            x = y1[pl.ds(4 * q, 4)].reshape(tokens, width).astype(F32)
            y1[pl.ds(4 * q, 4)] = (x + update).astype(BF16).reshape(4, n_seq, width)
        loop(quads, after, U_CA)

        def factors(q):
            y = layer_norm(y1[pl.ds(4 * q, 4)].reshape(tokens, width))
            all_four = dot_nt(w_ac[:], doubled(y)).astype(BF16).astype(F32)
            half = HD // 2
            for r in range(4):
                i = 4 * q + r
                both = all_four[:, seg(r, 128)] * m_t[pl.ds(i, 1), :]
                a = both[0:HD, :]
                at = pl.ds(pl.multiple_of(i * HD, HD), HD)
                a_t[c, 0, at, :] = jnp.where(low, a, 0.0).astype(BF16)
                a_t[c, 1, at, :] = jnp.where(low, 0.0, a).astype(BF16)
                packed = jnp.where(low[0:half], both[HD:HD + half, :], both[HD + half:2 * HD, :])
                c_t[pl.ds(pl.multiple_of(i * half, half), half), :] = packed.astype(BF16)
        loop(quads, factors, U_CF)
        g_c[c, me] = dot(p5[:], c_t[:]).astype(BF16)
        gather_start(g_c, 1, c)
        for db in range(n // 4):
            part = y1[:, seg(db, 16), :].reshape(16 * rows, width)
            s2[c, seg(db, sup), :] = dot(p3t[:], part).astype(BF16)
        exchange_start(s2, r2, 1, c, False)
    loop(crops, columns)

    def bias_send(buf, e, c, w_b):
        def one(i):
            y = layer_norm(z1[c, i])
            yn[c, i] = y
            tmp_b[pl.ds(pl.multiple_of(i * 8, 8), 4), :] = dot_nt(w_b[:], y)
        loop(rows, one, U_LN)
        buf[c, me] = dot(p6[0:blk, :], tmp_b[:].astype(BF16)).astype(BF16)
        gather_start(buf, e, c)

    def outer(c):
        gather_forward(g_c, 1, c)
        gather_wait(g_c, 1, c)

        def unpack(q):
            for sb in range(n // 4):
                part = g_c[c, 4 * sb:4 * sb + 4, pl.ds(pl.multiple_of(blk * q, 16), blk), :].reshape(sup, 128)
                moved = dot(p4[:], part).astype(BF16)
                for i in range(4):
                    c_f[4 * q + i, seg(sb, blk), :] = moved[seg(i, blk), :]
        loop(HD // 2 // 4, unpack, U_UNP)

        def products(fp):
            for half in range(2):
                u = dot_nt(a_t[c, half], c_f[fp])
                for i in range(rows):
                    at = pl.ds(pl.multiple_of(fp * 2 * HD + half * HD, HD), HD)
                    u_s[i, at, :] = (u[seg(i, HD), :] * rn[c, i:i + 1, :]).astype(BF16)
        loop(HD // 2, products, U_PROD)

        def one(i):
            update = dot(w_fet[:], u_s[i])
            z1[c, i] = (z_ref[c, i].astype(F32) + update.T).astype(BF16)
        loop(rows, one, U_OUT)
        bias_send(g_t1, 2, c, w_tsb)
    loop(crops, outer)

    def triangle(buf, e, c, perm, pieces, piece, select, w_t, w_out):
        gather_forward(buf, e, c)
        gather_wait(buf, e, c)
        unpack_bias(buf, c, 0, perm, 0, pieces, piece)
        col = mask_columns(rm_ref[c], select)
        col3 = jnp.concatenate([col] * (2 * length // 128), axis=1)
        for pair in range(2):
            at = two * pair
            bm_tri[:, at:at + two] = dot_nt(eye[:], b_q[at:at + two, :]) * LOG2E + col3
        loop(rows, lambda i: project(yn[c, i], w_t, i), U_TP)
        attend(rows, lambda u: bm_tri[:])

        def after(i):
            x3[i] = (z1[c, i].astype(F32) + dot_tn(o_s[i], w_out[:])).astype(BF16)
        loop(rows, after, U_TA)

    def start_node(c):
        triangle(g_t1, 2, c, p4, 4, blk, eye, w_ts, w_tso)
        for q in range(quads):
            for b in range(blocks):
                part = x3[4 * q:4 * q + 4, seg(b, 64), :].reshape(256, 128)
                s3[c, q, seg(b, 256), :] = dot(p2[:], part).astype(BF16)
        exchange_start(s3, r3, 2, c, True)
    loop(crops, start_node)

    def transposed(c):
        exchange_wait(r3, 2, c, True)
        for q in range(quads):
            for sb in range(n // 4):
                moved = dot(p3[:], r3[c, q, seg(sb, sup), :]).astype(BF16)
                for i in range(rows):
                    at = 64 * q + 16 * sb
                    z1[c, i, at:at + 16, :] = moved[seg(i, 16), :]

        bias_send(g_t2, 3, c, w_teb)
    loop(crops, transposed)

    def end_node(c):
        triangle(g_t2, 3, c, p4e, 4 * quads, 16, tok, w_te, w_teo)
        for q in range(quads):
            for db in range(n // 4):
                part = x3[:, 64 * q + 16 * db:64 * q + 16 * (db + 1), :].reshape(16 * rows, 128)
                s4[c, q, seg(db, sup), :] = dot(p3t[:], part).astype(BF16)
        exchange_start(s4, r4, 3, c, True)
    loop(crops, end_node)

    def finish(c):
        exchange_wait(r2, 1, c, False)
        for b in range(blocks):
            moved = dot(p2t[:], r2[c, seg(b, 256), :]).astype(BF16)
            for i in range(seqs):
                out_m[c, i, seg(b, 64), :] = moved[seg(i, 64), :]
        exchange_wait(r4, 3, c, True)
        for q in range(quads):
            for b in range(blocks):
                moved = dot(p2t[:], r4[c, q, seg(b, 256), :]).astype(BF16)
                for i in range(4):
                    out_z[c, 4 * q + i, seg(b, 64), :] = moved[seg(i, 64), :]
    loop(crops, finish)

    def drain(c):
        for e, buf in enumerate((g_row, g_c, g_t1, g_t2)):
            gather_end(buf, e, c)
        for e, (buf, planes) in enumerate(((s1, False), (s2, False), (s3, True), (s4, True))):
            exchange_end(buf, e, c, planes)
    loop(crops, drain)


def solution(mesh):
    n = mesh.shape[GROUP_AXIS]
    rows_spec = P(PART_AXIS, GROUP_AXIS, None, None)
    in_specs = (rows_spec, rows_spec, P(PART_AXIS, None, None), P(PART_AXIS, None)) + (P(),) * N_WEIGHTS

    def local_block(msa, pair, msa_mask, res_mask, *weights):
        (w_rb, w_r, w_ro, w_c, w_co, w_ac, w_oo, w_tsb, w_ts, w_tso, w_teb, w_te, w_teo) = weights
        crops, seqs, length, width = msa.shape
        rows, pair_width = pair.shape[1], pair.shape[3]
        n_seq = msa_mask.shape[1]
        heads, tri_heads = w_r.shape[2], w_ts.shape[2]
        quads = rows // 4

        def flat_t(w):
            return jnp.transpose(w, (1, 2, 3, 0)).reshape(-1, w.shape[0])

        operands = [
            msa, pair, msa_mask, res_mask.reshape(crops, 1, length),
            w_rb.T, flat_t(w_r), w_ro.reshape(width, width), flat_t(w_c), w_co.reshape(width, width),
            jnp.transpose(w_ac, (1, 2, 0)).reshape(-1, width), w_oo.reshape(-1, pair_width),
            w_tsb.T, flat_t(w_ts), w_tso.reshape(pair_width, pair_width),
            w_teb.T, flat_t(w_te), w_teo.reshape(pair_width, pair_width),
        ]
        p2 = permutation((4, 64), (1, 0))
        p3 = permutation((4, rows, 4), (1, 0, 2))
        p4 = permutation((4, 4, rows), (1, 0, 2))
        p4e = permutation((4, 4, quads, 4), (1, 2, 0, 3))
        p5 = permutation((rows, HD // 2), (1, 0))
        p6 = permutation((rows, heads), (1, 0))
        tok = permutation((n, quads, 4), (1, 0, 2))
        consts = [p2, p2.T, p3, p3.T, p4, p4e, p5, p6, np.eye(length), tok]
        operands += [jnp.asarray(a, BF16) for a in consts]

        vmem = pl.BlockSpec(memory_space=pltpu.VMEM)
        total = n * 4 * rows
        scratch = [
            pltpu.VMEM((crops, n, heads * rows, length), BF16),
            pltpu.VMEM((crops, n, HD // 2 * rows, 128), BF16),
            pltpu.VMEM((crops, n, tri_heads * rows, length), BF16),
            pltpu.VMEM((crops, n, tri_heads * rows, length), BF16),
        ]
        scratch += [pltpu.VMEM((crops, total, width), BF16)] * 4
        scratch += [pltpu.VMEM((crops, quads, total, pair_width), BF16)] * 4
        scratch += [
            pltpu.VMEM((8 * rows, length), F32),
            pltpu.VMEM((heads * length, length), BF16),
            pltpu.VMEM((width // 128, length, 4 * length), F32),
            pltpu.VMEM((length, tri_heads * length), F32),
            pltpu.VMEM((seqs, length, width), BF16),
            pltpu.VMEM((rows, n_seq, width), BF16),
            pltpu.VMEM((16, 2 * n_seq), F32),
            pltpu.VMEM((crops, 16, length), F32),
            pltpu.VMEM((crops, 2, rows * HD, 128), BF16),
            pltpu.VMEM((rows * HD // 2, 128), BF16),
            pltpu.VMEM((HD // 2, length, 128), BF16),
            pltpu.VMEM((rows, HD * HD, length), BF16),
            pltpu.VMEM((HD * HD, pair_width), F32),
            pltpu.VMEM((HD * HD, pair_width), F32),
            pltpu.VMEM((pair_width, HD * HD), BF16),
            pltpu.VMEM((crops, rows, length, pair_width), BF16),
            pltpu.VMEM((crops, rows, length, pair_width), BF16),
            pltpu.VMEM((rows, length, pair_width), BF16),
            pltpu.VMEM((rows, 128, 4 * length), BF16),
            pltpu.VMEM((rows, length, 128), BF16),
            pltpu.VMEM((rows, 128, length), BF16),
            pltpu.VMEM((rows, 128, length), F32),
            pltpu.VMEM((rows, 128, length), BF16),
            pltpu.VMEM((2, length, 4 * length), F32),
            pltpu.VMEM((seqs, length, 128), F32),
            pltpu.VMEM((quads, width, 8 * n_seq), BF16),
            pltpu.VMEM((quads, 4 * n_seq, width), BF16),
            pltpu.VMEM((quads, 4 * n_seq, width), BF16),
            pltpu.VMEM((quads, width, 4 * n_seq), F32),
            pltpu.VMEM((quads, width, 4 * n_seq), BF16),
            pltpu.VMEM((rows, n_seq, 128), F32),
        ]
        scratch += [pltpu.SemaphoreType.DMA((4, crops))] * 6
        return pl.pallas_call(
            functools.partial(block_kernel, n),
            out_shape=(jax.ShapeDtypeStruct(msa.shape, BF16), jax.ShapeDtypeStruct(pair.shape, BF16)),
            in_specs=[vmem] * len(operands),
            out_specs=(vmem, vmem),
            scratch_shapes=scratch,
            compiler_params=pltpu.CompilerParams(collective_id=0, has_side_effects=True, vmem_limit_bytes=VMEM_BYTES),
            name='evoformer_block',
        )(*operands)

    return jax.shard_map(local_block, mesh=mesh, in_specs=in_specs, out_specs=(rows_spec, rows_spec),
                         check_vma=False)
```

```python
import functools
import math

import jax
import jax.numpy as jnp
import numpy as np
from jax import lax
from jax.experimental import pallas as pl
from jax.experimental.pallas import tpu as pltpu
from jax.sharding import PartitionSpec as P

MASK_SCALE = 10000.0
LN_EPS = 1e-5
OPM_EPS = 1e-3
LOG2E = math.log2(math.e)
N_WEIGHTS = 13
PART_AXIS = 'data'
GROUP_AXIS = 'dap'
MESH = pl.DeviceIdType.MESH
F32 = jnp.float32
BF16 = jnp.bfloat16
HD = 32
U_LN, U_UNP, U_PROD, U_OUT = 12, 2, 4, 3
U_PR, U_PO, U_TP, U_TA, U_CP, U_CM, U_CA, U_CF = 2, 4, 3, 4, 1, 1, 3, 3
VMEM_BYTES = 60 * 1024 * 1024


def dot(a, b):
    return lax.dot_general(a, b, (((1,), (0,)), ((), ())), preferred_element_type=F32)


def dot_nt(a, b):
    return lax.dot_general(a, b, (((1,), (1,)), ((), ())), preferred_element_type=F32)


def dot_tn(a, b):
    return lax.dot_general(a, b, (((0,), (0,)), ((), ())), preferred_element_type=F32)


def layer_norm(x):
    x_float = x.astype(F32)
    centred = x_float - jnp.mean(x_float, axis=-1, keepdims=True)
    var = jnp.mean(centred * centred, axis=-1, keepdims=True)
    return (centred * lax.rsqrt(var + LN_EPS)).astype(BF16)


def seg(i, size):
    return slice(i * size, (i + 1) * size)


def sigmoid(x):
    return 1.0 / (1.0 + jnp.exp2(x * (-LOG2E)))


def iota(shape, dim):
    return lax.broadcasted_iota(jnp.int32, shape, dim)


def permutation(sizes, order, keep=None):
    total = int(np.prod(sizes))
    source = np.arange(total).reshape(sizes).transpose(order).reshape(-1)
    out = np.zeros((total, total), np.float32)
    out[np.arange(total), source] = 1.0
    return out


def softmax_cols(t):
    e = jnp.exp2(t - jnp.max(t, axis=0, keepdims=True))
    return (e * (1.0 / jnp.sum(e, axis=0, keepdims=True))).astype(BF16)


def same_half(width, lanes, half):
    return (iota((width, lanes), 0) // HD) % 2 == (iota((width, lanes), 1) // half) % 2


def block_kernel(n, x_ref, z_ref, mm_ref, rm_ref,
                 w_rb, w_r, w_ro, w_c, w_co, w_ac, w_oo, w_tsb, w_ts, w_tso, w_teb, w_te, w_teo,
                 p2, p2t, p3, p3t, p4, p4e, p5, p6, p64, eye, tok, tok_l, tok_r,
                 out_m, out_z,
                 g_row, g_c, g_t1, g_t2, s1, r1, s2, r2, s3, r3, s4, r4,
                 tmp_b, b_q, bm_row, bm_tri, x1, y1, m_t, rn, a_t, c_t, c_f, u_s, w_f32, w_fe, w_fet, z1, yn, x3,
                 q_s, k_s, v_s, g_s, o_s, s_buf, m_s, qc_s, kc_s, vc_s, gc_s, oc_s, mc_s,
                 gs_a, gr_a, gs_b, gr_b, gs_f, gr_f, as_sem, ar_sem):
    me = lax.axis_index(GROUP_AXIS)
    chips = n // 2
    chip = me // 2
    core = me % 2
    partner = me + 1 - 2 * core
    crops, seqs, length, width = x_ref.shape
    rows = z_ref.shape[1]
    quads = rows // 4
    blocks = length // 64
    blk = 4 * rows
    sup = 4 * blk
    steps = []
    for k in range(1, chips // 2 + 1):
        steps.append(k)
        if chips - k != k:
            steps.append(chips - k)

    near = (1, chips - 1, 2, chips - 2)
    far = tuple(k for k in steps if k not in near)

    barrier = pltpu.get_barrier_semaphore()
    for k in range(1, n):
        pl.semaphore_signal(barrier, inc=1, device_id={GROUP_AXIS: lax.rem(me + k, n)}, device_id_type=MESH)
    def remote(src, dst, send, recv, device):
        return pltpu.make_async_remote_copy(src_ref=src, dst_ref=dst, send_sem=send, recv_sem=recv,
                                            device_id={GROUP_AXIS: device}, device_id_type=MESH)

    def same_core(k):
        return 2 * lax.rem(chip + k, chips) + core

    def wait_bytes(ref, sem):
        pltpu.make_async_copy(ref, ref, sem).wait()

    def to_partner(block, e, c):
        remote(block, block, gs_b.at[e, c], gr_b.at[e, c], partner).start()

    def gather_start(buf, e, c, hops):
        mine = buf.at[c, me]
        for k in hops:
            remote(mine, mine, gs_a.at[e, c], gr_a.at[e, c], same_core(k)).start()
        to_partner(mine, e, c)

    def gather_forward(buf, e, c, hops):
        wait_bytes(buf.at[c, pl.ds(0, len(hops))], gr_a.at[e, c])
        for k in hops:
            to_partner(buf.at[c, same_core(k)], e, c)

    def gather_relay(buf, e, c, hops):
        wait_bytes(buf.at[c, pl.ds(0, len(hops))], gr_a.at[e, c])
        height = buf.shape[2]
        cut = height // 2 // 16 * 16
        for sign, part in ((1, pl.ds(0, cut)), (-1, pl.ds(cut, height - cut))):
            source = same_core(chips - 2 * sign)
            block = buf.at[c, source]
            remote(block, block, gs_f.at[e, c], gr_f.at[e, c], same_core(chips + sign)).start()
            half = buf.at[c, source, part]
            remote(half, half, gs_f.at[e, c], gr_f.at[e, c], same_core(chips + 2 * sign)).start()
        for k in hops:
            to_partner(buf.at[c, same_core(k)], e, c)

    def relay_forward(buf, e, c):
        wait_bytes(buf.at[c, pl.ds(0, len(far))], gr_f.at[e, c])
        for k in far:
            to_partner(buf.at[c, same_core(k)], e, c)

    def gather_wait(buf, e, c):
        wait_bytes(buf.at[c, pl.ds(0, chips)], gr_b.at[e, c])

    def gather_end(buf, e, c, hops):
        wait_bytes(buf.at[c, pl.ds(0, len(hops))], gs_a.at[e, c])
        wait_bytes(buf.at[c, pl.ds(0, chips)], gs_b.at[e, c])
        if hops is near:
            wait_bytes(buf.at[c, pl.ds(0, len(far))], gs_f.at[e, c])

    def rows_of(d, offset=0, height=None):
        return pl.ds(pl.multiple_of(d * blk + offset, 16), height or blk)

    def exchange_own(src, dst, index_of):
        dst[index_of(me)] = src[index_of(me)]

    def exchange_part(src, dst, e, c, index_of, hops):
        landing = dst.at[index_of(me)]
        for k in hops:
            for other in range(2):
                d = 2 * lax.rem(chip + k, chips) + (core + other) % 2
                if k or other:
                    remote(src.at[index_of(d)], landing, as_sem.at[e, c], ar_sem.at[e, c], d).start()

    def exchange_start(src, dst, e, c, index_of):
        exchange_own(src, dst, index_of)
        exchange_part(src, dst, e, c, index_of, steps + [0])

    def others(ref, c, planes):
        where = pl.ds(0, (n - 1) * blk)
        return ref.at[c, :, where, :] if planes else ref.at[c, where, :]

    def exchange_wait(dst, e, c, planes):
        wait_bytes(others(dst, c, planes), ar_sem.at[e, c])

    def exchange_end(src, e, c, planes):
        wait_bytes(others(src, c, planes), as_sem.at[e, c])

    def loop(count, body, unroll=1):
        def several(i, carry):
            for k in range(unroll):
                body(i * unroll + k)
            return carry
        lax.fori_loop(0, count // unroll, several, 0)

    tmp_b[:] = jnp.zeros_like(tmp_b)

    def row_bias(c):
        def one(i):
            tmp_b[pl.ds(pl.multiple_of(i * 8, 8), 8), :] = dot_nt(w_rb[:], layer_norm(z_ref[c, i]))
        loop(rows, one, U_LN)
        t = dot(p6[:], tmp_b[:].astype(BF16))
        height = t.shape[0]
        g_row[c, me, 0:height] = t[:, 0:128].astype(BF16)
        tail = jnp.concatenate([t[seg(g, blk), 128:length] for g in range(2)], axis=1)
        g_row[c, me, height:height + blk] = tail.astype(BF16)
    loop(crops, row_bias)
    pl.semaphore_wait(barrier, n - 1)
    loop(crops, lambda c: gather_start(g_row, 0, c, steps))

    w_f32[:] = w_oo[:].astype(F32)
    for fp in range(HD // 2):
        for half in range(2):
            at = fp * 2 * HD + half * HD
            w_fe[at:at + HD, :] = w_f32[pl.ds(half * (HD // 2) + fp, HD, stride=HD), :]
    for b in range(HD * HD // 128):
        w_fet[:, seg(b, 128)] = w_fe[seg(b, 128), :].T.astype(BF16)
    q_s[:] = jnp.zeros_like(q_s)

    def unpack_bias(buf, c, perm, pieces, piece):
        for sb in range(n // 4):
            moved = dot(perm[:], buf[c, seg(sb, 4)].reshape(sup, length)).astype(BF16)
            for i in range(pieces):
                at = i * (4 * length // pieces) + sb * piece
                b_q[at:at + piece, :] = moved[seg(i, piece), :]

    def mask_columns(row, select):
        wide = jnp.broadcast_to(row.astype(F32), (128, length)).astype(BF16)
        return (dot_nt(select[:], wide) - 1.0) * (MASK_SCALE * LOG2E)

    scale = HD ** -0.5 * LOG2E
    two, four = 2 * length, 4 * length

    def project(y, w_t, first):
        wide = y.shape[1]
        q = dot_nt(w_t[0:wide, :], jnp.concatenate([y, y], axis=0))
        q = jnp.where(same_half(wide, two, length), q, 0.0).astype(BF16)
        keys = dot_nt(y, w_t[wide:2 * wide, :]).astype(BF16)
        values = dot_nt(w_t[2 * wide:3 * wide, :], y).astype(BF16)
        gate = sigmoid(dot_nt(w_t[3 * wide:4 * wide, :], y))
        for g in range(wide // 128):
            u = first + g
            q_s[u, 0:64, 0:two] = q[128 * g:128 * g + 64, :]
            q_s[u, 64:128, two:four] = q[128 * g + 64:128 * g + 128, :]
            k_s[u] = keys[:, seg(g, 128)]
            v_s[u] = values[seg(g, 128), :]
            g_s[u] = gate[seg(g, 128), :]

    def attend(first, count, bias_of):
        def mix(u, probs):
            pieces = []
            for p in range(2):
                mixed = dot(v_s[u, seg(p, 64), :], probs[:, seg(p, two)])
                pieces += [mixed[0:HD, 0:length], mixed[HD:2 * HD, length:two]]
            return jnp.concatenate(pieces, axis=0)

        def finish(u, mixed):
            o_s[u] = (g_s[u] * mixed).astype(BF16)

        s_buf[0] = dot(k_s[first], q_s[first])

        def pair(i):
            u = first + 2 * i
            s_buf[1] = dot(k_s[u + 1], q_s[u + 1])
            mixed = mix(u, softmax_cols(s_buf[0] * scale + bias_of(u)))
            after = jnp.minimum(u + 2, first + count - 1)
            s_buf[0] = dot(k_s[after], q_s[after])
            probs = softmax_cols(s_buf[1] * scale + bias_of(u + 1))
            finish(u, mixed)
            finish(u + 1, mix(u + 1, probs))
        loop(count // 2, pair)

    groups = width // 128

    def row_attention(c):
        def before(s):
            m_s[s] = mask_columns(mm_ref[c, pl.ds(me * seqs + s, 1), :], eye)
            project(layer_norm(x_ref[c, s]), w_r, s * groups)
        loop(seqs, before, U_PR)

        @pl.when(c == 0)
        def _():
            gather_forward(g_row, 0, c, steps)
        gather_wait(g_row, 0, c)
        for sb in range(n // 4):
            for part in range(groups + 1):
                got = g_row[c, seg(sb, 4), seg(part, blk), :].reshape(sup, 128)
                moved = dot(p4[:], got).astype(BF16)
                for i in range(4):
                    piece = moved[seg(i, blk), :]
                    at = i * length + sb * blk
                    if part < groups:
                        b_q[part * four + at:part * four + at + blk, 0:128] = piece
                    else:
                        for g in range(groups):
                            b_q[g * four + at:g * four + at + blk, 128:length] = piece[:, seg(g, 64)]
        for pair in range(2 * groups):
            bm_row[pair // 2, :, two * (pair % 2):two * (pair % 2 + 1)] = \
                dot_nt(eye[:], b_q[seg(pair, two), :]) * LOG2E

        def bias_of(u):
            return bm_row[u % groups] + jnp.concatenate([m_s[u // groups]] * (four // 128), axis=1)
        attend(0, seqs * groups, bias_of)

        @pl.when(c == 0)
        def _():
            gather_forward(g_row, 0, 1, steps)

        def after(s):
            gated = jnp.concatenate([o_s[s * groups + g] for g in range(groups)], axis=0)
            x1[s] = (x_ref[c, s].astype(F32) + dot_tn(gated, w_ro[:])).astype(BF16)
        loop(seqs, after, U_PO)
        for b in range(blocks):
            part = x1[:, seg(b, 64), :].reshape(256, width)
            s1[c, seg(b, 256), :] = dot(p2[:], part).astype(BF16)
        exchange_start(s1, r1, 0, c, lambda d: (c, rows_of(d)))
    loop(crops, row_attention)

    def send_back(c, hops):
        exchange_part(s2, r2, 1, c, lambda d: (c, rows_of(d)), hops)

    def columns(c):
        exchange_wait(r1, 0, c, False)
        for sb in range(n // 4):
            moved = dot(p3[:], r1[c, seg(sb, sup), :]).astype(BF16)
            for i in range(rows):
                y1[i, seg(sb, 16), :] = moved[seg(i, 16), :]
        n_seq = y1.shape[1]
        mk = mm_ref[c].astype(F32).astype(BF16)
        mine = (iota((16, length), 1) == me * rows + iota((16, length), 0)).astype(F32).astype(BF16)
        m_t[:] = dot_nt(mine, jnp.concatenate([mk, mk], axis=0))
        rn[c] = 1.0 / (dot(m_t[:, 0:n_seq].astype(BF16), mk) + OPM_EPS)
        low = iota((HD, 2 * n_seq), 1) < n_seq
        picks = (iota((128 * rows, length), 1) == me * rows + iota((128 * rows, length), 0) // 128)
        mask_all = (dot_nt(mk, picks.astype(F32).astype(BF16)) - 1.0) * (MASK_SCALE * LOG2E)
        for i in range(rows):
            mc_s[i] = mask_all[:, seg(i, 128)]
        tokens = 4 * n_seq

        def doubled(y):
            return jnp.concatenate([y[n_seq * (r // 2):n_seq * (r // 2 + 1), :] for r in range(8)], axis=0)

        def before(q):
            y = layer_norm(y1[pl.ds(4 * q, 4)].reshape(tokens, width))
            qq = dot_nt(w_c[0:width, :], doubled(y))
            qc_s[q] = jnp.where(same_half(width, 2 * tokens, n_seq), qq, 0.0).astype(BF16)
            kc_s[q] = dot_nt(y, w_c[width:2 * width, :]).astype(BF16)
            vc_s[q] = dot_nt(y, w_c[2 * width:3 * width, :]).astype(BF16)
            gc_s[q] = sigmoid(dot_nt(w_c[3 * width:4 * width, :], y))
        loop(quads, before, U_CP)

        @pl.when(c == 1)
        def _():
            gather_relay(g_c, 1, 0, near)
            send_back(0, near)

        def middle(q):
            zeros = jnp.zeros((64, 128), BF16)
            for g in range(groups):
                heads = [[] for _ in range(4)]
                for r in range(4):
                    at = n_seq * r
                    wide = qc_s[q, seg(g, 128), seg(r, 128)]
                    stacked = jnp.concatenate([jnp.concatenate([wide[0:64], zeros], axis=0),
                                               jnp.concatenate([zeros, wide[64:128]], axis=0)], axis=1)
                    logits = dot(kc_s[q, at:at + n_seq, seg(g, 128)], stacked)
                    col = mc_s[4 * q + r]
                    probs = softmax_cols(logits * scale + jnp.concatenate([col, col], axis=1))
                    mixed = dot_tn(vc_s[q, at:at + n_seq, seg(g, 128)], probs)
                    for h in range(4):
                        heads[h].append(mixed[seg(h, HD), seg(h, n_seq)])
                mixed = jnp.concatenate([jnp.concatenate(h, axis=1) for h in heads], axis=0)
                oc_s[q, seg(g, 128), :] = (gc_s[q, seg(g, 128), :] * mixed).astype(BF16)
        loop(quads, middle, U_CM)

        def after(q):
            update = dot_tn(oc_s[q], w_co[:])
            x = y1[pl.ds(4 * q, 4)].reshape(tokens, width).astype(F32)
            y1[pl.ds(4 * q, 4)] = (x + update).astype(BF16).reshape(4, n_seq, width)
        loop(quads, after, U_CA)

        @pl.when(c == 1)
        def _():
            relay_forward(g_c, 1, 0)
            send_back(0, far[:2])

        def factors(q):
            y = layer_norm(y1[pl.ds(4 * q, 4)].reshape(tokens, width))
            all_four = dot_nt(w_ac[:], doubled(y)).astype(BF16).astype(F32)
            half = HD // 2
            for r in range(4):
                i = 4 * q + r
                both = all_four[:, seg(r, 128)] * m_t[pl.ds(i, 1), :]
                a = both[0:HD, :]
                at = pl.ds(pl.multiple_of(i * HD, HD), HD)
                a_t[c, 0, at, :] = jnp.where(low, a, 0.0).astype(BF16)
                a_t[c, 1, at, :] = jnp.where(low, 0.0, a).astype(BF16)
                packed = jnp.where(low[0:half], both[HD:HD + half, :], both[HD + half:2 * HD, :])
                c_t[pl.ds(pl.multiple_of(i * half, half), half), :] = packed.astype(BF16)
        loop(quads, factors, U_CF)
        g_c[c, me] = dot(p5[:], c_t[:]).astype(BF16)
        gather_start(g_c, 1, c, near)
        for db in range(n // 4):
            part = y1[:, seg(db, 16), :].reshape(16 * rows, width)
            s2[c, seg(db, sup), :] = dot(p3t[:], part).astype(BF16)
        exchange_own(s2, r2, lambda d: (c, rows_of(d)))

        @pl.when(c == 1)
        def _():
            send_back(0, far[2:] + (0,))
    loop(crops, columns)

    def bias_row(i, y, w_b):
        tmp_b[pl.ds(pl.multiple_of(i * 8, 8), 4), :] = dot_nt(w_b[:], y)

    def bias_send(buf, e, c, hops):
        buf[c, me] = dot(p6[0:blk, :], tmp_b[:].astype(BF16)).astype(BF16)
        gather_start(buf, e, c, hops)

    def outer(c):
        gather_wait(g_c, 1, c)

        def unpack(q):
            for sb in range(n // 4):
                part = g_c[c, 4 * sb:4 * sb + 4, pl.ds(pl.multiple_of(blk * q, 16), blk), :].reshape(sup, 128)
                moved = dot(p4[:], part).astype(BF16)
                for i in range(4):
                    c_f[4 * q + i, seg(sb, blk), :] = moved[seg(i, blk), :]
        loop(HD // 2 // 4, unpack, U_UNP)

        @pl.when(c == 1)
        def _():
            gather_relay(g_t1, 2, 0, near)
            send_back(1, far[:2])

        def products(fp):
            for half in range(2):
                u = dot_nt(a_t[c, half], c_f[fp])
                for i in range(rows):
                    at = pl.ds(pl.multiple_of(fp * 2 * HD + half * HD, HD), HD)
                    u_s[i, at, :] = (u[seg(i, HD), :] * rn[c, i:i + 1, :]).astype(BF16)
        loop(HD // 2, products, U_PROD)

        @pl.when(c == 1)
        def _():
            relay_forward(g_t1, 2, 0)
            send_back(1, far[2:] + (0,))

        def one(i):
            update = dot(w_fet[:], u_s[i])
            z1[c, i] = (z_ref[c, i].astype(F32) + update.T).astype(BF16)
        loop(rows, one, U_OUT)

        @pl.when(c == 0)
        def _():
            gather_relay(g_c, 1, 1, near)

        def norm(i):
            y = layer_norm(z1[c, i])
            yn[c, i] = y
            bias_row(i, y, w_tsb)
        loop(rows, norm, U_LN)
        bias_send(g_t1, 2, c, near)

        @pl.when(c == 0)
        def _():
            send_back(1, near)
            relay_forward(g_c, 1, 1)
    loop(crops, outer)

    def triangle(c, w_out, done):
        def quad(q):
            attend(4 * q, 4, lambda u: bm_tri[:])

            def after(k):
                i = 4 * q + k
                x3[i] = (z1[c, i].astype(F32) + dot_tn(o_s[i], w_out[:])).astype(BF16)
            loop(4, after, 4)
            done(q)
        loop(quads, quad)

    def start_node(c):
        loop(rows, lambda i: project(yn[c, i], w_ts, i), U_TP)

        @pl.when(c == 0)
        def _():
            gather_relay(g_t1, 2, 1, near)
        gather_wait(g_t1, 2, c)
        unpack_bias(g_t1, c, p4, 4, blk)
        col = mask_columns(rm_ref[pl.ds(c, 1), :], eye)
        col3 = jnp.concatenate([col] * (two // 128), axis=1)
        for pair in range(2):
            bm_tri[:, seg(pair, two)] = dot_nt(eye[:], b_q[seg(pair, two), :]) * LOG2E + col3

        def done(q):
            for k in range(4):
                i = 4 * q + k
                bias_row(i, layer_norm(x3[i]), w_teb)

            @pl.when(q == quads - 1)
            def _():
                bias_send(g_t2, 3, c, steps)
            for b in range(blocks):
                part = x3[pl.ds(4 * q, 4), seg(b, 64), :].reshape(256, 128)
                s3[c, q, seg(b, 256), :] = dot(p2[:], part).astype(BF16)
            exchange_start(s3, r3, 2, c, lambda d: (c, q, rows_of(d)))

            @pl.when((c == 0) & (q == 0))
            def _():
                relay_forward(g_t1, 2, 1)
        triangle(c, w_tso, done)
    loop(crops, start_node)

    def end_node(c):
        exchange_wait(r3, 2, c, True)
        for q in range(quads):
            for sb in range(n // 4):
                moved = dot(p3[:], r3[c, q, seg(sb, sup), :]).astype(BF16)
                for i in range(rows):
                    at = 64 * q + 16 * sb
                    z1[c, i, at:at + 16, :] = moved[seg(i, 16), :]
        loop(rows, lambda i: project(layer_norm(z1[c, i]), w_te, i), U_TP)
        gather_forward(g_t2, 3, c, steps)
        gather_wait(g_t2, 3, c)
        unpack_bias(g_t2, c, p4e, 4 * quads, 16)
        col = mask_columns(rm_ref[pl.ds(c, 1), :], tok)
        col3 = jnp.concatenate([col] * (two // 128), axis=1)
        for pair in range(2):
            left = dot_nt(b_q[seg(2 * pair, length), :], tok_l[:])
            right = dot_nt(b_q[seg(2 * pair + 1, length), :], tok_r[:])
            bm_tri[:, seg(pair, two)] = (left + right) * LOG2E + col3

        def done(q):
            for p in range(quads):
                for db in range(n // 4):
                    part = x3[pl.ds(4 * q, 4), 64 * p + 16 * db:64 * p + 16 * (db + 1), :].reshape(64, 128)
                    moved = dot(p64[:], part).astype(BF16)
                    for i in range(4):
                        s4[c, p, rows_of(4 * db + i, 16 * q, 16), :] = moved[seg(i, 16), :]
            exchange_start(s4, r4, 3, c, lambda d: (c, slice(None), rows_of(d, 16 * q, 16)))
        triangle(c, w_teo, done)
    loop(crops, end_node)

    def finish_msa(c):
        exchange_wait(r2, 1, c, False)
        for b in range(blocks):
            moved = dot(p2t[:], r2[c, seg(b, 256), :]).astype(BF16)
            for i in range(seqs):
                out_m[c, i, seg(b, 64), :] = moved[seg(i, 64), :]
    loop(crops, finish_msa)

    def finish_pair(c):
        exchange_wait(r4, 3, c, True)
        for q in range(quads):
            for b in range(blocks):
                moved = dot(p2t[:], r4[c, q, seg(b, 256), :]).astype(BF16)
                for i in range(4):
                    out_z[c, 4 * q + i, seg(b, 64), :] = moved[seg(i, 64), :]
    loop(crops, finish_pair)

    def drain(c):
        for e, (buf, hops) in enumerate(((g_row, steps), (g_c, near), (g_t1, near), (g_t2, steps))):
            gather_end(buf, e, c, hops)
        for e, (buf, planes) in enumerate(((s1, False), (s2, False), (s3, True), (s4, True))):
            exchange_end(buf, e, c, planes)
    loop(crops, drain)


def solution(mesh):
    n = mesh.shape[GROUP_AXIS]
    rows_spec = P(PART_AXIS, GROUP_AXIS, None, None)
    in_specs = (rows_spec, rows_spec, P(PART_AXIS, None, None), P(PART_AXIS, None)) + (P(),) * N_WEIGHTS

    def local_block(msa, pair, msa_mask, res_mask, *weights):
        (w_rb, w_r, w_ro, w_c, w_co, w_ac, w_oo, w_tsb, w_ts, w_tso, w_teb, w_te, w_teo) = weights
        crops, seqs, length, width = msa.shape
        rows, pair_width = pair.shape[1], pair.shape[3]
        n_seq = msa_mask.shape[1]
        heads, tri_heads = w_r.shape[2], w_ts.shape[2]
        quads = rows // 4

        def flat_t(w):
            return jnp.transpose(w, (1, 2, 3, 0)).reshape(-1, w.shape[0])

        operands = [
            msa, pair, msa_mask, res_mask,
            w_rb.T, flat_t(w_r), w_ro.reshape(width, width), flat_t(w_c), w_co.reshape(width, width),
            jnp.transpose(w_ac, (1, 2, 0)).reshape(-1, width), w_oo.reshape(-1, pair_width),
            w_tsb.T, flat_t(w_ts), w_tso.reshape(pair_width, pair_width),
            w_teb.T, flat_t(w_te), w_teo.reshape(pair_width, pair_width),
        ]
        p2 = permutation((4, 64), (1, 0))
        p3 = permutation((4, rows, 4), (1, 0, 2))
        p4 = permutation((4, 4, rows), (1, 0, 2))
        p4e = permutation((4, 4, quads, 4), (1, 2, 0, 3))
        p5 = permutation((rows, HD // 2), (1, 0))
        p6 = permutation((rows, heads), (1, 0))
        p64 = permutation((4, 4, 4), (1, 0, 2))
        tok = permutation((n, quads, 4), (1, 0, 2))
        consts = [p2, p2.T, p3, p3.T, p4, p4e, p5, p6, p64, np.eye(length), tok,
                  np.concatenate([tok, 0 * tok]), np.concatenate([0 * tok, tok])]
        operands += [jnp.asarray(a, BF16) for a in consts]

        vmem = pl.BlockSpec(memory_space=pltpu.VMEM)
        total = n * 4 * rows
        scratch = [
            pltpu.VMEM((crops, n, heads * rows + 4 * rows, 128), BF16),
            pltpu.VMEM((crops, n, HD // 2 * rows, 128), BF16),
            pltpu.VMEM((crops, n, tri_heads * rows, length), BF16),
            pltpu.VMEM((crops, n, tri_heads * rows, length), BF16),
        ]
        scratch += [pltpu.VMEM((crops, total, width), BF16)] * 4
        scratch += [pltpu.VMEM((crops, quads, total, pair_width), BF16)] * 4
        scratch += [
            pltpu.VMEM((8 * rows, length), F32),
            pltpu.VMEM((heads * length, length), BF16),
            pltpu.VMEM((width // 128, length, 4 * length), F32),
            pltpu.VMEM((length, tri_heads * length), F32),
            pltpu.VMEM((seqs, length, width), BF16),
            pltpu.VMEM((rows, n_seq, width), BF16),
            pltpu.VMEM((16, 2 * n_seq), F32),
            pltpu.VMEM((crops, 16, length), F32),
            pltpu.VMEM((crops, 2, rows * HD, 128), BF16),
            pltpu.VMEM((rows * HD // 2, 128), BF16),
            pltpu.VMEM((HD // 2, length, 128), BF16),
            pltpu.VMEM((rows, HD * HD, length), BF16),
            pltpu.VMEM((HD * HD, pair_width), F32),
            pltpu.VMEM((HD * HD, pair_width), F32),
            pltpu.VMEM((pair_width, HD * HD), BF16),
            pltpu.VMEM((crops, rows, length, pair_width), BF16),
            pltpu.VMEM((crops, rows, length, pair_width), BF16),
            pltpu.VMEM((rows, length, pair_width), BF16),
            pltpu.VMEM((rows, 128, 4 * length), BF16),
            pltpu.VMEM((rows, length, 128), BF16),
            pltpu.VMEM((rows, 128, length), BF16),
            pltpu.VMEM((rows, 128, length), F32),
            pltpu.VMEM((rows, 128, length), BF16),
            pltpu.VMEM((2, length, 4 * length), F32),
            pltpu.VMEM((seqs, length, 128), F32),
            pltpu.VMEM((quads, width, 8 * n_seq), BF16),
            pltpu.VMEM((quads, 4 * n_seq, width), BF16),
            pltpu.VMEM((quads, 4 * n_seq, width), BF16),
            pltpu.VMEM((quads, width, 4 * n_seq), F32),
            pltpu.VMEM((quads, width, 4 * n_seq), BF16),
            pltpu.VMEM((rows, n_seq, 128), F32),
        ]
        scratch += [pltpu.SemaphoreType.DMA((4, crops))] * 8
        return pl.pallas_call(
            functools.partial(block_kernel, n),
            out_shape=(jax.ShapeDtypeStruct(msa.shape, BF16), jax.ShapeDtypeStruct(pair.shape, BF16)),
            in_specs=[vmem] * len(operands),
            out_specs=(vmem, vmem),
            scratch_shapes=scratch,
            compiler_params=pltpu.CompilerParams(collective_id=0, has_side_effects=True, vmem_limit_bytes=VMEM_BYTES),
            name='evoformer_block',
        )(*operands)

    return jax.shard_map(local_block, mesh=mesh, in_specs=in_specs, out_specs=(rows_spec, rows_spec),
                         check_vma=False)
```

```python
import functools
import math

import jax
import jax.numpy as jnp
import numpy as np
from jax import lax
from jax.experimental import pallas as pl
from jax.experimental.pallas import tpu as pltpu
from jax.sharding import PartitionSpec as P

MASK_SCALE = 10000.0
LN_EPS = 1e-5
OPM_EPS = 1e-3
LOG2E = math.log2(math.e)
N_WEIGHTS = 13
PART_AXIS = 'data'
GROUP_AXIS = 'dap'
MESH = pl.DeviceIdType.MESH
F32 = jnp.float32
BF16 = jnp.bfloat16
HD = 32
U_LN, U_UNP, U_PROD, U_OUT = 12, 2, 4, 3
U_PR, U_PO, U_TP, U_TA, U_CP, U_CM, U_CA, U_CF = 2, 4, 3, 4, 1, 1, 3, 3
VMEM_BYTES = 60 * 1024 * 1024


def dot(a, b):
    return lax.dot_general(a, b, (((1,), (0,)), ((), ())), preferred_element_type=F32)


def dot_nt(a, b):
    return lax.dot_general(a, b, (((1,), (1,)), ((), ())), preferred_element_type=F32)


def dot_tn(a, b):
    return lax.dot_general(a, b, (((0,), (0,)), ((), ())), preferred_element_type=F32)


def layer_norm(x):
    x_float = x.astype(F32)
    centred = x_float - jnp.mean(x_float, axis=-1, keepdims=True)
    var = jnp.mean(centred * centred, axis=-1, keepdims=True)
    return (centred * lax.rsqrt(var + LN_EPS)).astype(BF16)


def seg(i, size):
    return slice(i * size, (i + 1) * size)


def sigmoid(x):
    return 1.0 / (1.0 + jnp.exp2(x * (-LOG2E)))


def iota(shape, dim):
    return lax.broadcasted_iota(jnp.int32, shape, dim)


def permutation(sizes, order, keep=None):
    total = int(np.prod(sizes))
    source = np.arange(total).reshape(sizes).transpose(order).reshape(-1)
    out = np.zeros((total, total), np.float32)
    out[np.arange(total), source] = 1.0
    return out


def softmax_cols(t):
    e = jnp.exp2(t - jnp.max(t, axis=0, keepdims=True))
    return (e * (1.0 / jnp.sum(e, axis=0, keepdims=True))).astype(BF16)


def same_half(width, lanes, half):
    return (iota((width, lanes), 0) // HD) % 2 == (iota((width, lanes), 1) // half) % 2


def block_kernel(n, x_ref, z_ref, mm_ref, rm_ref,
                 w_rb, w_r, w_ro, w_c, w_co, w_ac, w_oo, w_tsb, w_ts, w_tso, w_teb, w_te, w_teo,
                 p2, p2t, p3, p3t, p4, p4b, p4e, p4eb, p5, p6, p64, eye, tok, tok_l, tok_r,
                 out_m, out_z,
                 g_r0, g_r1, g_c, g_t1, g_t2, s1, r1, s2, r2, s3, r3, s4, r4,
                 tmp_b, b_q, bm_tri, x1, y1, m_t, rn, a_t, c_t, c_f, u_s, w_f32, w_fe, w_fet, z1, yn, x3,
                 q_s, k_s, v_s, g_s, o_s, s_buf, m_s, qc_s, kc_s, vc_s, gc_s, oc_s, mc_s,
                 gs_a, gr_a, gs_b, gr_b, gs_f, gr_f, as_sem, ar_sem):
    me = lax.axis_index(GROUP_AXIS)
    g_row = (g_r0, g_r1)
    chips = n // 2
    chip = me // 2
    core = me % 2
    partner = me + 1 - 2 * core
    crops, seqs, length, width = x_ref.shape
    rows = z_ref.shape[1]
    quads = rows // 4
    blocks = length // 64
    blk = 4 * rows
    sup = 4 * blk
    steps = []
    for k in range(1, chips // 2 + 1):
        steps.append(k)
        if chips - k != k:
            steps.append(chips - k)

    near = (1, chips - 1, 2, chips - 2)
    far = tuple(k for k in steps if k not in near)

    barrier = pltpu.get_barrier_semaphore()
    for k in range(1, n):
        pl.semaphore_signal(barrier, inc=1, device_id={GROUP_AXIS: lax.rem(me + k, n)}, device_id_type=MESH)
    def remote(src, dst, send, recv, device):
        return pltpu.make_async_remote_copy(src_ref=src, dst_ref=dst, send_sem=send, recv_sem=recv,
                                            device_id={GROUP_AXIS: device}, device_id_type=MESH)

    def same_core(k):
        return 2 * lax.rem(chip + k, chips) + core

    def wait_bytes(ref, sem):
        pltpu.make_async_copy(ref, ref, sem).wait()

    def to_partner(block, e, c):
        remote(block, block, gs_b.at[e, c], gr_b.at[e, c], partner).start()

    def gather_start(buf, e, c, hops):
        mine = buf.at[c, me]
        for k in hops:
            remote(mine, mine, gs_a.at[e, c], gr_a.at[e, c], same_core(k)).start()
        to_partner(mine, e, c)

    def gather_forward(buf, e, c, hops):
        wait_bytes(buf.at[c, pl.ds(0, len(hops))], gr_a.at[e, c])
        for k in hops:
            to_partner(buf.at[c, same_core(k)], e, c)

    def gather_relay(buf, e, c, hops):
        wait_bytes(buf.at[c, pl.ds(0, len(hops))], gr_a.at[e, c])
        height = buf.shape[2]
        cut = height // 2 // 16 * 16
        for sign, part in ((1, pl.ds(0, cut)), (-1, pl.ds(cut, height - cut))):
            source = same_core(chips - 2 * sign)
            block = buf.at[c, source]
            remote(block, block, gs_f.at[e, c], gr_f.at[e, c], same_core(chips + sign)).start()
            half = buf.at[c, source, part]
            remote(half, half, gs_f.at[e, c], gr_f.at[e, c], same_core(chips + 2 * sign)).start()
        for k in hops:
            to_partner(buf.at[c, same_core(k)], e, c)

    def relay_forward(buf, e, c):
        wait_bytes(buf.at[c, pl.ds(0, len(far))], gr_f.at[e, c])
        for k in far:
            to_partner(buf.at[c, same_core(k)], e, c)

    def gather_wait(buf, e, c):
        wait_bytes(buf.at[c, pl.ds(0, chips)], gr_b.at[e, c])

    def gather_end(buf, e, c, hops):
        wait_bytes(buf.at[c, pl.ds(0, len(hops))], gs_a.at[e, c])
        wait_bytes(buf.at[c, pl.ds(0, chips)], gs_b.at[e, c])
        if hops is near:
            wait_bytes(buf.at[c, pl.ds(0, len(far))], gs_f.at[e, c])

    def rows_of(d, offset=0, height=None):
        return pl.ds(pl.multiple_of(d * blk + offset, 16), height or blk)

    def exchange_own(src, dst, index_of):
        dst[index_of(me)] = src[index_of(me)]

    def exchange_part(src, dst, e, c, index_of, hops):
        landing = dst.at[index_of(me)]
        for k in hops:
            for other in range(2):
                d = 2 * lax.rem(chip + k, chips) + (core + other) % 2
                if k or other:
                    remote(src.at[index_of(d)], landing, as_sem.at[e, c], ar_sem.at[e, c], d).start()

    def exchange_start(src, dst, e, c, index_of):
        exchange_own(src, dst, index_of)
        exchange_part(src, dst, e, c, index_of, steps + [0])

    def others(ref, c, planes):
        where = pl.ds(0, (n - 1) * blk)
        return ref.at[c, :, where, :] if planes else ref.at[c, where, :]

    def exchange_wait(dst, e, c, planes):
        wait_bytes(others(dst, c, planes), ar_sem.at[e, c])

    def exchange_end(src, e, c, planes):
        wait_bytes(others(src, c, planes), as_sem.at[e, c])

    def loop(count, body, unroll=1):
        def several(i, carry):
            for k in range(unroll):
                body(i * unroll + k)
            return carry
        lax.fori_loop(0, count // unroll, several, 0)

    def pack_bias(rows_f32):
        half = blk // 2
        last = jnp.concatenate([rows_f32[seg(g, half), 128:length] for g in range(2)], axis=1)
        return jnp.concatenate([rows_f32[:, 0:128], last, jnp.zeros((8, 128), F32)], axis=0).astype(BF16)

    tmp_b[:] = jnp.zeros_like(tmp_b)

    def row_bias(c):
        def one(i):
            tmp_b[pl.ds(pl.multiple_of(i * 8, 8), 8), :] = dot_nt(w_rb[:], layer_norm(z_ref[c, i]))
        loop(rows, one, U_LN)
        t = dot(p6[:], tmp_b[:].astype(BF16))
        for g, buf in enumerate(g_row):
            buf[c, me] = pack_bias(t[seg(g, blk), :])
    loop(crops, row_bias)
    pl.semaphore_wait(barrier, n - 1)

    def row_bias_send(c):
        for g, buf in enumerate(g_row):
            gather_start(buf, g, c, steps)
    loop(crops, row_bias_send)

    w_f32[:] = w_oo[:].astype(F32)
    for fp in range(HD // 2):
        for half in range(2):
            at = fp * 2 * HD + half * HD
            w_fe[at:at + HD, :] = w_f32[pl.ds(half * (HD // 2) + fp, HD, stride=HD), :]
    for b in range(HD * HD // 128):
        w_fet[:, seg(b, 128)] = w_fe[seg(b, 128), :].T.astype(BF16)
    q_s[:] = jnp.zeros_like(q_s)

    def unpack_bias(buf, c, perm, perm_last, pieces, piece):
        for sb in range(n // 4):
            moved = dot(perm[:], buf[c, seg(sb, 4), 0:blk, :].reshape(sup, 128)).astype(BF16)
            last = dot(perm_last[:], buf[c, seg(sb, 4), blk:, :].reshape(128, 128)).astype(BF16)
            for i in range(pieces):
                at = i * (4 * length // pieces) + sb * piece
                b_q[at:at + piece, 0:128] = moved[seg(i, piece), :]
                b_q[at:at + piece, 128:length] = last[seg(i % (pieces // 2), piece), seg(2 * i // pieces, 64)]

    def mask_columns(row, select):
        wide = jnp.broadcast_to(row.astype(F32), (128, length)).astype(BF16)
        return (dot_nt(select[:], wide) - 1.0) * (MASK_SCALE * LOG2E)

    scale = HD ** -0.5 * LOG2E
    two, four = 2 * length, 4 * length

    def project(y, w_t, first, stride=1):
        wide = y.shape[1]
        q = dot_nt(w_t[0:wide, :], jnp.concatenate([y, y], axis=0))
        q = jnp.where(same_half(wide, two, length), q, 0.0).astype(BF16)
        keys = dot_nt(y, w_t[wide:2 * wide, :]).astype(BF16)
        values = dot_nt(w_t[2 * wide:3 * wide, :], y).astype(BF16)
        gate = sigmoid(dot_nt(w_t[3 * wide:4 * wide, :], y))
        for g in range(wide // 128):
            u = first + g * stride
            q_s[u, 0:64, 0:two] = q[128 * g:128 * g + 64, :]
            q_s[u, 64:128, two:four] = q[128 * g + 64:128 * g + 128, :]
            k_s[u] = keys[:, seg(g, 128)]
            v_s[u] = values[seg(g, 128), :]
            g_s[u] = gate[seg(g, 128), :]

    def attend(first, count, bias_of):
        def mix(u, probs):
            pieces = []
            for p in range(2):
                mixed = dot(v_s[u, seg(p, 64), :], probs[:, seg(p, two)])
                pieces += [mixed[0:HD, 0:length], mixed[HD:2 * HD, length:two]]
            return jnp.concatenate(pieces, axis=0)

        def finish(u, mixed):
            o_s[u] = (g_s[u] * mixed).astype(BF16)

        s_buf[0] = dot(k_s[first], q_s[first])

        def pair(i):
            u = first + 2 * i
            s_buf[1] = dot(k_s[u + 1], q_s[u + 1])
            mixed = mix(u, softmax_cols(s_buf[0] * scale + bias_of(u)))
            after = jnp.minimum(u + 2, first + count - 1)
            s_buf[0] = dot(k_s[after], q_s[after])
            probs = softmax_cols(s_buf[1] * scale + bias_of(u + 1))
            finish(u, mixed)
            finish(u + 1, mix(u + 1, probs))
        loop(count // 2, pair)

    groups = width // 128

    def row_attention(c):
        def before(s):
            m_s[s] = mask_columns(mm_ref[c, pl.ds(me * seqs + s, 1), :], eye)
            project(layer_norm(x_ref[c, s]), w_r, s, seqs)
        loop(seqs, before, U_PR)
        for g, buf in enumerate(g_row):
            gather_forward(buf, g, c, steps)
            gather_wait(buf, g, c)
            unpack_bias(buf, c, p4, p4b, 4, blk)
            for pair in range(2):
                bm_tri[:, seg(pair, two)] = dot_nt(eye[:], b_q[seg(pair, two), :]) * LOG2E

            def bias_of(u):
                return bm_tri[:] + jnp.concatenate([m_s[u - g * seqs]] * (four // 128), axis=1)
            attend(g * seqs, seqs, bias_of)

        def after(s):
            gated = jnp.concatenate([o_s[g * seqs + s] for g in range(groups)], axis=0)
            x1[s] = (x_ref[c, s].astype(F32) + dot_tn(gated, w_ro[:])).astype(BF16)
        loop(seqs, after, U_PO)
        for b in range(blocks):
            part = x1[:, seg(b, 64), :].reshape(256, width)
            s1[c, seg(b, 256), :] = dot(p2[:], part).astype(BF16)
        exchange_start(s1, r1, 0, c, lambda d: (c, rows_of(d)))
    loop(crops, row_attention)

    def send_back(c, hops):
        exchange_part(s2, r2, 1, c, lambda d: (c, rows_of(d)), hops)

    def columns(c):
        exchange_wait(r1, 0, c, False)
        for sb in range(n // 4):
            moved = dot(p3[:], r1[c, seg(sb, sup), :]).astype(BF16)
            for i in range(rows):
                y1[i, seg(sb, 16), :] = moved[seg(i, 16), :]
        n_seq = y1.shape[1]
        mk = mm_ref[c].astype(F32).astype(BF16)
        mine = (iota((16, length), 1) == me * rows + iota((16, length), 0)).astype(F32).astype(BF16)
        m_t[:] = dot_nt(mine, jnp.concatenate([mk, mk], axis=0))
        rn[c] = 1.0 / (dot(m_t[:, 0:n_seq].astype(BF16), mk) + OPM_EPS)
        low = iota((HD, 2 * n_seq), 1) < n_seq
        picks = (iota((128 * rows, length), 1) == me * rows + iota((128 * rows, length), 0) // 128)
        mask_all = (dot_nt(mk, picks.astype(F32).astype(BF16)) - 1.0) * (MASK_SCALE * LOG2E)
        for i in range(rows):
            mc_s[i] = mask_all[:, seg(i, 128)]
        tokens = 4 * n_seq

        def doubled(y):
            return jnp.concatenate([y[n_seq * (r // 2):n_seq * (r // 2 + 1), :] for r in range(8)], axis=0)

        def before(q):
            y = layer_norm(y1[pl.ds(4 * q, 4)].reshape(tokens, width))
            qq = dot_nt(w_c[0:width, :], doubled(y))
            qc_s[q] = jnp.where(same_half(width, 2 * tokens, n_seq), qq, 0.0).astype(BF16)
            kc_s[q] = dot_nt(y, w_c[width:2 * width, :]).astype(BF16)
            vc_s[q] = dot_nt(y, w_c[2 * width:3 * width, :]).astype(BF16)
            gc_s[q] = sigmoid(dot_nt(w_c[3 * width:4 * width, :], y))
        loop(quads, before, U_CP)

        @pl.when(c == 1)
        def _():
            gather_relay(g_c, 2, 0, near)
            send_back(0, near + far[:2])

        def middle(q):
            zeros = jnp.zeros((64, 128), BF16)
            for g in range(groups):
                heads = [[] for _ in range(4)]
                for r in range(4):
                    at = n_seq * r
                    wide = qc_s[q, seg(g, 128), seg(r, 128)]
                    stacked = jnp.concatenate([jnp.concatenate([wide[0:64], zeros], axis=0),
                                               jnp.concatenate([zeros, wide[64:128]], axis=0)], axis=1)
                    logits = dot(kc_s[q, at:at + n_seq, seg(g, 128)], stacked)
                    col = mc_s[4 * q + r]
                    probs = softmax_cols(logits * scale + jnp.concatenate([col, col], axis=1))
                    mixed = dot_tn(vc_s[q, at:at + n_seq, seg(g, 128)], probs)
                    for h in range(4):
                        heads[h].append(mixed[seg(h, HD), seg(h, n_seq)])
                mixed = jnp.concatenate([jnp.concatenate(h, axis=1) for h in heads], axis=0)
                oc_s[q, seg(g, 128), :] = (gc_s[q, seg(g, 128), :] * mixed).astype(BF16)
        loop(quads, middle, U_CM)

        def after(q):
            update = dot_tn(oc_s[q], w_co[:])
            x = y1[pl.ds(4 * q, 4)].reshape(tokens, width).astype(F32)
            y1[pl.ds(4 * q, 4)] = (x + update).astype(BF16).reshape(4, n_seq, width)
        loop(quads, after, U_CA)

        @pl.when(c == 1)
        def _():
            relay_forward(g_c, 2, 0)

        def factors(q):
            y = layer_norm(y1[pl.ds(4 * q, 4)].reshape(tokens, width))
            all_four = dot_nt(w_ac[:], doubled(y)).astype(BF16).astype(F32)
            half = HD // 2
            for r in range(4):
                i = 4 * q + r
                both = all_four[:, seg(r, 128)] * m_t[pl.ds(i, 1), :]
                a = both[0:HD, :]
                at = pl.ds(pl.multiple_of(i * HD, HD), HD)
                a_t[c, 0, at, :] = jnp.where(low, a, 0.0).astype(BF16)
                a_t[c, 1, at, :] = jnp.where(low, 0.0, a).astype(BF16)
                packed = jnp.where(low[0:half], both[HD:HD + half, :], both[HD + half:2 * HD, :])
                c_t[pl.ds(pl.multiple_of(i * half, half), half), :] = packed.astype(BF16)
        loop(quads, factors, U_CF)
        g_c[c, me] = dot(p5[:], c_t[:]).astype(BF16)
        gather_start(g_c, 2, c, near)
        for db in range(n // 4):
            part = y1[:, seg(db, 16), :].reshape(16 * rows, width)
            s2[c, seg(db, sup), :] = dot(p3t[:], part).astype(BF16)
        exchange_own(s2, r2, lambda d: (c, rows_of(d)))
    loop(crops, columns)

    def bias_row(i, y, w_b):
        tmp_b[pl.ds(pl.multiple_of(i * 8, 8), 4), :] = dot_nt(w_b[:], y)

    def bias_send(buf, e, c, hops):
        buf[c, me] = pack_bias(dot(p6[0:blk, :], tmp_b[:].astype(BF16)))
        gather_start(buf, e, c, hops)

    def start_project(c):
        loop(rows, lambda i: project(yn[c, i], w_ts, i), U_TP)

    def outer(c):
        gather_wait(g_c, 2, c)

        def unpack(q):
            for sb in range(n // 4):
                part = g_c[c, 4 * sb:4 * sb + 4, pl.ds(pl.multiple_of(blk * q, 16), blk), :].reshape(sup, 128)
                moved = dot(p4[:], part).astype(BF16)
                for i in range(4):
                    c_f[4 * q + i, seg(sb, blk), :] = moved[seg(i, blk), :]
        loop(HD // 2 // 4, unpack, U_UNP)

        def products(fp):
            for half in range(2):
                u = dot_nt(a_t[c, half], c_f[fp])
                for i in range(rows):
                    at = pl.ds(pl.multiple_of(fp * 2 * HD + half * HD, HD), HD)
                    u_s[i, at, :] = (u[seg(i, HD), :] * rn[c, i:i + 1, :]).astype(BF16)
        loop(HD // 2, products, U_PROD)

        @pl.when(c == 1)
        def _():
            send_back(1, near + far[:2])

        def one(i):
            update = dot(w_fet[:], u_s[i])
            z1[c, i] = (z_ref[c, i].astype(F32) + update.T).astype(BF16)
        loop(rows, one, U_OUT)

        @pl.when(c == 0)
        def _():
            gather_relay(g_c, 2, 1, near)

        def norm(i):
            y = layer_norm(z1[c, i])
            yn[c, i] = y
            bias_row(i, y, w_tsb)
        loop(rows, norm, U_LN)

        @pl.when(c == 0)
        def _():
            start_project(0)
            relay_forward(g_c, 2, 1)
        bias_send(g_t1, 3, c, steps)
        send_back(c, far[2:] + (0,))

        @pl.when(c == 1)
        def _():
            gather_forward(g_t1, 3, 0, steps)
    loop(crops, outer)

    def triangle(c, w_out, done):
        def quad(q):
            attend(4 * q, 4, lambda u: bm_tri[:])

            def after(k):
                i = 4 * q + k
                x3[i] = (z1[c, i].astype(F32) + dot_tn(o_s[i], w_out[:])).astype(BF16)
            loop(4, after, 4)
            done(q)
        loop(quads, quad)

    def start_node(c):
        @pl.when(c == 1)
        def _():
            start_project(1)
            gather_forward(g_t1, 3, 1, steps)
        gather_wait(g_t1, 3, c)
        unpack_bias(g_t1, c, p4, p4b, 4, blk)
        col = mask_columns(rm_ref[pl.ds(c, 1), :], eye)
        col3 = jnp.concatenate([col] * (two // 128), axis=1)
        for pair in range(2):
            bm_tri[:, seg(pair, two)] = dot_nt(eye[:], b_q[seg(pair, two), :]) * LOG2E + col3

        def done(q):
            for k in range(4):
                i = 4 * q + k
                bias_row(i, layer_norm(x3[i]), w_teb)

            @pl.when(q == quads - 1)
            def _():
                bias_send(g_t2, 4, c, steps)
            for b in range(blocks):
                part = x3[pl.ds(4 * q, 4), seg(b, 64), :].reshape(256, 128)
                s3[c, q, seg(b, 256), :] = dot(p2[:], part).astype(BF16)
            exchange_start(s3, r3, 2, c, lambda d: (c, q, rows_of(d)))
        triangle(c, w_tso, done)
    loop(crops, start_node)

    def end_node(c):
        exchange_wait(r3, 2, c, True)
        for q in range(quads):
            for sb in range(n // 4):
                moved = dot(p3[:], r3[c, q, seg(sb, sup), :]).astype(BF16)
                for i in range(rows):
                    at = 64 * q + 16 * sb
                    z1[c, i, at:at + 16, :] = moved[seg(i, 16), :]
        loop(rows, lambda i: project(layer_norm(z1[c, i]), w_te, i), U_TP)
        gather_forward(g_t2, 4, c, steps)
        gather_wait(g_t2, 4, c)
        unpack_bias(g_t2, c, p4e, p4eb, 4 * quads, 16)
        col = mask_columns(rm_ref[pl.ds(c, 1), :], tok)
        col3 = jnp.concatenate([col] * (two // 128), axis=1)
        for pair in range(2):
            left = dot_nt(b_q[seg(2 * pair, length), :], tok_l[:])
            right = dot_nt(b_q[seg(2 * pair + 1, length), :], tok_r[:])
            bm_tri[:, seg(pair, two)] = (left + right) * LOG2E + col3

        def done(q):
            for p in range(quads):
                for db in range(n // 4):
                    part = x3[pl.ds(4 * q, 4), 64 * p + 16 * db:64 * p + 16 * (db + 1), :].reshape(64, 128)
                    moved = dot(p64[:], part).astype(BF16)
                    for i in range(4):
                        s4[c, p, rows_of(4 * db + i, 16 * q, 16), :] = moved[seg(i, 16), :]
            exchange_start(s4, r4, 3, c, lambda d: (c, slice(None), rows_of(d, 16 * q, 16)))
        triangle(c, w_teo, done)
    loop(crops, end_node)

    def finish_msa(c):
        exchange_wait(r2, 1, c, False)
        for b in range(blocks):
            moved = dot(p2t[:], r2[c, seg(b, 256), :]).astype(BF16)
            for i in range(seqs):
                out_m[c, i, seg(b, 64), :] = moved[seg(i, 64), :]
    loop(crops, finish_msa)

    def finish_pair(c):
        exchange_wait(r4, 3, c, True)
        for q in range(quads):
            for b in range(blocks):
                moved = dot(p2t[:], r4[c, q, seg(b, 256), :]).astype(BF16)
                for i in range(4):
                    out_z[c, 4 * q + i, seg(b, 64), :] = moved[seg(i, 64), :]
    loop(crops, finish_pair)

    def drain(c):
        for e, (buf, hops) in enumerate([(b, steps) for b in g_row] + [(g_c, near), (g_t1, steps), (g_t2, steps)]):
            gather_end(buf, e, c, hops)
        for e, (buf, planes) in enumerate(((s1, False), (s2, False), (s3, True), (s4, True))):
            exchange_end(buf, e, c, planes)
    loop(crops, drain)


def solution(mesh):
    n = mesh.shape[GROUP_AXIS]
    rows_spec = P(PART_AXIS, GROUP_AXIS, None, None)
    in_specs = (rows_spec, rows_spec, P(PART_AXIS, None, None), P(PART_AXIS, None)) + (P(),) * N_WEIGHTS

    def local_block(msa, pair, msa_mask, res_mask, *weights):
        (w_rb, w_r, w_ro, w_c, w_co, w_ac, w_oo, w_tsb, w_ts, w_tso, w_teb, w_te, w_teo) = weights
        crops, seqs, length, width = msa.shape
        rows, pair_width = pair.shape[1], pair.shape[3]
        n_seq = msa_mask.shape[1]
        heads, tri_heads = w_r.shape[2], w_ts.shape[2]
        quads = rows // 4

        def flat_t(w):
            return jnp.transpose(w, (1, 2, 3, 0)).reshape(-1, w.shape[0])

        operands = [
            msa, pair, msa_mask, res_mask,
            w_rb.T, flat_t(w_r), w_ro.reshape(width, width), flat_t(w_c), w_co.reshape(width, width),
            jnp.transpose(w_ac, (1, 2, 0)).reshape(-1, width), w_oo.reshape(-1, pair_width),
            w_tsb.T, flat_t(w_ts), w_tso.reshape(pair_width, pair_width),
            w_teb.T, flat_t(w_te), w_teo.reshape(pair_width, pair_width),
        ]
        p2 = permutation((4, 64), (1, 0))
        p3 = permutation((4, rows, 4), (1, 0, 2))
        p4 = permutation((4, 4, rows), (1, 0, 2))
        p4e = permutation((4, 4, quads, 4), (1, 2, 0, 3))

        def last(p):
            half = p[:len(p) // 2].reshape(-1, 4, 4 * rows)[:, :, :2 * rows]
            return np.pad(half, ((0, 0), (0, 0), (0, 32 - 2 * rows))).reshape(len(p) // 2, -1)
        p5 = permutation((rows, HD // 2), (1, 0))
        p6 = permutation((rows, heads), (1, 0))
        p64 = permutation((4, 4, 4), (1, 0, 2))
        tok = permutation((n, quads, 4), (1, 0, 2))
        consts = [p2, p2.T, p3, p3.T, p4, last(p4), p4e, last(p4e), p5, p6, p64, np.eye(length), tok,
                  np.concatenate([tok, 0 * tok]), np.concatenate([0 * tok, tok])]
        operands += [jnp.asarray(a, BF16) for a in consts]

        vmem = pl.BlockSpec(memory_space=pltpu.VMEM)
        total = n * 4 * rows
        bias = pltpu.VMEM((crops, n, 4 * rows + 32, 128), BF16)
        scratch = [
            bias, bias,
            pltpu.VMEM((crops, n, HD // 2 * rows, 128), BF16),
            bias, bias,
        ]
        scratch += [pltpu.VMEM((crops, total, width), BF16)] * 4
        scratch += [pltpu.VMEM((crops, quads, total, pair_width), BF16)] * 4
        scratch += [
            pltpu.VMEM((8 * rows, length), F32),
            pltpu.VMEM((tri_heads * length, length), BF16),
            pltpu.VMEM((length, tri_heads * length), F32),
            pltpu.VMEM((seqs, length, width), BF16),
            pltpu.VMEM((rows, n_seq, width), BF16),
            pltpu.VMEM((16, 2 * n_seq), F32),
            pltpu.VMEM((crops, 16, length), F32),
            pltpu.VMEM((crops, 2, rows * HD, 128), BF16),
            pltpu.VMEM((rows * HD // 2, 128), BF16),
            pltpu.VMEM((HD // 2, length, 128), BF16),
            pltpu.VMEM((rows, HD * HD, length), BF16),
            pltpu.VMEM((HD * HD, pair_width), F32),
            pltpu.VMEM((HD * HD, pair_width), F32),
            pltpu.VMEM((pair_width, HD * HD), BF16),
            pltpu.VMEM((crops, rows, length, pair_width), BF16),
            pltpu.VMEM((crops, rows, length, pair_width), BF16),
            pltpu.VMEM((rows, length, pair_width), BF16),
            pltpu.VMEM((rows, 128, 4 * length), BF16),
            pltpu.VMEM((rows, length, 128), BF16),
            pltpu.VMEM((rows, 128, length), BF16),
            pltpu.VMEM((rows, 128, length), F32),
            pltpu.VMEM((rows, 128, length), BF16),
            pltpu.VMEM((2, length, 4 * length), F32),
            pltpu.VMEM((seqs, length, 128), F32),
            pltpu.VMEM((quads, width, 8 * n_seq), BF16),
            pltpu.VMEM((quads, 4 * n_seq, width), BF16),
            pltpu.VMEM((quads, 4 * n_seq, width), BF16),
            pltpu.VMEM((quads, width, 4 * n_seq), F32),
            pltpu.VMEM((quads, width, 4 * n_seq), BF16),
            pltpu.VMEM((rows, n_seq, 128), F32),
        ]
        scratch += [pltpu.SemaphoreType.DMA((5, crops))] * 8
        return pl.pallas_call(
            functools.partial(block_kernel, n),
            out_shape=(jax.ShapeDtypeStruct(msa.shape, BF16), jax.ShapeDtypeStruct(pair.shape, BF16)),
            in_specs=[vmem] * len(operands),
            out_specs=(vmem, vmem),
            scratch_shapes=scratch,
            compiler_params=pltpu.CompilerParams(collective_id=0, has_side_effects=True, vmem_limit_bytes=VMEM_BYTES),
            name='evoformer_block',
        )(*operands)

    return jax.shard_map(local_block, mesh=mesh, in_specs=in_specs, out_specs=(rows_spec, rows_spec),
                         check_vma=False)
```

```python
import functools
import math

import jax
import jax.numpy as jnp
import numpy as np
from jax import lax
from jax.experimental import pallas as pl
from jax.experimental.pallas import tpu as pltpu
from jax.sharding import PartitionSpec as P

MASK_SCALE = 10000.0
LN_EPS = 1e-5
OPM_EPS = 1e-3
LOG2E = math.log2(math.e)
N_WEIGHTS = 13
PART_AXIS = 'data'
GROUP_AXIS = 'dap'
MESH = pl.DeviceIdType.MESH
F32 = jnp.float32
BF16 = jnp.bfloat16
HD = 32
U_LN, U_UNP, U_PROD, U_OUT = 12, 2, 4, 3
U_PR, U_PO, U_TP, U_CP, U_CM, U_CF = 2, 4, 3, 3, 3, 3
VMEM_BYTES = 60 * 1024 * 1024


def dot(a, b):
    return lax.dot_general(a, b, (((1,), (0,)), ((), ())), preferred_element_type=F32)


def dot_nt(a, b):
    return lax.dot_general(a, b, (((1,), (1,)), ((), ())), preferred_element_type=F32)


def dot_tn(a, b):
    return lax.dot_general(a, b, (((0,), (0,)), ((), ())), preferred_element_type=F32)


def layer_norm(x):
    x_float = x.astype(F32)
    centred = x_float - jnp.mean(x_float, axis=-1, keepdims=True)
    var = jnp.mean(centred * centred, axis=-1, keepdims=True)
    return (centred * lax.rsqrt(var + LN_EPS)).astype(BF16)


def seg(i, size):
    return slice(i * size, (i + 1) * size)


def sigmoid(x):
    return 1.0 / (1.0 + jnp.exp2(x * (-LOG2E)))


def iota(shape, dim):
    return lax.broadcasted_iota(jnp.int32, shape, dim)


def permutation(sizes, order, keep=None):
    total = int(np.prod(sizes))
    source = np.arange(total).reshape(sizes).transpose(order).reshape(-1)
    out = np.zeros((total, total), np.float32)
    out[np.arange(total), source] = 1.0
    return out


def softmax_cols(t):
    e = jnp.exp2(t - jnp.max(t, axis=0, keepdims=True))
    return (e * (1.0 / jnp.sum(e, axis=0, keepdims=True))).astype(BF16)


def same_half(width, lanes, half):
    return (iota((width, lanes), 0) // HD) % 2 == (iota((width, lanes), 1) // half) % 2


def block_kernel(n, x_ref, z_ref, mm_ref, rm_ref,
                 w_rb, w_r, w_ro, w_c, w_co, w_ac, w_oo, w_tsb, w_ts, w_tso, w_teb, w_te, w_teo,
                 p2, p2t, p3, p3t, p4, p4b, p4e, p4eb, p5, p6, p64, eye, tok, tok_l, tok_r,
                 out_m, out_z,
                 g_r0, g_r1, g_c, g_t1, g_t2, s1, r1, s2, r2, s3, r3, s4, r4,
                 tmp_b, b_q, bm_tri, x1, y1, m_t, rn, a_t, c_t, c_f, u_s, w_f32, w_fe, w_fet, z1, yn, x3,
                 q_s, k_s, v_s, g_s, o_s, s_buf, m_s, qc_s, kc_s, vc_s, gc_s, oc_s, mc_s,
                 gs_a, gr_a, gs_b, gr_b, gs_f, gr_f, as_sem, ar_sem):
    me = lax.axis_index(GROUP_AXIS)
    g_row = (g_r0, g_r1)
    chips = n // 2
    chip = me // 2
    core = me % 2
    partner = me + 1 - 2 * core
    crops, seqs, length, width = x_ref.shape
    rows = z_ref.shape[1]
    quads = rows // 4
    blocks = length // 64
    blk = 4 * rows
    sup = 4 * blk
    steps = []
    for k in range(chips // 2, 0, -1):
        steps += [k] if chips - k == k else [chips - k, k]
    near = (2, chips - 2, 1, chips - 1)
    far = tuple(k for k in steps if k not in near)
    middle_hops, last_hops = far[1:], far[:1] + (0,)

    barrier = pltpu.get_barrier_semaphore()
    for k in range(1, n):
        pl.semaphore_signal(barrier, inc=1, device_id={GROUP_AXIS: lax.rem(me + k, n)}, device_id_type=MESH)
    def remote(src, dst, send, recv, device):
        return pltpu.make_async_remote_copy(src_ref=src, dst_ref=dst, send_sem=send, recv_sem=recv,
                                            device_id={GROUP_AXIS: device}, device_id_type=MESH)

    def same_core(k):
        return 2 * lax.rem(chip + k, chips) + core

    def wait_bytes(ref, sem):
        pltpu.make_async_copy(ref, ref, sem).wait()

    def to_partner(block, e, c):
        remote(block, block, gs_b.at[e, c], gr_b.at[e, c], partner).start()

    def gather_start(buf, e, c, hops):
        mine = buf.at[c, me]
        for k in hops:
            remote(mine, mine, gs_a.at[e, c], gr_a.at[e, c], same_core(k)).start()
        to_partner(mine, e, c)

    def gather_forward(buf, e, c, hops):
        wait_bytes(buf.at[c, pl.ds(0, len(hops))], gr_a.at[e, c])
        for k in hops:
            to_partner(buf.at[c, same_core(k)], e, c)

    def gather_relay(buf, e, c, hops):
        wait_bytes(buf.at[c, pl.ds(0, len(hops))], gr_a.at[e, c])
        height = buf.shape[2]
        cut = height // 2 // 16 * 16
        for sign, part in ((1, pl.ds(0, cut)), (-1, pl.ds(cut, height - cut))):
            source = same_core(chips - 2 * sign)
            block = buf.at[c, source]
            remote(block, block, gs_f.at[e, c], gr_f.at[e, c], same_core(chips + sign)).start()
            half = buf.at[c, source, part]
            remote(half, half, gs_f.at[e, c], gr_f.at[e, c], same_core(chips + 2 * sign)).start()
        for k in hops:
            to_partner(buf.at[c, same_core(k)], e, c)

    def relay_forward(buf, e, c):
        wait_bytes(buf.at[c, pl.ds(0, len(far))], gr_f.at[e, c])
        for k in far:
            to_partner(buf.at[c, same_core(k)], e, c)

    def gather_wait(buf, e, c):
        wait_bytes(buf.at[c, pl.ds(0, chips)], gr_b.at[e, c])

    def gather_end(buf, e, c, hops):
        wait_bytes(buf.at[c, pl.ds(0, len(hops))], gs_a.at[e, c])
        wait_bytes(buf.at[c, pl.ds(0, chips)], gs_b.at[e, c])
        if hops is near:
            wait_bytes(buf.at[c, pl.ds(0, len(far))], gs_f.at[e, c])

    def rows_of(d, offset=0, height=None):
        return pl.ds(pl.multiple_of(d * blk + offset, 16), height or blk)

    def exchange_own(src, dst, index_of):
        dst[index_of(me)] = src[index_of(me)]

    def exchange_part(src, dst, e, c, index_of, hops):
        landing = dst.at[index_of(me)]
        for k in hops:
            for other in range(2):
                d = 2 * lax.rem(chip + k, chips) + (core + other) % 2
                if k or other:
                    remote(src.at[index_of(d)], landing, as_sem.at[e, c], ar_sem.at[e, c], d).start()

    def exchange_start(src, dst, e, c, index_of):
        exchange_own(src, dst, index_of)
        exchange_part(src, dst, e, c, index_of, steps + [0])

    def others(ref, c, planes):
        where = pl.ds(0, (n - 1) * blk)
        return ref.at[c, :, where, :] if planes else ref.at[c, where, :]

    def exchange_wait(dst, e, c, planes):
        wait_bytes(others(dst, c, planes), ar_sem.at[e, c])

    def exchange_end(src, e, c, planes):
        wait_bytes(others(src, c, planes), as_sem.at[e, c])

    def loop(count, body, unroll=1):
        def several(i, carry):
            for k in range(unroll):
                body(i * unroll + k)
            return carry
        lax.fori_loop(0, count // unroll, several, 0)

    def pack_bias(rows_f32):
        half = blk // 2
        last = jnp.concatenate([rows_f32[seg(g, half), 128:length] for g in range(2)], axis=1)
        return jnp.concatenate([rows_f32[:, 0:128], last, jnp.zeros((8, 128), F32)], axis=0).astype(BF16)

    tmp_b[:] = jnp.zeros_like(tmp_b)

    def row_bias(c):
        def one(i):
            tmp_b[pl.ds(pl.multiple_of(i * 8, 8), 8), :] = dot_nt(w_rb[:], layer_norm(z_ref[c, i]))
        loop(rows, one, U_LN)
        t = dot(p6[:], tmp_b[:].astype(BF16))
        for g, buf in enumerate(g_row):
            buf[c, me] = pack_bias(t[seg(g, blk), :])
    loop(crops, row_bias)
    pl.semaphore_wait(barrier, n - 1)

    def row_bias_send(c):
        for g, buf in enumerate(g_row):
            gather_start(buf, g, c, steps)
    loop(crops, row_bias_send)

    w_f32[:] = w_oo[:].astype(F32)
    for fp in range(HD // 2):
        for half in range(2):
            at = fp * 2 * HD + half * HD
            w_fe[at:at + HD, :] = w_f32[pl.ds(half * (HD // 2) + fp, HD, stride=HD), :]
    for b in range(HD * HD // 128):
        w_fet[:, seg(b, 128)] = w_fe[seg(b, 128), :].T.astype(BF16)
    q_s[:] = jnp.zeros_like(q_s)

    def unpack_bias(buf, c, perm, perm_last, pieces, piece):
        for sb in range(n // 4):
            moved = dot(perm[:], buf[c, seg(sb, 4), 0:blk, :].reshape(sup, 128)).astype(BF16)
            last = dot(perm_last[:], buf[c, seg(sb, 4), blk:, :].reshape(128, 128)).astype(BF16)
            for i in range(pieces):
                at = i * (4 * length // pieces) + sb * piece
                b_q[at:at + piece, 0:128] = moved[seg(i, piece), :]
                b_q[at:at + piece, 128:length] = last[seg(i % (pieces // 2), piece), seg(2 * i // pieces, 64)]

    def mask_columns(row, select):
        wide = jnp.broadcast_to(row.astype(F32), (128, length)).astype(BF16)
        return (dot_nt(select[:], wide) - 1.0) * (MASK_SCALE * LOG2E)

    scale = HD ** -0.5 * LOG2E
    two, four = 2 * length, 4 * length

    def project(y, w_t, first, stride=1):
        wide = y.shape[1]
        q = dot_nt(w_t[0:wide, :], jnp.concatenate([y, y], axis=0))
        q = jnp.where(same_half(wide, two, length), q, 0.0).astype(BF16)
        keys = dot_nt(y, w_t[wide:2 * wide, :]).astype(BF16)
        values = dot_nt(w_t[2 * wide:3 * wide, :], y).astype(BF16)
        gate = sigmoid(dot_nt(w_t[3 * wide:4 * wide, :], y))
        for g in range(wide // 128):
            u = first + g * stride
            q_s[u, 0:64, 0:two] = q[128 * g:128 * g + 64, :]
            q_s[u, 64:128, two:four] = q[128 * g + 64:128 * g + 128, :]
            k_s[u] = keys[:, seg(g, 128)]
            v_s[u] = values[seg(g, 128), :]
            g_s[u] = gate[seg(g, 128), :]

    def attend(first, count, bias_of):
        def mix(u, probs):
            pieces = []
            for p in range(2):
                mixed = dot(v_s[u, seg(p, 64), :], probs[:, seg(p, two)])
                pieces += [mixed[0:HD, 0:length], mixed[HD:2 * HD, length:two]]
            return jnp.concatenate(pieces, axis=0)

        def finish(u, mixed):
            o_s[u] = (g_s[u] * mixed).astype(BF16)

        s_buf[0] = dot(k_s[first], q_s[first])

        def pair(i):
            u = first + 2 * i
            s_buf[1] = dot(k_s[u + 1], q_s[u + 1])
            mixed = mix(u, softmax_cols(s_buf[0] * scale + bias_of(u)))
            after = jnp.minimum(u + 2, first + count - 1)
            s_buf[0] = dot(k_s[after], q_s[after])
            probs = softmax_cols(s_buf[1] * scale + bias_of(u + 1))
            finish(u, mixed)
            finish(u + 1, mix(u + 1, probs))
        loop(count // 2, pair, 2)

    groups = width // 128

    def row_attention(c):
        def before(s):
            m_s[s] = mask_columns(mm_ref[c, pl.ds(me * seqs + s, 1), :], eye)
            project(layer_norm(x_ref[c, s]), w_r, s, seqs)
        loop(seqs, before, U_PR)
        for g, buf in enumerate(g_row):
            gather_forward(buf, g, c, steps)
            gather_wait(buf, g, c)
            unpack_bias(buf, c, p4, p4b, 4, blk)
            for pair in range(2):
                bm_tri[:, seg(pair, two)] = dot_nt(eye[:], b_q[seg(pair, two), :]) * LOG2E

            def bias_of(u):
                return bm_tri[:] + jnp.concatenate([m_s[u - g * seqs]] * (four // 128), axis=1)
            attend(g * seqs, seqs, bias_of)

        def after(s):
            gated = jnp.concatenate([o_s[g * seqs + s] for g in range(groups)], axis=0)
            x1[s] = (x_ref[c, s].astype(F32) + dot_tn(gated, w_ro[:])).astype(BF16)
        loop(seqs, after, U_PO)
        for b in range(blocks):
            part = x1[:, seg(b, 64), :].reshape(256, width)
            s1[c, seg(b, 256), :] = dot(p2[:], part).astype(BF16)
        exchange_start(s1, r1, 0, c, lambda d: (c, rows_of(d)))
    loop(crops, row_attention)

    def send_back(c, hops):
        exchange_part(s2, r2, 1, c, lambda d: (c, rows_of(d)), hops)

    def columns(c):
        exchange_wait(r1, 0, c, False)
        for sb in range(n // 4):
            moved = dot(p3[:], r1[c, seg(sb, sup), :]).astype(BF16)
            for i in range(rows):
                y1[i, seg(sb, 16), :] = moved[seg(i, 16), :]
        n_seq = y1.shape[1]
        mk = mm_ref[c].astype(F32).astype(BF16)
        mine = (iota((16, length), 1) == me * rows + iota((16, length), 0)).astype(F32).astype(BF16)
        m_t[:] = dot_nt(mine, jnp.concatenate([mk, mk], axis=0))
        rn[c] = 1.0 / (dot(m_t[:, 0:n_seq].astype(BF16), mk) + OPM_EPS)
        low = iota((HD, 2 * n_seq), 1) < n_seq
        mask_all = (dot_nt(mk, mine) - 1.0) * (MASK_SCALE * LOG2E)
        for i in range(rows):
            mc_s[i] = jnp.broadcast_to(mask_all[:, i:i + 1], (n_seq, 128))
        tokens = 4 * n_seq

        def doubled(y):
            return jnp.concatenate([y[n_seq * (r // 2):n_seq * (r // 2 + 1), :] for r in range(8)], axis=0)

        def before(q):
            y = layer_norm(y1[pl.ds(4 * q, 4)].reshape(tokens, width))
            qq = dot_nt(w_c[0:width, :], doubled(y))
            qc_s[q] = jnp.where(same_half(width, 2 * tokens, n_seq), qq, 0.0).astype(BF16)
            kc_s[q] = dot_nt(y, w_c[width:2 * width, :]).astype(BF16)
            vc_s[q] = dot_nt(y, w_c[2 * width:3 * width, :]).astype(BF16)
            gc_s[q] = sigmoid(dot_nt(w_c[3 * width:4 * width, :], y))
        loop(quads, before, U_CP)

        @pl.when(c == 1)
        def _():
            gather_relay(g_c, 2, 0, near)
            send_back(0, middle_hops)

        def middle(q):
            zeros = jnp.zeros((64, 128), BF16)
            for g in range(groups):
                heads = [[] for _ in range(4)]
                for r in range(4):
                    at = n_seq * r
                    wide = qc_s[q, seg(g, 128), seg(r, 128)]
                    stacked = jnp.concatenate([jnp.concatenate([wide[0:64], zeros], axis=0),
                                               jnp.concatenate([zeros, wide[64:128]], axis=0)], axis=1)
                    logits = dot(kc_s[q, at:at + n_seq, seg(g, 128)], stacked)
                    col = mc_s[4 * q + r]
                    probs = softmax_cols(logits * scale + jnp.concatenate([col, col], axis=1))
                    mixed = dot_tn(vc_s[q, at:at + n_seq, seg(g, 128)], probs)
                    for h in range(4):
                        heads[h].append(mixed[seg(h, HD), seg(h, n_seq)])
                mixed = jnp.concatenate([jnp.concatenate(h, axis=1) for h in heads], axis=0)
                oc_s[q, seg(g, 128), :] = (gc_s[q, seg(g, 128), :] * mixed).astype(BF16)
        loop(quads, middle, U_CM)

        def after(q):
            update = dot_tn(oc_s[q], w_co[:])
            x = y1[pl.ds(4 * q, 4)].reshape(tokens, width).astype(F32)
            y1[pl.ds(4 * q, 4)] = (x + update).astype(BF16).reshape(4, n_seq, width)
        loop(quads, after, U_CF)

        @pl.when(c == 1)
        def _():
            relay_forward(g_c, 2, 0)

        def factors(q):
            y = layer_norm(y1[pl.ds(4 * q, 4)].reshape(tokens, width))
            all_four = dot_nt(w_ac[:], doubled(y)).astype(BF16).astype(F32)
            half = HD // 2
            for r in range(4):
                i = 4 * q + r
                both = all_four[:, seg(r, 128)] * m_t[pl.ds(i, 1), :]
                a = both[0:HD, :]
                at = pl.ds(pl.multiple_of(i * HD, HD), HD)
                a_t[c, 0, at, :] = jnp.where(low, a, 0.0).astype(BF16)
                a_t[c, 1, at, :] = jnp.where(low, 0.0, a).astype(BF16)
                packed = jnp.where(low[0:half], both[HD:HD + half, :], both[HD + half:2 * HD, :])
                c_t[pl.ds(pl.multiple_of(i * half, half), half), :] = packed.astype(BF16)
        loop(quads, factors, U_CF)
        g_c[c, me] = dot(p5[:], c_t[:]).astype(BF16)
        gather_start(g_c, 2, c, near)
        for db in range(n // 4):
            part = y1[:, seg(db, 16), :].reshape(16 * rows, width)
            s2[c, seg(db, sup), :] = dot(p3t[:], part).astype(BF16)
        exchange_own(s2, r2, lambda d: (c, rows_of(d)))

        @pl.when(c == 0)
        def _():
            send_back(0, near)

        @pl.when(c == 1)
        def _():
            send_back(0, last_hops)
    loop(crops, columns)

    def bias_row(i, y, w_b):
        tmp_b[pl.ds(pl.multiple_of(i * 8, 8), 4), :] = dot_nt(w_b[:], y)

    def bias_send(buf, e, c, hops):
        buf[c, me] = pack_bias(dot(p6[0:blk, :], tmp_b[:].astype(BF16)))
        gather_start(buf, e, c, hops)

    def start_project(c):
        loop(rows, lambda i: project(yn[c, i], w_ts, i), U_TP)

    def outer(c):
        gather_wait(g_c, 2, c)

        def unpack(q):
            for sb in range(n // 4):
                part = g_c[c, 4 * sb:4 * sb + 4, pl.ds(pl.multiple_of(blk * q, 16), blk), :].reshape(sup, 128)
                moved = dot(p4[:], part).astype(BF16)
                for i in range(4):
                    c_f[4 * q + i, seg(sb, blk), :] = moved[seg(i, blk), :]
        loop(HD // 2 // 4, unpack, U_UNP)

        def products(fp):
            for half in range(2):
                u = dot_nt(a_t[c, half], c_f[fp])
                for i in range(rows):
                    at = pl.ds(pl.multiple_of(fp * 2 * HD + half * HD, HD), HD)
                    u_s[i, at, :] = (u[seg(i, HD), :] * rn[c, i:i + 1, :]).astype(BF16)
        loop(HD // 2, products, U_PROD)

        @pl.when(c == 1)
        def _():
            send_back(1, last_hops)

        def one(i):
            update = dot(w_fet[:], u_s[i])
            z1[c, i] = (z_ref[c, i].astype(F32) + update.T).astype(BF16)
        loop(rows, one, U_OUT)

        @pl.when(c == 0)
        def _():
            gather_relay(g_c, 2, 1, near)
            send_back(1, near)

        def norm(i):
            y = layer_norm(z1[c, i])
            yn[c, i] = y
            bias_row(i, y, w_tsb)
        loop(rows, norm, U_LN)

        @pl.when(c == 0)
        def _():
            start_project(0)
            relay_forward(g_c, 2, 1)
        bias_send(g_t1, 3, c, steps)

        @pl.when(c == 0)
        def _():
            send_back(1, middle_hops)

        @pl.when(c == 1)
        def _():
            gather_forward(g_t1, 3, 0, steps)
    loop(crops, outer)

    def triangle(c, w_out, done):
        def quad(q):
            attend(4 * q, 4, lambda u: bm_tri[:])

            def after(k):
                i = 4 * q + k
                x3[i] = (z1[c, i].astype(F32) + dot_tn(o_s[i], w_out[:])).astype(BF16)
            loop(4, after, 4)
            done(q)
        loop(quads, quad)

    def start_node(c):
        @pl.when(c == 1)
        def _():
            start_project(1)
            gather_forward(g_t1, 3, 1, steps)
        gather_wait(g_t1, 3, c)
        unpack_bias(g_t1, c, p4, p4b, 4, blk)
        col = mask_columns(rm_ref[pl.ds(c, 1), :], eye)
        col3 = jnp.concatenate([col] * (two // 128), axis=1)
        for pair in range(2):
            bm_tri[:, seg(pair, two)] = dot_nt(eye[:], b_q[seg(pair, two), :]) * LOG2E + col3

        def done(q):
            for k in range(4):
                i = 4 * q + k
                bias_row(i, layer_norm(x3[i]), w_teb)

            @pl.when(q == quads - 1)
            def _():
                bias_send(g_t2, 4, c, steps)
            for b in range(blocks):
                part = x3[pl.ds(4 * q, 4), seg(b, 64), :].reshape(256, 128)
                s3[c, q, seg(b, 256), :] = dot(p2[:], part).astype(BF16)
            exchange_start(s3, r3, 2, c, lambda d: (c, q, rows_of(d)))
        triangle(c, w_tso, done)
    loop(crops, start_node)

    def end_node(c):
        exchange_wait(r3, 2, c, True)
        for q in range(quads):
            for sb in range(n // 4):
                moved = dot(p3[:], r3[c, q, seg(sb, sup), :]).astype(BF16)
                for i in range(rows):
                    at = 64 * q + 16 * sb
                    z1[c, i, at:at + 16, :] = moved[seg(i, 16), :]
        loop(rows, lambda i: project(layer_norm(z1[c, i]), w_te, i), U_TP)
        gather_forward(g_t2, 4, c, steps)
        gather_wait(g_t2, 4, c)
        unpack_bias(g_t2, c, p4e, p4eb, 4 * quads, 16)
        col = mask_columns(rm_ref[pl.ds(c, 1), :], tok)
        col3 = jnp.concatenate([col] * (two // 128), axis=1)
        for pair in range(2):
            left = dot_nt(b_q[seg(2 * pair, length), :], tok_l[:])
            right = dot_nt(b_q[seg(2 * pair + 1, length), :], tok_r[:])
            bm_tri[:, seg(pair, two)] = (left + right) * LOG2E + col3

        def done(q):
            for p in range(quads):
                for db in range(n // 4):
                    part = x3[pl.ds(4 * q, 4), 64 * p + 16 * db:64 * p + 16 * (db + 1), :].reshape(64, 128)
                    moved = dot(p64[:], part).astype(BF16)
                    for i in range(4):
                        s4[c, p, rows_of(4 * db + i, 16 * q, 16), :] = moved[seg(i, 16), :]
            exchange_start(s4, r4, 3, c, lambda d: (c, slice(None), rows_of(d, 16 * q, 16)))
        triangle(c, w_teo, done)
    loop(crops, end_node)

    def finish_msa(c):
        exchange_wait(r2, 1, c, False)
        for b in range(blocks):
            moved = dot(p2t[:], r2[c, seg(b, 256), :]).astype(BF16)
            for i in range(seqs):
                out_m[c, i, seg(b, 64), :] = moved[seg(i, 64), :]
    loop(crops, finish_msa)

    def finish_pair(c):
        exchange_wait(r4, 3, c, True)
        for q in range(quads):
            for b in range(blocks):
                moved = dot(p2t[:], r4[c, q, seg(b, 256), :]).astype(BF16)
                for i in range(4):
                    out_z[c, 4 * q + i, seg(b, 64), :] = moved[seg(i, 64), :]
    loop(crops, finish_pair)

    def drain(c):
        for e, (buf, hops) in enumerate([(b, steps) for b in g_row] + [(g_c, near), (g_t1, steps), (g_t2, steps)]):
            gather_end(buf, e, c, hops)
        for e, (buf, planes) in enumerate(((s1, False), (s2, False), (s3, True), (s4, True))):
            exchange_end(buf, e, c, planes)
    loop(crops, drain)


def solution(mesh):
    n = mesh.shape[GROUP_AXIS]
    rows_spec = P(PART_AXIS, GROUP_AXIS, None, None)
    in_specs = (rows_spec, rows_spec, P(PART_AXIS, None, None), P(PART_AXIS, None)) + (P(),) * N_WEIGHTS

    def local_block(msa, pair, msa_mask, res_mask, *weights):
        (w_rb, w_r, w_ro, w_c, w_co, w_ac, w_oo, w_tsb, w_ts, w_tso, w_teb, w_te, w_teo) = weights
        crops, seqs, length, width = msa.shape
        rows, pair_width = pair.shape[1], pair.shape[3]
        n_seq = msa_mask.shape[1]
        heads, tri_heads = w_r.shape[2], w_ts.shape[2]
        quads = rows // 4

        def flat_t(w):
            return jnp.transpose(w, (1, 2, 3, 0)).reshape(-1, w.shape[0])

        operands = [
            msa, pair, msa_mask, res_mask,
            w_rb.T, flat_t(w_r), w_ro.reshape(width, width), flat_t(w_c), w_co.reshape(width, width),
            jnp.transpose(w_ac, (1, 2, 0)).reshape(-1, width), w_oo.reshape(-1, pair_width),
            w_tsb.T, flat_t(w_ts), w_tso.reshape(pair_width, pair_width),
            w_teb.T, flat_t(w_te), w_teo.reshape(pair_width, pair_width),
        ]
        p2 = permutation((4, 64), (1, 0))
        p3 = permutation((4, rows, 4), (1, 0, 2))
        p4 = permutation((4, 4, rows), (1, 0, 2))
        p4e = permutation((4, 4, quads, 4), (1, 2, 0, 3))

        def last(p):
            half = p[:len(p) // 2].reshape(-1, 4, 4 * rows)[:, :, :2 * rows]
            return np.pad(half, ((0, 0), (0, 0), (0, 32 - 2 * rows))).reshape(len(p) // 2, -1)
        p5 = permutation((rows, HD // 2), (1, 0))
        p6 = permutation((rows, heads), (1, 0))
        p64 = permutation((4, 4, 4), (1, 0, 2))
        tok = permutation((n, quads, 4), (1, 0, 2))
        consts = [p2, p2.T, p3, p3.T, p4, last(p4), p4e, last(p4e), p5, p6, p64, np.eye(length), tok,
                  np.concatenate([tok, 0 * tok]), np.concatenate([0 * tok, tok])]
        operands += [jnp.asarray(a, BF16) for a in consts]

        vmem = pl.BlockSpec(memory_space=pltpu.VMEM)
        total = n * 4 * rows
        bias = pltpu.VMEM((crops, n, 4 * rows + 32, 128), BF16)
        scratch = [
            bias, bias,
            pltpu.VMEM((crops, n, HD // 2 * rows, 128), BF16),
            bias, bias,
        ]
        scratch += [pltpu.VMEM((crops, total, width), BF16)] * 4
        scratch += [pltpu.VMEM((crops, quads, total, pair_width), BF16)] * 4
        scratch += [
            pltpu.VMEM((8 * rows, length), F32),
            pltpu.VMEM((tri_heads * length, length), BF16),
            pltpu.VMEM((length, tri_heads * length), F32),
            pltpu.VMEM((seqs, length, width), BF16),
            pltpu.VMEM((rows, n_seq, width), BF16),
            pltpu.VMEM((16, 2 * n_seq), F32),
            pltpu.VMEM((crops, 16, length), F32),
            pltpu.VMEM((crops, 2, rows * HD, 128), BF16),
            pltpu.VMEM((rows * HD // 2, 128), BF16),
            pltpu.VMEM((HD // 2, length, 128), BF16),
            pltpu.VMEM((rows, HD * HD, length), BF16),
            pltpu.VMEM((HD * HD, pair_width), F32),
            pltpu.VMEM((HD * HD, pair_width), F32),
            pltpu.VMEM((pair_width, HD * HD), BF16),
            pltpu.VMEM((crops, rows, length, pair_width), BF16),
            pltpu.VMEM((crops, rows, length, pair_width), BF16),
            pltpu.VMEM((rows, length, pair_width), BF16),
            pltpu.VMEM((rows, 128, 4 * length), BF16),
            pltpu.VMEM((rows, length, 128), BF16),
            pltpu.VMEM((rows, 128, length), BF16),
            pltpu.VMEM((rows, 128, length), F32),
            pltpu.VMEM((rows, 128, length), BF16),
            pltpu.VMEM((2, length, 4 * length), F32),
            pltpu.VMEM((seqs, length, 128), F32),
            pltpu.VMEM((quads, width, 8 * n_seq), BF16),
            pltpu.VMEM((quads, 4 * n_seq, width), BF16),
            pltpu.VMEM((quads, 4 * n_seq, width), BF16),
            pltpu.VMEM((quads, width, 4 * n_seq), F32),
            pltpu.VMEM((quads, width, 4 * n_seq), BF16),
            pltpu.VMEM((rows, n_seq, 128), F32),
        ]
        scratch += [pltpu.SemaphoreType.DMA((5, crops))] * 8
        return pl.pallas_call(
            functools.partial(block_kernel, n),
            out_shape=(jax.ShapeDtypeStruct(msa.shape, BF16), jax.ShapeDtypeStruct(pair.shape, BF16)),
            in_specs=[vmem] * len(operands),
            out_specs=(vmem, vmem),
            scratch_shapes=scratch,
            compiler_params=pltpu.CompilerParams(collective_id=0, has_side_effects=True, vmem_limit_bytes=VMEM_BYTES),
            name='evoformer_block',
        )(*operands)

    return jax.shard_map(local_block, mesh=mesh, in_specs=in_specs, out_specs=(rows_spec, rows_spec),
                         check_vma=False)
```

```python
import functools
import math

import jax
import jax.numpy as jnp
import numpy as np
from jax import lax
from jax.experimental import pallas as pl
from jax.experimental.pallas import tpu as pltpu
from jax.sharding import PartitionSpec as P

MASK_SCALE = 10000.0
LN_EPS = 1e-5
OPM_EPS = 1e-3
LOG2E = math.log2(math.e)
N_WEIGHTS = 13
PART_AXIS = 'data'
GROUP_AXIS = 'dap'
MESH = pl.DeviceIdType.MESH
F32 = jnp.float32
BF16 = jnp.bfloat16
HD = 32
U_LN, U_UNP, U_PROD, U_OUT = 12, 2, 4, 3
U_PR, U_PO, U_TP, U_CP, U_CM, U_CF = 2, 4, 3, 3, 3, 3
VMEM_BYTES = 60 * 1024 * 1024


def dot(a, b):
    return lax.dot(a, b, preferred_element_type=F32)


def dot_nt(a, b):
    return lax.dot_general(a, b, (((1,), (1,)), ((), ())), preferred_element_type=F32)


def dot_tn(a, b):
    return lax.dot_general(a, b, (((0,), (0,)), ((), ())), preferred_element_type=F32)


def layer_norm(x):
    x_float = x.astype(F32)
    centred = x_float - jnp.mean(x_float, axis=-1, keepdims=True)
    var = jnp.mean(centred * centred, axis=-1, keepdims=True)
    return (centred * lax.rsqrt(var + LN_EPS)).astype(BF16)


def seg(i, size):
    return slice(i * size, (i + 1) * size)


def sigmoid(x):
    return 1.0 / (1.0 + jnp.exp2(x * (-LOG2E)))


def iota(shape, dim):
    return lax.broadcasted_iota(jnp.int32, shape, dim)


def permutation(sizes, order, keep=None):
    total = int(np.prod(sizes))
    source = np.arange(total).reshape(sizes).transpose(order).reshape(-1)
    out = np.zeros((total, total), np.float32)
    out[np.arange(total), source] = 1.0
    return out


def softmax_cols(t):
    e = jnp.exp2(t - jnp.max(t, axis=0, keepdims=True))
    return (e * (1.0 / jnp.sum(e, axis=0, keepdims=True))).astype(BF16)


def same_half(width, lanes, half):
    return (iota((width, lanes), 0) // HD) % 2 == (iota((width, lanes), 1) // half) % 2


def staged_kernel(n, early, n_in, *refs):
    operands, rest = list(refs[:n_in]), refs[n_in:]
    late = [i for i in range(n_in) if i not in early]
    landing, sems = rest[-len(late) - 1:-1], rest[-1]
    copies = [pltpu.make_async_copy(operands[i], landing[k], sems.at[k]) for k, i in enumerate(late)]
    for copy in copies:
        copy.start()
    for k, i in enumerate(late):
        operands[i] = landing[k]

    def arrive():
        for copy in copies:
            copy.wait()
    block_kernel(n, arrive, *operands, *rest[:-len(late) - 1])


def block_kernel(n, arrive, x_ref, z_ref, mm_ref, rm_ref,
                 w_rb, w_r, w_ro, w_c, w_co, w_ac, w_oo, w_tsb, w_ts, w_tso, w_teb, w_te, w_teo,
                 p2, p2t, p3, p3t, p4, p4b, p4e, p4eb, p5, p6, p64, eye, tok, tok_l, tok_r,
                 out_m, out_z,
                 g_r0, g_r1, g_c, g_t1, g_t2, s1, r1, s2, r2, s3, r3, s4, r4,
                 tmp_b, b_q, bm_tri, x1, y1, m_t, rn, a_t, c_t, c_f, u_s, w_f32, w_fe, w_fet, z1, yn, x3,
                 q_s, k_s, v_s, g_s, o_s, s_buf, m_s, qc_s, kc_s, vc_s, gc_s, oc_s, mc_s,
                 gs_a, gr_a, gs_b, gr_b, gs_f, gr_f, as_sem, ar_sem):
    me = lax.axis_index(GROUP_AXIS)
    g_row = (g_r0, g_r1)
    chips = n // 2
    chip = me // 2
    core = me % 2
    partner = me + 1 - 2 * core
    crops, seqs, length, width = x_ref.shape
    rows = z_ref.shape[1]
    quads = rows // 4
    blocks = length // 64
    blk = 4 * rows
    sup = 4 * blk
    steps = []
    for k in reversed(range(chips // 2)):
        steps += sorted({k + 1, chips - k - 1}, reverse=True)
    near = (2, chips - 2, 1, chips - 1)
    far = tuple(k for k in steps if k not in near)
    middle_hops, last_hops = far[1:], far[:1] + (0,)

    barrier = pltpu.get_barrier_semaphore()
    for k in range(1, n):
        pl.semaphore_signal(barrier, inc=1, device_id={GROUP_AXIS: lax.rem(me + k, n)}, device_id_type=MESH)
    def remote(src, dst, send, recv, device):
        return pltpu.make_async_remote_copy(src_ref=src, dst_ref=dst, send_sem=send, recv_sem=recv,
                                            device_id={GROUP_AXIS: device}, device_id_type=MESH)

    def same_core(k):
        return 2 * lax.rem(chip + k, chips) + core

    def wait_bytes(ref, sem):
        pltpu.make_async_copy(ref, ref, sem).wait()

    def to_partner(block, e, c):
        remote(block, block, gs_b.at[e, c], gr_b.at[e, c], partner).start()

    def gather_start(buf, e, c, hops):
        mine = buf.at[c, me]
        for k in hops:
            remote(mine, mine, gs_a.at[e, c], gr_a.at[e, c], same_core(k)).start()
        to_partner(mine, e, c)

    def gather_forward(buf, e, c, hops):
        wait_bytes(buf.at[c, pl.ds(0, len(hops))], gr_a.at[e, c])
        for k in hops:
            to_partner(buf.at[c, same_core(k)], e, c)

    def gather_relay(buf, e, c, hops):
        wait_bytes(buf.at[c, pl.ds(0, len(hops))], gr_a.at[e, c])
        height = buf.shape[2]
        cut = height // 2 // 16 * 16
        for sign, part in ((1, pl.ds(0, cut)), (-1, pl.ds(cut, height - cut))):
            source = same_core(chips - 2 * sign)
            block = buf.at[c, source]
            remote(block, block, gs_f.at[e, c], gr_f.at[e, c], same_core(chips + sign)).start()
            half = buf.at[c, source, part]
            remote(half, half, gs_f.at[e, c], gr_f.at[e, c], same_core(chips + 2 * sign)).start()
        for k in hops:
            to_partner(buf.at[c, same_core(k)], e, c)

    def relay_forward(buf, e, c):
        wait_bytes(buf.at[c, pl.ds(0, len(far))], gr_f.at[e, c])
        for k in far:
            to_partner(buf.at[c, same_core(k)], e, c)

    def gather_wait(buf, e, c):
        wait_bytes(buf.at[c, pl.ds(0, chips)], gr_b.at[e, c])

    def gather_end(buf, e, c, hops):
        wait_bytes(buf.at[c, pl.ds(0, len(hops))], gs_a.at[e, c])
        wait_bytes(buf.at[c, pl.ds(0, chips)], gs_b.at[e, c])
        if hops is near:
            wait_bytes(buf.at[c, pl.ds(0, len(far))], gs_f.at[e, c])

    def rows_of(d, offset=0, height=None):
        return pl.ds(pl.multiple_of(d * blk + offset, 16), height or blk)

    def exchange_own(src, dst, index_of):
        dst[index_of(me)] = src[index_of(me)]

    def exchange_part(src, dst, e, c, index_of, hops):
        landing = dst.at[index_of(me)]
        for k in hops:
            for other in range(2):
                d = 2 * lax.rem(chip + k, chips) + (core + other) % 2
                if k or other:
                    remote(src.at[index_of(d)], landing, as_sem.at[e, c], ar_sem.at[e, c], d).start()

    def exchange_start(src, dst, e, c, index_of):
        exchange_own(src, dst, index_of)
        exchange_part(src, dst, e, c, index_of, steps + [0])

    def others(ref, c, planes):
        where = pl.ds(0, (n - 1) * blk)
        return ref.at[c, :, where, :] if planes else ref.at[c, where, :]

    def exchange_wait(dst, e, c, planes):
        wait_bytes(others(dst, c, planes), ar_sem.at[e, c])

    def exchange_end(src, e, c, planes):
        wait_bytes(others(src, c, planes), as_sem.at[e, c])

    def loop(count, body, unroll=1):
        def several(i, carry):
            for k in range(unroll):
                body(i * unroll + k)
            return carry
        lax.fori_loop(0, count // unroll, several, 0)

    def pack_bias(rows_f32):
        half = blk // 2
        last = jnp.concatenate([rows_f32[seg(g, half), 128:length] for g in range(2)], axis=1)
        return jnp.concatenate([rows_f32[:, 0:128], last, jnp.zeros((8, 128), F32)], axis=0).astype(BF16)

    tmp_b[:] = jnp.zeros_like(tmp_b)

    def row_bias(c):
        def one(i):
            tmp_b[pl.ds(pl.multiple_of(i * 8, 8), 8), :] = dot_nt(w_rb[:], layer_norm(z_ref[c, i]))
        loop(rows, one, U_LN)
        t = dot(p6[:], tmp_b[:].astype(BF16))
        for g, buf in enumerate(g_row):
            buf[c, me] = pack_bias(t[seg(g, blk), :])
    loop(crops, row_bias)
    pl.semaphore_wait(barrier, n - 1)
    arrive()

    def row_bias_send(c):
        for g, buf in enumerate(g_row):
            gather_start(buf, g, c, steps)
    loop(crops, row_bias_send)

    w_f32[:] = w_oo[:].astype(F32)
    for fp in range(HD // 2):
        for half in range(2):
            at = fp * 2 * HD + half * HD
            w_fe[at:at + HD, :] = w_f32[pl.ds(half * (HD // 2) + fp, HD, stride=HD), :]
    for b in range(HD * HD // 128):
        w_fet[:, seg(b, 128)] = w_fe[seg(b, 128), :].T.astype(BF16)
    q_s[:] = jnp.zeros_like(q_s)

    def unpack_bias(buf, c, perm, perm_last, pieces, piece):
        for sb in range(n // 4):
            moved = dot(perm[:], buf[c, seg(sb, 4), 0:blk, :].reshape(sup, 128)).astype(BF16)
            last = dot(perm_last[:], buf[c, seg(sb, 4), blk:, :].reshape(128, 128)).astype(BF16)
            for i in range(pieces):
                at = i * (4 * length // pieces) + sb * piece
                b_q[at:at + piece, 0:128] = moved[seg(i, piece), :]
                b_q[at:at + piece, 128:length] = last[seg(i % (pieces // 2), piece), seg(2 * i // pieces, 64)]

    def mask_columns(row, select):
        wide = jnp.broadcast_to(row.astype(F32), (128, length)).astype(BF16)
        return (dot_nt(select[:], wide) - 1.0) * (MASK_SCALE * LOG2E)

    scale = HD ** -0.5 * LOG2E
    two, four = 2 * length, 4 * length

    def project(y, w_t, first, stride=1):
        wide = y.shape[1]
        q = dot_nt(w_t[0:wide, :], jnp.concatenate([y, y], axis=0))
        q = jnp.where(same_half(wide, two, length), q, 0.0).astype(BF16)
        keys = dot_nt(y, w_t[wide:2 * wide, :]).astype(BF16)
        values = dot_nt(w_t[2 * wide:3 * wide, :], y).astype(BF16)
        gate = sigmoid(dot_nt(w_t[3 * wide:4 * wide, :], y))
        for g in range(wide // 128):
            u = first + g * stride
            q_s[u, 0:64, 0:two] = q[128 * g:128 * g + 64, :]
            q_s[u, 64:128, two:four] = q[128 * g + 64:128 * g + 128, :]
            k_s[u] = keys[:, seg(g, 128)]
            v_s[u] = values[seg(g, 128), :]
            g_s[u] = gate[seg(g, 128), :]

    def attend(first, count, bias_of):
        def mix(u, probs):
            pieces = []
            for p in range(2):
                mixed = dot(v_s[u, seg(p, 64), :], probs[:, seg(p, two)])
                pieces += [mixed[0:HD, 0:length], mixed[HD:2 * HD, length:two]]
            return jnp.concatenate(pieces, axis=0)

        def finish(u, mixed):
            o_s[u] = (g_s[u] * mixed).astype(BF16)

        s_buf[0] = dot(k_s[first], q_s[first])

        def pair(i):
            u = first + 2 * i
            s_buf[1] = dot(k_s[u + 1], q_s[u + 1])
            mixed = mix(u, softmax_cols(s_buf[0] * scale + bias_of(u)))
            after = jnp.minimum(u + 2, first + count - 1)
            s_buf[0] = dot(k_s[after], q_s[after])
            probs = softmax_cols(s_buf[1] * scale + bias_of(u + 1))
            finish(u, mixed)
            finish(u + 1, mix(u + 1, probs))
        loop(count // 2, pair, 2)

    groups = width // 128

    def row_attention(c):
        def before(s):
            m_s[s] = mask_columns(mm_ref[c, pl.ds(me * seqs + s, 1), :], eye)
            project(layer_norm(x_ref[c, s]), w_r, s, seqs)
        loop(seqs, before, U_PR)
        for g, buf in enumerate(g_row):
            gather_forward(buf, g, c, steps)
            gather_wait(buf, g, c)
            unpack_bias(buf, c, p4, p4b, 4, blk)
            for pair in range(2):
                bm_tri[:, seg(pair, two)] = dot_nt(eye[:], b_q[seg(pair, two), :]) * LOG2E

            def bias_of(u):
                return bm_tri[:] + jnp.concatenate([m_s[u - g * seqs]] * (four // 128), axis=1)
            attend(g * seqs, seqs, bias_of)

        def after(s):
            gated = jnp.concatenate([o_s[g * seqs + s] for g in range(groups)], axis=0)
            x1[s] = (x_ref[c, s].astype(F32) + dot_tn(gated, w_ro[:])).astype(BF16)
        loop(seqs, after, U_PO)
        for b in range(blocks):
            part = x1[:, seg(b, 64), :].reshape(256, width)
            s1[c, seg(b, 256), :] = dot(p2[:], part).astype(BF16)
        exchange_start(s1, r1, 0, c, lambda d: (c, rows_of(d)))
    loop(crops, row_attention)

    def send_back(c, hops):
        exchange_part(s2, r2, 1, c, lambda d: (c, rows_of(d)), hops)

    def columns(c):
        exchange_wait(r1, 0, c, False)
        for sb in range(n // 4):
            moved = dot(p3[:], r1[c, seg(sb, sup), :]).astype(BF16)
            for i in range(rows):
                y1[i, seg(sb, 16), :] = moved[seg(i, 16), :]
        n_seq = y1.shape[1]
        mk = mm_ref[c].astype(F32).astype(BF16)
        mine = (iota((16, length), 1) == me * rows + iota((16, length), 0)).astype(F32).astype(BF16)
        m_t[:] = dot_nt(mine, jnp.concatenate([mk, mk], axis=0))
        rn[c] = 1.0 / (dot(m_t[:, 0:n_seq].astype(BF16), mk) + OPM_EPS)
        low = iota((HD, 2 * n_seq), 1) < n_seq
        mask_all = (dot_nt(mk, mine) - 1.0) * (MASK_SCALE * LOG2E)
        for i in range(rows):
            mc_s[i] = jnp.broadcast_to(mask_all[:, i:i + 1], (n_seq, 128))
        tokens = 4 * n_seq

        def doubled(y):
            return jnp.concatenate([y[n_seq * (r // 2):n_seq * (r // 2 + 1), :] for r in range(8)], axis=0)

        def before(q):
            y = layer_norm(y1[pl.ds(4 * q, 4)].reshape(tokens, width))
            qq = dot_nt(w_c[0:width, :], doubled(y))
            qc_s[q] = jnp.where(same_half(width, 2 * tokens, n_seq), qq, 0.0).astype(BF16)
            kc_s[q] = dot_nt(y, w_c[width:2 * width, :]).astype(BF16)
            vc_s[q] = dot_nt(y, w_c[2 * width:3 * width, :]).astype(BF16)
            gc_s[q] = sigmoid(dot_nt(w_c[3 * width:4 * width, :], y))
        loop(quads, before, U_CP)

        @pl.when(c == 1)
        def _():
            gather_relay(g_c, 2, 0, near)
            send_back(0, middle_hops)

        def middle(q):
            zeros = jnp.zeros((64, 128), BF16)
            for g in range(groups):
                heads = [[] for _ in range(4)]
                for r in range(4):
                    at = n_seq * r
                    wide = qc_s[q, seg(g, 128), seg(r, 128)]
                    stacked = jnp.concatenate([jnp.concatenate([wide[0:64], zeros], axis=0),
                                               jnp.concatenate([zeros, wide[64:128]], axis=0)], axis=1)
                    logits = dot(kc_s[q, at:at + n_seq, seg(g, 128)], stacked)
                    col = mc_s[4 * q + r]
                    probs = softmax_cols(logits * scale + jnp.concatenate([col, col], axis=1))
                    mixed = dot_tn(vc_s[q, at:at + n_seq, seg(g, 128)], probs)
                    for h in range(4):
                        heads[h].append(mixed[seg(h, HD), seg(h, n_seq)])
                mixed = jnp.concatenate([jnp.concatenate(h, axis=1) for h in heads], axis=0)
                oc_s[q, seg(g, 128), :] = (gc_s[q, seg(g, 128), :] * mixed).astype(BF16)
        loop(quads, middle, U_CM)

        def after(q):
            update = dot_tn(oc_s[q], w_co[:])
            x = y1[pl.ds(4 * q, 4)].reshape(tokens, width).astype(F32)
            y1[pl.ds(4 * q, 4)] = (x + update).astype(BF16).reshape(4, n_seq, width)
        loop(quads, after, U_CF)

        def factors(q):
            y = layer_norm(y1[pl.ds(4 * q, 4)].reshape(tokens, width))
            all_four = dot_nt(w_ac[:], doubled(y)).astype(BF16).astype(F32)
            half = HD // 2
            for r in range(4):
                i = 4 * q + r
                both = all_four[:, seg(r, 128)] * m_t[pl.ds(i, 1), :]
                a = both[0:HD, :]
                at = pl.ds(pl.multiple_of(i * HD, HD), HD)
                a_t[c, 0, at, :] = jnp.where(low, a, 0.0).astype(BF16)
                a_t[c, 1, at, :] = jnp.where(low, 0.0, a).astype(BF16)
                packed = jnp.where(low[0:half], both[HD:HD + half, :], both[HD + half:2 * HD, :])
                c_t[pl.ds(pl.multiple_of(i * half, half), half), :] = packed.astype(BF16)
        loop(quads, factors, U_CF)
        g_c[c, me] = dot(p5[:], c_t[:]).astype(BF16)
        gather_start(g_c, 2, c, near)
        for db in range(n // 4):
            part = y1[:, seg(db, 16), :].reshape(16 * rows, width)
            s2[c, seg(db, sup), :] = dot(p3t[:], part).astype(BF16)
        exchange_own(s2, r2, lambda d: (c, rows_of(d)))

        @pl.when(c == 0)
        def _():
            send_back(0, near)

        @pl.when(c == 1)
        def _():
            send_back(0, last_hops)
    loop(crops, columns)

    def bias_row(i, y, w_b):
        tmp_b[pl.ds(pl.multiple_of(i * 8, 8), 4), :] = dot_nt(w_b[:], y)

    def bias_send(buf, e, c, hops):
        buf[c, me] = pack_bias(dot(p6[0:blk, :], tmp_b[:].astype(BF16)))
        gather_start(buf, e, c, hops)

    def start_project(c):
        loop(rows, lambda i: project(yn[c, i], w_ts, i), U_TP)

    def outer(c):
        @pl.when(c == 0)
        def _():
            relay_forward(g_c, 2, 0)
        gather_wait(g_c, 2, c)

        def unpack(q):
            for sb in range(n // 4):
                part = g_c[c, 4 * sb:4 * sb + 4, pl.ds(pl.multiple_of(blk * q, 16), blk), :].reshape(sup, 128)
                moved = dot(p4[:], part).astype(BF16)
                for i in range(4):
                    c_f[4 * q + i, seg(sb, blk), :] = moved[seg(i, blk), :]
        loop(HD // 2 // 4, unpack, U_UNP)

        def products(fp):
            for half in range(2):
                u = dot_nt(a_t[c, half], c_f[fp])
                for i in range(rows):
                    at = pl.ds(pl.multiple_of(fp * 2 * HD + half * HD, HD), HD)
                    u_s[i, at, :] = (u[seg(i, HD), :] * rn[c, i:i + 1, :]).astype(BF16)
        loop(HD // 2, products, U_PROD)

        @pl.when(c == 1)
        def _():
            send_back(1, last_hops)

        def one(i):
            update = dot(w_fet[:], u_s[i])
            z1[c, i] = (z_ref[c, i].astype(F32) + update.T).astype(BF16)
        loop(rows, one, U_OUT)

        @pl.when(c == 0)
        def _():
            gather_relay(g_c, 2, 1, near)
            send_back(1, near)

        def norm(i):
            y = layer_norm(z1[c, i])
            yn[c, i] = y
            bias_row(i, y, w_tsb)
        loop(rows, norm, U_LN)

        @pl.when(c == 0)
        def _():
            start_project(0)
            relay_forward(g_c, 2, 1)
        bias_send(g_t1, 3, c, steps)

        @pl.when(c == 0)
        def _():
            send_back(1, middle_hops)

        @pl.when(c == 1)
        def _():
            gather_forward(g_t1, 3, 0, steps)
    loop(crops, outer)

    def relay_bias_at(turn, q, c):
        pl.when(turn & (q == 0))(lambda: gather_relay(g_t2, 4, c, near))

    def triangle(c, w_out, done):
        def quad(q):
            attend(4 * q, 4, lambda u: bm_tri[:])

            def after(k):
                i = 4 * q + k
                x3[i] = (z1[c, i].astype(F32) + dot_tn(o_s[i], w_out[:])).astype(BF16)
            loop(4, after, 4)
            done(q)
        loop(quads, quad)

    def start_node(c):
        @pl.when(c == 1)
        def _():
            start_project(1)
            gather_forward(g_t1, 3, 1, steps)
        gather_wait(g_t1, 3, c)
        unpack_bias(g_t1, c, p4, p4b, 4, blk)
        col = mask_columns(rm_ref[pl.ds(c, 1), :], eye)
        col3 = jnp.concatenate([col] * (two // 128), axis=1)
        for pair in range(2):
            bm_tri[:, seg(pair, two)] = dot_nt(eye[:], b_q[seg(pair, two), :]) * LOG2E + col3

        def done(q):
            for k in range(4):
                i = 4 * q + k
                bias_row(i, layer_norm(x3[i]), w_teb)

            @pl.when(q == quads - 1)
            def _():
                bias_send(g_t2, 4, c, near)
            for b in range(blocks):
                part = x3[pl.ds(4 * q, 4), seg(b, 64), :].reshape(256, 128)
                s3[c, q, seg(b, 256), :] = dot(p2[:], part).astype(BF16)
            relay_bias_at(c == 1, q, 0)
            exchange_start(s3, r3, 2, c, lambda d: (c, q, rows_of(d)))
        triangle(c, w_tso, done)
    loop(crops, start_node)

    def end_node(c):
        exchange_wait(r3, 2, c, True)
        for q in range(quads):
            for sb in range(n // 4):
                moved = dot(p3[:], r3[c, q, seg(sb, sup), :]).astype(BF16)
                for i in range(rows):
                    at = 64 * q + 16 * sb
                    z1[c, i, at:at + 16, :] = moved[seg(i, 16), :]
        loop(rows, lambda i: project(layer_norm(z1[c, i]), w_te, i), U_TP)
        relay_forward(g_t2, 4, c)
        gather_wait(g_t2, 4, c)
        unpack_bias(g_t2, c, p4e, p4eb, 4 * quads, 16)
        col = mask_columns(rm_ref[pl.ds(c, 1), :], tok)
        col3 = jnp.concatenate([col] * (two // 128), axis=1)
        for pair in range(2):
            left = dot_nt(b_q[seg(2 * pair, length), :], tok_l[:])
            right = dot_nt(b_q[seg(2 * pair + 1, length), :], tok_r[:])
            bm_tri[:, seg(pair, two)] = (left + right) * LOG2E + col3

        def done(q):
            for p in range(quads):
                for db in range(n // 4):
                    part = x3[pl.ds(4 * q, 4), 64 * p + 16 * db:64 * p + 16 * (db + 1), :].reshape(64, 128)
                    moved = dot(p64[:], part).astype(BF16)
                    for i in range(4):
                        s4[c, p, rows_of(4 * db + i, 16 * q, 16), :] = moved[seg(i, 16), :]
            relay_bias_at(c == 0, q, 1)
            exchange_start(s4, r4, 3, c, lambda d: (c, slice(None), rows_of(d, 16 * q, 16)))
        triangle(c, w_teo, done)
    loop(crops, end_node)

    def finish_msa(c):
        exchange_wait(r2, 1, c, False)
        for b in range(blocks):
            moved = dot(p2t[:], r2[c, seg(b, 256), :]).astype(BF16)
            for i in range(seqs):
                out_m[c, i, seg(b, 64), :] = moved[seg(i, 64), :]
    loop(crops, finish_msa)

    def finish_pair(c):
        exchange_wait(r4, 3, c, True)
        for q in range(quads):
            for b in range(blocks):
                moved = dot(p2t[:], r4[c, q, seg(b, 256), :]).astype(BF16)
                for i in range(4):
                    out_z[c, 4 * q + i, seg(b, 64), :] = moved[seg(i, 64), :]
    loop(crops, finish_pair)

    def drain(c):
        for e, (buf, hops) in enumerate([(b, steps) for b in g_row] + [(g_c, near), (g_t1, steps), (g_t2, near)]):
            gather_end(buf, e, c, hops)
        for e, (buf, planes) in enumerate(((s1, False), (s2, False), (s3, True), (s4, True))):
            exchange_end(buf, e, c, planes)
    loop(crops, drain)


def solution(mesh):
    n = mesh.shape[GROUP_AXIS]
    rows_spec = P(PART_AXIS, GROUP_AXIS)
    in_specs = (rows_spec, rows_spec, P(PART_AXIS), P(PART_AXIS)) + (P(),) * N_WEIGHTS

    def local_block(msa, pair, msa_mask, res_mask, *weights):
        (w_rb, w_r, w_ro, w_c, w_co, w_ac, w_oo, w_tsb, w_ts, w_tso, w_teb, w_te, w_teo) = weights
        crops, seqs, length, width = msa.shape
        rows, pair_width = pair.shape[1], pair.shape[3]
        n_seq = msa_mask.shape[1]
        heads, tri_heads = w_r.shape[2], w_ts.shape[2]
        quads = rows // 4

        def flat_t(w):
            return jnp.transpose(w, (1, 2, 3, 0)).reshape(-1, w.shape[0])

        bias_t = w_rb.T
        operands = [
            msa, pair, msa_mask, res_mask,
            bias_t, flat_t(w_r), w_ro.reshape(width, width), flat_t(w_c), w_co.reshape(width, width),
            jnp.transpose(w_ac, (1, 2, 0)).reshape(-1, width), w_oo.reshape(-1, pair_width),
            w_tsb.T, flat_t(w_ts), w_tso.reshape(pair_width, pair_width),
            w_teb.T, flat_t(w_te), w_teo.reshape(pair_width, pair_width),
        ]
        p2 = permutation((4, 64), (1, 0))
        p3 = permutation((4, rows, 4), (1, 0, 2))
        p4 = permutation((4, 4, rows), (1, 0, 2))
        p4e = permutation((4, 4, quads, 4), (1, 2, 0, 3))

        def last(p):
            half = p[:len(p) // 2].reshape(-1, 4, 4 * rows)[:, :, :2 * rows]
            blank = np.zeros(half.shape[:2] + (32 - 2 * rows,))
            return np.concatenate([half, blank], axis=2).reshape(len(half), -1)
        p5 = permutation((rows, HD // 2), (1, 0))
        p6 = permutation((rows, heads), (1, 0))
        p64 = permutation((4, 4, 4), (1, 0, 2))
        tok = permutation((n, quads, 4), (1, 0, 2))
        consts = [p2, p2.T, p3, p3.T, p4, last(p4), p4e, last(p4e), p5, p6, p64, np.eye(length), tok,
                  np.concatenate([tok, 0 * tok]), np.concatenate([0 * tok, tok])]
        first_const, names = len(operands), [a is p6 for a in consts]
        operands += [jnp.asarray(a, BF16) for a in consts]

        vmem = pl.BlockSpec(memory_space=pltpu.VMEM)
        anywhere = pl.BlockSpec(memory_space=pl.ANY)
        early = tuple(i for i, a in enumerate(operands) if a is pair or a is bias_t or (i >= first_const and names[i - first_const]))
        total = n * 4 * rows
        bias = pltpu.VMEM((crops, n, 4 * rows + 32, 128), BF16)
        scratch = [
            bias, bias,
            pltpu.VMEM((crops, n, HD // 2 * rows, 128), BF16),
            bias, bias,
        ]
        scratch += [pltpu.VMEM((crops, total, width), BF16)] * 4
        scratch += [pltpu.VMEM((crops, quads, total, pair_width), BF16)] * 4
        scratch += [
            pltpu.VMEM((8 * rows, length), F32),
            pltpu.VMEM((tri_heads * length, length), BF16),
            pltpu.VMEM((length, tri_heads * length), F32),
            pltpu.VMEM((seqs, length, width), BF16),
            pltpu.VMEM((rows, n_seq, width), BF16),
            pltpu.VMEM((16, 2 * n_seq), F32),
            pltpu.VMEM((crops, 16, length), F32),
            pltpu.VMEM((crops, 2, rows * HD, 128), BF16),
            pltpu.VMEM((rows * HD // 2, 128), BF16),
            pltpu.VMEM((HD // 2, length, 128), BF16),
            pltpu.VMEM((rows, HD * HD, length), BF16),
            pltpu.VMEM((HD * HD, pair_width), F32),
            pltpu.VMEM((HD * HD, pair_width), F32),
            pltpu.VMEM((pair_width, HD * HD), BF16),
            pltpu.VMEM((crops, rows, length, pair_width), BF16),
            pltpu.VMEM((crops, rows, length, pair_width), BF16),
            pltpu.VMEM((rows, length, pair_width), BF16),
            pltpu.VMEM((rows, 128, 4 * length), BF16),
            pltpu.VMEM((rows, length, 128), BF16),
            pltpu.VMEM((rows, 128, length), BF16),
            pltpu.VMEM((rows, 128, length), F32),
            pltpu.VMEM((rows, 128, length), BF16),
            pltpu.VMEM((2, length, 4 * length), F32),
            pltpu.VMEM((seqs, length, 128), F32),
            pltpu.VMEM((quads, width, 8 * n_seq), BF16),
            pltpu.VMEM((quads, 4 * n_seq, width), BF16),
            pltpu.VMEM((quads, 4 * n_seq, width), BF16),
            pltpu.VMEM((quads, width, 4 * n_seq), F32),
            pltpu.VMEM((quads, width, 4 * n_seq), BF16),
            pltpu.VMEM((rows, n_seq, 128), F32),
        ]
        scratch += [pltpu.SemaphoreType.DMA((5, crops))] * 8
        late = [a for i, a in enumerate(operands) if i not in early]
        scratch += [pltpu.VMEM(a.shape, a.dtype) for a in late] + [pltpu.SemaphoreType.DMA((len(late),))]
        return pl.pallas_call(
            functools.partial(staged_kernel, n, early, len(operands)),
            out_shape=(jax.ShapeDtypeStruct(msa.shape, BF16), jax.ShapeDtypeStruct(pair.shape, BF16)),
            in_specs=[vmem if i in early else anywhere for i in range(len(operands))],
            out_specs=(vmem, vmem),
            scratch_shapes=scratch,
            compiler_params=pltpu.CompilerParams(collective_id=0, has_side_effects=True, vmem_limit_bytes=VMEM_BYTES),
            name='evoformer_block',
        )(*operands)

    return jax.shard_map(local_block, mesh=mesh, in_specs=in_specs, out_specs=(rows_spec, rows_spec),
                         check_vma=False)
```

```python
import functools
import math

import jax
import jax.numpy as jnp
import numpy as np
from jax import lax
from jax.experimental import pallas as pl
from jax.experimental.pallas import tpu as pltpu
from jax.sharding import PartitionSpec as P

MASK_SCALE = 10000.0
LN_EPS = 1e-5
OPM_EPS = 1e-3
LOG2E = math.log2(math.e)
N_WEIGHTS = 13
PART_AXIS = 'data'
GROUP_AXIS = 'dap'
MESH = pl.DeviceIdType.MESH
F32 = jnp.float32
BF16 = jnp.bfloat16
HD = 32
U_LN, U_UNP, U_PROD, U_OUT = 12, 2, 4, 3
U_PR, U_PO, U_TP, U_CP, U_CM, U_CF = 2, 4, 3, 3, 3, 3
VMEM_BYTES = 60 * 1024 * 1024


def dot(a, b):
    return lax.dot(a, b, preferred_element_type=F32)


def dot_nt(a, b):
    return lax.dot_general(a, b, (((1,), (1,)), ((), ())), preferred_element_type=F32)


def dot_tn(a, b):
    return lax.dot_general(a, b, (((0,), (0,)), ((), ())), preferred_element_type=F32)


def layer_norm(x):
    x_float = x.astype(F32)
    centred = x_float - jnp.mean(x_float, axis=-1, keepdims=True)
    var = jnp.mean(centred * centred, axis=-1, keepdims=True)
    return (centred * lax.rsqrt(var + LN_EPS)).astype(BF16)


def seg(i, size):
    return slice(i * size, (i + 1) * size)


def sigmoid(x):
    return 1.0 / (1.0 + jnp.exp2(x * (-LOG2E)))


def iota(shape, dim):
    return lax.broadcasted_iota(jnp.int32, shape, dim)


def permutation(sizes, order, keep=None):
    total = int(np.prod(sizes))
    source = np.arange(total).reshape(sizes).transpose(order).reshape(-1)
    out = np.zeros((total, total), np.float32)
    out[np.arange(total), source] = 1.0
    return out


def softmax_cols(t):
    e = jnp.exp2(t - jnp.max(t, axis=0, keepdims=True))
    return (e * (1.0 / jnp.sum(e, axis=0, keepdims=True))).astype(BF16)


def same_half(width, lanes, half):
    return (iota((width, lanes), 0) // HD) % 2 == (iota((width, lanes), 1) // half) % 2


def staged_kernel(n, early, n_in, *refs):
    operands, rest = list(refs[:n_in]), refs[n_in:]
    late = [i for i in range(n_in) if i not in early]
    landing, sems = rest[-len(late) - 1:-1], rest[-1]
    copies = [pltpu.make_async_copy(operands[i], landing[k], sems.at[k]) for k, i in enumerate(late)]
    for copy in copies:
        copy.start()
    for k, i in enumerate(late):
        operands[i] = landing[k]

    def arrive():
        for copy in copies:
            copy.wait()
    block_kernel(n, arrive, *operands, *rest[:-len(late) - 1])


def block_kernel(n, arrive, x_ref, z_ref, mm_ref, rm_ref,
                 w_rb, w_r, w_ro, w_c, w_co, w_ac, w_oo, w_tsb, w_ts, w_tso, w_teb, w_te, w_teo,
                 p2, p2t, p3, p3t, p4, p4b, p4e, p4eb, p5, p6, p64, eye, tok, tok_l, tok_r,
                 out_m, out_z,
                 g_r0, g_r1, g_c, g_t1, g_t2, s1, r1, s2, r2, s3, r3, s4, r4,
                 tmp_b, b_q, bm_tri, x1, y1, m_t, rn, a_t, c_t, c_f, u_s, w_f32, w_fe, w_fet, z1, yn, x3,
                 q_s, k_s, v_s, g_s, o_s, s_buf, m_s, qc_s, kc_s, vc_s, gc_s, oc_s, mc_s,
                 gs_a, gr_a, gs_b, gr_b, gs_f, gr_f, as_sem, ar_sem):
    me = lax.axis_index(GROUP_AXIS)
    g_row = (g_r0, g_r1)
    chips = n // 2
    chip = me // 2
    core = me % 2
    partner = me + 1 - 2 * core
    crops, seqs, length, width = x_ref.shape
    rows = z_ref.shape[1]
    quads = rows // 4
    blocks = length // 64
    blk = 4 * rows
    sup = 4 * blk
    steps = []
    for k in reversed(range(chips // 2)):
        steps += sorted({k + 1, chips - k - 1}, reverse=True)
    near = (2, chips - 2, 1, chips - 1)
    far = tuple(k for k in steps if k not in near)
    middle_hops, last_hops = far[1:], far[:1] + (0,)

    barrier = pltpu.get_barrier_semaphore()
    for k in range(1, n):
        pl.semaphore_signal(barrier, inc=1, device_id={GROUP_AXIS: lax.rem(me + k, n)}, device_id_type=MESH)
    def remote(src, dst, send, recv, device):
        return pltpu.make_async_remote_copy(src_ref=src, dst_ref=dst, send_sem=send, recv_sem=recv,
                                            device_id={GROUP_AXIS: device}, device_id_type=MESH)

    def same_core(k):
        return 2 * lax.rem(chip + k, chips) + core

    def wait_bytes(ref, sem):
        pltpu.make_async_copy(ref, ref, sem).wait()

    def to_partner(block, e, c):
        remote(block, block, gs_b.at[e, c], gr_b.at[e, c], partner).start()

    def gather_start(buf, e, c, hops):
        mine = buf.at[c, me]
        for k in hops:
            remote(mine, mine, gs_a.at[e, c], gr_a.at[e, c], same_core(k)).start()
        to_partner(mine, e, c)

    def gather_forward(buf, e, c, hops):
        wait_bytes(buf.at[c, pl.ds(0, len(hops))], gr_a.at[e, c])
        for k in hops:
            to_partner(buf.at[c, same_core(k)], e, c)

    def gather_relay(buf, e, c, hops):
        wait_bytes(buf.at[c, pl.ds(0, len(hops))], gr_a.at[e, c])
        height = buf.shape[2]
        cut = height // 2 // 16 * 16
        for sign, part in ((1, pl.ds(0, cut)), (-1, pl.ds(cut, height - cut))):
            source = same_core(chips - 2 * sign)
            block = buf.at[c, source]
            remote(block, block, gs_f.at[e, c], gr_f.at[e, c], same_core(chips + sign)).start()
            half = buf.at[c, source, part]
            remote(half, half, gs_f.at[e, c], gr_f.at[e, c], same_core(chips + 2 * sign)).start()
        for k in hops:
            to_partner(buf.at[c, same_core(k)], e, c)

    def relay_forward(buf, e, c):
        wait_bytes(buf.at[c, pl.ds(0, len(far))], gr_f.at[e, c])
        for k in far:
            to_partner(buf.at[c, same_core(k)], e, c)

    def gather_wait(buf, e, c):
        wait_bytes(buf.at[c, pl.ds(0, chips)], gr_b.at[e, c])

    def gather_end(buf, e, c, hops):
        wait_bytes(buf.at[c, pl.ds(0, len(hops))], gs_a.at[e, c])
        wait_bytes(buf.at[c, pl.ds(0, chips)], gs_b.at[e, c])
        if hops is near:
            wait_bytes(buf.at[c, pl.ds(0, len(far))], gs_f.at[e, c])

    def rows_of(d, offset=0, height=None):
        return pl.ds(pl.multiple_of(d * blk + offset, 16), height or blk)

    def exchange_own(src, dst, index_of):
        dst[index_of(me)] = src[index_of(me)]

    def exchange_part(src, dst, e, c, index_of, hops):
        landing = dst.at[index_of(me)]
        for k in hops:
            for other in range(2):
                d = 2 * lax.rem(chip + k, chips) + (core + other) % 2
                if k or other:
                    remote(src.at[index_of(d)], landing, as_sem.at[e, c], ar_sem.at[e, c], d).start()

    def exchange_start(src, dst, e, c, index_of):
        exchange_own(src, dst, index_of)
        exchange_part(src, dst, e, c, index_of, steps + [0])

    def others(ref, c, planes):
        where = pl.ds(0, (n - 1) * blk)
        return ref.at[c, :, where, :] if planes else ref.at[c, where, :]

    def exchange_wait(dst, e, c, planes):
        wait_bytes(others(dst, c, planes), ar_sem.at[e, c])

    def exchange_end(src, e, c, planes):
        wait_bytes(others(src, c, planes), as_sem.at[e, c])

    def loop(count, body, unroll=1):
        def several(i, carry):
            for k in range(unroll):
                body(i * unroll + k)
            return carry
        lax.fori_loop(0, count // unroll, several, 0)

    def pack_bias(rows_f32):
        half = blk // 2
        last = jnp.concatenate([rows_f32[seg(g, half), 128:length] for g in range(2)], axis=1)
        return jnp.concatenate([rows_f32[:, 0:128], last, jnp.zeros((8, 128), F32)], axis=0).astype(BF16)

    tmp_b[:] = jnp.zeros_like(tmp_b)

    def row_bias(c):
        def one(i):
            tmp_b[pl.ds(pl.multiple_of(i * 8, 8), 8), :] = dot_nt(w_rb[:], layer_norm(z_ref[c, i]))
        loop(rows, one, U_LN)
        t = dot(p6[:], tmp_b[:].astype(BF16))
        for g, buf in enumerate(g_row):
            buf[c, me] = pack_bias(t[seg(g, blk), :])
    loop(crops, row_bias)
    pl.semaphore_wait(barrier, n - 1)
    arrive()

    def row_bias_send(c):
        for g, buf in enumerate(g_row):
            gather_start(buf, g, c, steps)
    row_bias_send(0)

    w_f32[:] = w_oo[:].astype(F32)
    for fp in range(HD // 2):
        for half in range(2):
            at = fp * 2 * HD + half * HD
            w_fe[at:at + HD, :] = w_f32[pl.ds(half * (HD // 2) + fp, HD, stride=HD), :]
    for b in range(HD * HD // 128):
        w_fet[:, seg(b, 128)] = w_fe[seg(b, 128), :].T.astype(BF16)
    q_s[:] = jnp.zeros_like(q_s)

    def unpack_bias(buf, c, perm, perm_last, pieces, piece):
        for sb in range(n // 4):
            moved = dot(perm[:], buf[c, seg(sb, 4), 0:blk, :].reshape(sup, 128)).astype(BF16)
            last = dot(perm_last[:], buf[c, seg(sb, 4), blk:, :].reshape(128, 128)).astype(BF16)
            for i in range(pieces):
                at = i * (4 * length // pieces) + sb * piece
                b_q[at:at + piece, 0:128] = moved[seg(i, piece), :]
                b_q[at:at + piece, 128:length] = last[seg(i % (pieces // 2), piece), seg(2 * i // pieces, 64)]

    def mask_columns(row, select):
        wide = jnp.broadcast_to(row.astype(F32), (128, length)).astype(BF16)
        return (dot_nt(select[:], wide) - 1.0) * (MASK_SCALE * LOG2E)

    scale = HD ** -0.5 * LOG2E
    two, four = 2 * length, 4 * length

    def project(y, w_t, first, stride=1):
        wide = y.shape[1]
        q = dot_nt(w_t[0:wide, :], jnp.concatenate([y, y], axis=0))
        q = jnp.where(same_half(wide, two, length), q, 0.0).astype(BF16)
        keys = dot_nt(y, w_t[wide:2 * wide, :]).astype(BF16)
        values = dot_nt(w_t[2 * wide:3 * wide, :], y).astype(BF16)
        gate = sigmoid(dot_nt(w_t[3 * wide:4 * wide, :], y))
        for g in range(wide // 128):
            u = first + g * stride
            q_s[u, 0:64, 0:two] = q[128 * g:128 * g + 64, :]
            q_s[u, 64:128, two:four] = q[128 * g + 64:128 * g + 128, :]
            k_s[u] = keys[:, seg(g, 128)]
            v_s[u] = values[seg(g, 128), :]
            g_s[u] = gate[seg(g, 128), :]

    def attend(first, count, bias_of):
        def mix(u, probs):
            pieces = []
            for p in range(2):
                mixed = dot(v_s[u, seg(p, 64), :], probs[:, seg(p, two)])
                pieces += [mixed[0:HD, 0:length], mixed[HD:2 * HD, length:two]]
            return jnp.concatenate(pieces, axis=0)

        def finish(u, mixed):
            o_s[u] = (g_s[u] * mixed).astype(BF16)

        s_buf[0] = dot(k_s[first], q_s[first])

        def pair(i):
            u = first + 2 * i
            s_buf[1] = dot(k_s[u + 1], q_s[u + 1])
            mixed = mix(u, softmax_cols(s_buf[0] * scale + bias_of(u)))
            after = jnp.minimum(u + 2, first + count - 1)
            s_buf[0] = dot(k_s[after], q_s[after])
            probs = softmax_cols(s_buf[1] * scale + bias_of(u + 1))
            finish(u, mixed)
            finish(u + 1, mix(u + 1, probs))
        loop(count // 2, pair, 2)

    groups = width // 128

    def row_attention(c):
        def before(s):
            m_s[s] = mask_columns(mm_ref[c, pl.ds(me * seqs + s, 1), :], eye)
            project(layer_norm(x_ref[c, s]), w_r, s, seqs)
        loop(seqs, before, U_PR)
        pl.when(c == 0)(lambda: row_bias_send(1))
        for g, buf in enumerate(g_row):
            gather_forward(buf, g, c, steps)
            gather_wait(buf, g, c)
            unpack_bias(buf, c, p4, p4b, 4, blk)
            for pair in range(2):
                bm_tri[:, seg(pair, two)] = dot_nt(eye[:], b_q[seg(pair, two), :]) * LOG2E

            def bias_of(u):
                return bm_tri[:] + jnp.concatenate([m_s[u - g * seqs]] * (four // 128), axis=1)
            attend(g * seqs, seqs, bias_of)

        def after(s):
            gated = jnp.concatenate([o_s[g * seqs + s] for g in range(groups)], axis=0)
            x1[s] = (x_ref[c, s].astype(F32) + dot_tn(gated, w_ro[:])).astype(BF16)
        loop(seqs, after, U_PO)
        for b in range(blocks):
            part = x1[:, seg(b, 64), :].reshape(256, width)
            s1[c, seg(b, 256), :] = dot(p2[:], part).astype(BF16)
        exchange_start(s1, r1, 0, c, lambda d: (c, rows_of(d)))
    loop(crops, row_attention)

    def send_back(c, hops):
        exchange_part(s2, r2, 1, c, lambda d: (c, rows_of(d)), hops)

    def columns(c):
        exchange_wait(r1, 0, c, False)
        for sb in range(n // 4):
            moved = dot(p3[:], r1[c, seg(sb, sup), :]).astype(BF16)
            for i in range(rows):
                y1[i, seg(sb, 16), :] = moved[seg(i, 16), :]
        n_seq = y1.shape[1]
        mk = mm_ref[c].astype(F32).astype(BF16)
        mine = (iota((16, length), 1) == me * rows + iota((16, length), 0)).astype(F32).astype(BF16)
        m_t[:] = dot_nt(mine, jnp.concatenate([mk, mk], axis=0))
        rn[c] = 1.0 / (dot(m_t[:, 0:n_seq].astype(BF16), mk) + OPM_EPS)
        low = iota((HD, 2 * n_seq), 1) < n_seq
        mask_all = (dot_nt(mk, mine) - 1.0) * (MASK_SCALE * LOG2E)
        for i in range(rows):
            mc_s[i] = jnp.broadcast_to(mask_all[:, i:i + 1], (n_seq, 128))
        tokens = 4 * n_seq

        def doubled(y):
            return jnp.concatenate([y[n_seq * (r // 2):n_seq * (r // 2 + 1), :] for r in range(8)], axis=0)

        def before(q):
            y = layer_norm(y1[pl.ds(4 * q, 4)].reshape(tokens, width))
            qq = dot_nt(w_c[0:width, :], doubled(y))
            qc_s[q] = jnp.where(same_half(width, 2 * tokens, n_seq), qq, 0.0).astype(BF16)
            kc_s[q] = dot_nt(y, w_c[width:2 * width, :]).astype(BF16)
            vc_s[q] = dot_nt(y, w_c[2 * width:3 * width, :]).astype(BF16)
            gc_s[q] = sigmoid(dot_nt(w_c[3 * width:4 * width, :], y))
        loop(quads, before, U_CP)

        @pl.when(c == 1)
        def _():
            gather_relay(g_c, 2, 0, near)
            send_back(0, middle_hops)

        def middle(q):
            zeros = jnp.zeros((64, 128), BF16)
            for g in range(groups):
                heads = [[] for _ in range(4)]
                for r in range(4):
                    at = n_seq * r
                    wide = qc_s[q, seg(g, 128), seg(r, 128)]
                    stacked = jnp.concatenate([jnp.concatenate([wide[0:64], zeros], axis=0),
                                               jnp.concatenate([zeros, wide[64:128]], axis=0)], axis=1)
                    logits = dot(kc_s[q, at:at + n_seq, seg(g, 128)], stacked)
                    col = mc_s[4 * q + r]
                    probs = softmax_cols(logits * scale + jnp.concatenate([col, col], axis=1))
                    mixed = dot_tn(vc_s[q, at:at + n_seq, seg(g, 128)], probs)
                    for h in range(4):
                        heads[h].append(mixed[seg(h, HD), seg(h, n_seq)])
                mixed = jnp.concatenate([jnp.concatenate(h, axis=1) for h in heads], axis=0)
                oc_s[q, seg(g, 128), :] = (gc_s[q, seg(g, 128), :] * mixed).astype(BF16)
        loop(quads, middle, U_CM)

        def after(q):
            update = dot_tn(oc_s[q], w_co[:])
            x = y1[pl.ds(4 * q, 4)].reshape(tokens, width).astype(F32)
            y1[pl.ds(4 * q, 4)] = (x + update).astype(BF16).reshape(4, n_seq, width)
        loop(quads, after, U_CF)

        def factors(q):
            y = layer_norm(y1[pl.ds(4 * q, 4)].reshape(tokens, width))
            all_four = dot_nt(w_ac[:], doubled(y)).astype(BF16).astype(F32)
            half = HD // 2
            for r in range(4):
                i = 4 * q + r
                both = all_four[:, seg(r, 128)] * m_t[pl.ds(i, 1), :]
                a = both[0:HD, :]
                at = pl.ds(pl.multiple_of(i * HD, HD), HD)
                a_t[c, 0, at, :] = jnp.where(low, a, 0.0).astype(BF16)
                a_t[c, 1, at, :] = jnp.where(low, 0.0, a).astype(BF16)
                packed = jnp.where(low[0:half], both[HD:HD + half, :], both[HD + half:2 * HD, :])
                c_t[pl.ds(pl.multiple_of(i * half, half), half), :] = packed.astype(BF16)
        loop(quads, factors, U_CF)
        g_c[c, me] = dot(p5[:], c_t[:]).astype(BF16)
        gather_start(g_c, 2, c, near)
        for db in range(n // 4):
            part = y1[:, seg(db, 16), :].reshape(16 * rows, width)
            s2[c, seg(db, sup), :] = dot(p3t[:], part).astype(BF16)
        exchange_own(s2, r2, lambda d: (c, rows_of(d)))

        @pl.when(c == 0)
        def _():
            send_back(0, near)

        @pl.when(c == 1)
        def _():
            send_back(0, last_hops)
    loop(crops, columns)

    def bias_row(i, y, w_b):
        tmp_b[pl.ds(pl.multiple_of(i * 8, 8), 4), :] = dot_nt(w_b[:], y)

    def bias_send(buf, e, c, hops):
        buf[c, me] = pack_bias(dot(p6[0:blk, :], tmp_b[:].astype(BF16)))
        gather_start(buf, e, c, hops)

    def start_project(c):
        loop(rows, lambda i: project(yn[c, i], w_ts, i), U_TP)

    def outer(c):
        @pl.when(c == 0)
        def _():
            relay_forward(g_c, 2, 0)
        gather_wait(g_c, 2, c)

        def unpack(q):
            for sb in range(n // 4):
                part = g_c[c, 4 * sb:4 * sb + 4, pl.ds(pl.multiple_of(blk * q, 16), blk), :].reshape(sup, 128)
                moved = dot(p4[:], part).astype(BF16)
                for i in range(4):
                    c_f[4 * q + i, seg(sb, blk), :] = moved[seg(i, blk), :]
        loop(HD // 2 // 4, unpack, U_UNP)

        def products(fp):
            for half in range(2):
                u = dot_nt(a_t[c, half], c_f[fp])
                for i in range(rows):
                    at = pl.ds(pl.multiple_of(fp * 2 * HD + half * HD, HD), HD)
                    u_s[i, at, :] = (u[seg(i, HD), :] * rn[c, i:i + 1, :]).astype(BF16)
        loop(HD // 2, products, U_PROD)

        @pl.when(c == 1)
        def _():
            send_back(1, last_hops)

        def one(i):
            update = dot(w_fet[:], u_s[i])
            z1[c, i] = (z_ref[c, i].astype(F32) + update.T).astype(BF16)
        loop(rows, one, U_OUT)

        @pl.when(c == 0)
        def _():
            gather_relay(g_c, 2, 1, near)
            send_back(1, near)

        def norm(i):
            y = layer_norm(z1[c, i])
            yn[c, i] = y
            bias_row(i, y, w_tsb)
        loop(rows, norm, U_LN)

        @pl.when(c == 0)
        def _():
            start_project(0)
            relay_forward(g_c, 2, 1)
        bias_send(g_t1, 3, c, steps)

        @pl.when(c == 0)
        def _():
            send_back(1, middle_hops)

        @pl.when(c == 1)
        def _():
            gather_forward(g_t1, 3, 0, steps)
    loop(crops, outer)

    def relay_bias_at(turn, q, c):
        pl.when(turn & (q == 0))(lambda: gather_relay(g_t2, 4, c, near))

    def triangle(c, w_out, done):
        def quad(q):
            attend(4 * q, 4, lambda u: bm_tri[:])

            def after(k):
                i = 4 * q + k
                x3[i] = (z1[c, i].astype(F32) + dot_tn(o_s[i], w_out[:])).astype(BF16)
            loop(4, after, 4)
            done(q)
        loop(quads, quad)

    def start_node(c):
        @pl.when(c == 1)
        def _():
            start_project(1)
            gather_forward(g_t1, 3, 1, steps)
        gather_wait(g_t1, 3, c)
        unpack_bias(g_t1, c, p4, p4b, 4, blk)
        col = mask_columns(rm_ref[pl.ds(c, 1), :], eye)
        col3 = jnp.concatenate([col] * (two // 128), axis=1)
        for pair in range(2):
            bm_tri[:, seg(pair, two)] = dot_nt(eye[:], b_q[seg(pair, two), :]) * LOG2E + col3

        def done(q):
            for k in range(4):
                i = 4 * q + k
                bias_row(i, layer_norm(x3[i]), w_teb)

            @pl.when(q == quads - 1)
            def _():
                bias_send(g_t2, 4, c, near)
            for b in range(blocks):
                part = x3[pl.ds(4 * q, 4), seg(b, 64), :].reshape(256, 128)
                s3[c, q, seg(b, 256), :] = dot(p2[:], part).astype(BF16)
            exchange_start(s3, r3, 2, c, lambda d: (c, q, rows_of(d)))
            relay_bias_at(c == 1, q, 0)
        triangle(c, w_tso, done)
    loop(crops, start_node)

    def end_node(c):
        exchange_wait(r3, 2, c, True)
        for q in range(quads):
            for sb in range(n // 4):
                moved = dot(p3[:], r3[c, q, seg(sb, sup), :]).astype(BF16)
                for i in range(rows):
                    at = 64 * q + 16 * sb
                    z1[c, i, at:at + 16, :] = moved[seg(i, 16), :]
        loop(rows, lambda i: project(layer_norm(z1[c, i]), w_te, i), U_TP)
        relay_forward(g_t2, 4, c)
        gather_wait(g_t2, 4, c)
        unpack_bias(g_t2, c, p4e, p4eb, 4 * quads, 16)
        col = mask_columns(rm_ref[pl.ds(c, 1), :], tok)
        col3 = jnp.concatenate([col] * (two // 128), axis=1)
        for pair in range(2):
            left = dot_nt(b_q[seg(2 * pair, length), :], tok_l[:])
            right = dot_nt(b_q[seg(2 * pair + 1, length), :], tok_r[:])
            bm_tri[:, seg(pair, two)] = (left + right) * LOG2E + col3

        def done(q):
            for p in range(quads):
                for db in range(n // 4):
                    part = x3[pl.ds(4 * q, 4), 64 * p + 16 * db:64 * p + 16 * (db + 1), :].reshape(64, 128)
                    moved = dot(p64[:], part).astype(BF16)
                    for i in range(4):
                        s4[c, p, rows_of(4 * db + i, 16 * q, 16), :] = moved[seg(i, 16), :]
            relay_bias_at(c == 0, q, 1)
            exchange_start(s4, r4, 3, c, lambda d: (c, slice(None), rows_of(d, 16 * q, 16)))
        triangle(c, w_teo, done)
    loop(crops, end_node)

    def finish_msa(c):
        exchange_wait(r2, 1, c, False)
        for b in range(blocks):
            moved = dot(p2t[:], r2[c, seg(b, 256), :]).astype(BF16)
            for i in range(seqs):
                out_m[c, i, seg(b, 64), :] = moved[seg(i, 64), :]
    loop(crops, finish_msa)

    def finish_pair(c):
        exchange_wait(r4, 3, c, True)
        for q in range(quads):
            for b in range(blocks):
                moved = dot(p2t[:], r4[c, q, seg(b, 256), :]).astype(BF16)
                for i in range(4):
                    out_z[c, 4 * q + i, seg(b, 64), :] = moved[seg(i, 64), :]
    loop(crops, finish_pair)

    def drain(c):
        for e, (buf, hops) in enumerate([(b, steps) for b in g_row] + [(g_c, near), (g_t1, steps), (g_t2, near)]):
            gather_end(buf, e, c, hops)
        for e, (buf, planes) in enumerate(((s1, False), (s2, False), (s3, True), (s4, True))):
            exchange_end(buf, e, c, planes)
    loop(crops, drain)


def solution(mesh):
    n = mesh.shape[GROUP_AXIS]
    rows_spec = P(PART_AXIS, GROUP_AXIS)
    in_specs = (rows_spec, rows_spec, P(PART_AXIS), P(PART_AXIS)) + (P(),) * N_WEIGHTS

    def local_block(msa, pair, msa_mask, res_mask, *weights):
        (w_rb, w_r, w_ro, w_c, w_co, w_ac, w_oo, w_tsb, w_ts, w_tso, w_teb, w_te, w_teo) = weights
        crops, seqs, length, width = msa.shape
        rows, pair_width = pair.shape[1], pair.shape[3]
        n_seq = msa_mask.shape[1]
        heads, tri_heads = w_r.shape[2], w_ts.shape[2]
        quads = rows // 4

        def flat_t(w):
            return jnp.transpose(w, (1, 2, 3, 0)).reshape(-1, w.shape[0])

        bias_t = w_rb.T
        operands = [
            msa, pair, msa_mask, res_mask,
            bias_t, flat_t(w_r), w_ro.reshape(width, width), flat_t(w_c), w_co.reshape(width, width),
            jnp.transpose(w_ac, (1, 2, 0)).reshape(-1, width), w_oo.reshape(-1, pair_width),
            w_tsb.T, flat_t(w_ts), w_tso.reshape(pair_width, pair_width),
            w_teb.T, flat_t(w_te), w_teo.reshape(pair_width, pair_width),
        ]
        p2 = permutation((4, 64), (1, 0))
        p3 = permutation((4, rows, 4), (1, 0, 2))
        p4 = permutation((4, 4, rows), (1, 0, 2))
        p4e = permutation((4, 4, quads, 4), (1, 2, 0, 3))

        def last(p):
            half = p[:len(p) // 2].reshape(-1, 4, 4 * rows)[:, :, :2 * rows]
            blank = np.zeros(half.shape[:2] + (32 - 2 * rows,))
            return np.concatenate([half, blank], axis=2).reshape(len(half), -1)
        p5 = permutation((rows, HD // 2), (1, 0))
        p6 = permutation((rows, heads), (1, 0))
        p64 = permutation((4, 4, 4), (1, 0, 2))
        tok = permutation((n, quads, 4), (1, 0, 2))
        consts = [p2, p2.T, p3, p3.T, p4, last(p4), p4e, last(p4e), p5, p6, p64, np.eye(length), tok,
                  np.concatenate([tok, 0 * tok]), np.concatenate([0 * tok, tok])]
        first_const, names = len(operands), [a is p6 for a in consts]
        operands += [jnp.asarray(a, BF16) for a in consts]

        vmem = pl.BlockSpec(memory_space=pltpu.VMEM)
        anywhere = pl.BlockSpec(memory_space=pl.ANY)
        early = tuple(i for i, a in enumerate(operands) if a is pair or a is bias_t or (i >= first_const and names[i - first_const]))
        total = n * 4 * rows
        bias = pltpu.VMEM((crops, n, 4 * rows + 32, 128), BF16)
        scratch = [
            bias, bias,
            pltpu.VMEM((crops, n, HD // 2 * rows, 128), BF16),
            bias, bias,
        ]
        scratch += [pltpu.VMEM((crops, total, width), BF16)] * 4
        scratch += [pltpu.VMEM((crops, quads, total, pair_width), BF16)] * 4
        scratch += [
            pltpu.VMEM((8 * rows, length), F32),
            pltpu.VMEM((tri_heads * length, length), BF16),
            pltpu.VMEM((length, tri_heads * length), F32),
            pltpu.VMEM((seqs, length, width), BF16),
            pltpu.VMEM((rows, n_seq, width), BF16),
            pltpu.VMEM((16, 2 * n_seq), F32),
            pltpu.VMEM((crops, 16, length), F32),
            pltpu.VMEM((crops, 2, rows * HD, 128), BF16),
            pltpu.VMEM((rows * HD // 2, 128), BF16),
            pltpu.VMEM((HD // 2, length, 128), BF16),
            pltpu.VMEM((rows, HD * HD, length), BF16),
            pltpu.VMEM((HD * HD, pair_width), F32),
            pltpu.VMEM((HD * HD, pair_width), F32),
            pltpu.VMEM((pair_width, HD * HD), BF16),
            pltpu.VMEM((crops, rows, length, pair_width), BF16),
            pltpu.VMEM((crops, rows, length, pair_width), BF16),
            pltpu.VMEM((rows, length, pair_width), BF16),
            pltpu.VMEM((rows, 128, 4 * length), BF16),
            pltpu.VMEM((rows, length, 128), BF16),
            pltpu.VMEM((rows, 128, length), BF16),
            pltpu.VMEM((rows, 128, length), F32),
            pltpu.VMEM((rows, 128, length), BF16),
            pltpu.VMEM((2, length, 4 * length), F32),
            pltpu.VMEM((seqs, length, 128), F32),
            pltpu.VMEM((quads, width, 8 * n_seq), BF16),
            pltpu.VMEM((quads, 4 * n_seq, width), BF16),
            pltpu.VMEM((quads, 4 * n_seq, width), BF16),
            pltpu.VMEM((quads, width, 4 * n_seq), F32),
            pltpu.VMEM((quads, width, 4 * n_seq), BF16),
            pltpu.VMEM((rows, n_seq, 128), F32),
        ]
        scratch += [pltpu.SemaphoreType.DMA((5, crops))] * 8
        late = [a for i, a in enumerate(operands) if i not in early]
        scratch += [pltpu.VMEM(a.shape, a.dtype) for a in late] + [pltpu.SemaphoreType.DMA((len(late),))]
        return pl.pallas_call(
            functools.partial(staged_kernel, n, early, len(operands)),
            out_shape=(jax.ShapeDtypeStruct(msa.shape, BF16), jax.ShapeDtypeStruct(pair.shape, BF16)),
            in_specs=[vmem if i in early else anywhere for i in range(len(operands))],
            out_specs=(vmem, vmem),
            scratch_shapes=scratch,
            compiler_params=pltpu.CompilerParams(collective_id=0, has_side_effects=True, vmem_limit_bytes=VMEM_BYTES),
            name='evoformer_block',
        )(*operands)

    return jax.shard_map(local_block, mesh=mesh, in_specs=in_specs, out_specs=(rows_spec, rows_spec),
                         check_vma=False)
```
